8 devices in a mesh: dp: 1 (over z), cp: 8 (over y, x, core).
Axes of the slice: x: 2, y: 2, z: 1, core: 2. Of those that a mesh axis runs over, the one named last changes fastest.
Arguments:
- x_in: bfloat16 [1536, 3584], P(('dp', 'cp'))
- dy_in: bfloat16 [1536, 3584], P(('dp', 'cp'))
- doc_id: int32 [1536], P(('dp', 'cp'))
- w_q: bfloat16 [3584, 7, 128], replicated
- w_k: bfloat16 [3584, 1, 128], replicated
- w_v: bfloat16 [3584, 1, 128], replicated
- w_o: bfloat16 [7, 128, 3584], replicated
Outputs:
- output 1: bfloat16 [1536, 3584], P(('dp', 'cp'))
- output 2: bfloat16 [1536, 3584], P(('dp', 'cp'))
All inputs are finite; a program needn't handle non-finite values.
Results may differ from the reference program's by a relative error of at most 0.00949353.
Values are sent between devices in bfloat16 or wider.
A program may use at most 1 GiB of HBM per device.

```python
import jax
import jax.numpy as jnp
from jax import lax

D_MODEL = 3584
Q_HEADS = 7
KV_HEADS = 1
HEAD_DIM = 128
TOK_DEV = 192
GROUP_DEVS = 8
SEQ_LEN = GROUP_DEVS * TOK_DEV
PIECE_LEN = TOK_DEV // 2
QUERY_GROUP = Q_HEADS // KV_HEADS
DOC_CUTS = max(1, GROUP_DEVS // 2)
NEG_BIG = -1.0e30


def stored_positions():
    row_idx = jnp.arange(SEQ_LEN, dtype=jnp.int32)
    owner_dev = row_idx // TOK_DEV
    offset = row_idx % TOK_DEV
    piece_idx = jnp.where(offset < PIECE_LEN, owner_dev, 2 * GROUP_DEVS - 1 - owner_dev)
    return piece_idx * PIECE_LEN + offset % PIECE_LEN


def setup_inputs(seed: int = 0, part: int = 0) -> dict:
    part_key = jax.random.fold_in(jax.random.key(seed), part)
    key_x, key_dy, key_doc = jax.random.split(part_key, 3)
    key_q, key_k, key_v, key_o = jax.random.split(jax.random.key(seed + 1), 4)
    in_scale = D_MODEL ** -0.5
    out_scale = (Q_HEADS * HEAD_DIM) ** -0.5
    x_in = jax.random.normal(key_x, (SEQ_LEN, D_MODEL), jnp.float32).astype(jnp.bfloat16)
    dy_in = jax.random.normal(key_dy, (SEQ_LEN, D_MODEL), jnp.float32).astype(jnp.bfloat16)
    cut_pos = jax.random.randint(key_doc, (DOC_CUTS,), 1, SEQ_LEN, dtype=jnp.int32)
    doc_id = jnp.sum((stored_positions()[:, None] >= cut_pos[None, :]).astype(jnp.int32), axis=1)
    w_q = (jax.random.normal(key_q, (D_MODEL, Q_HEADS, HEAD_DIM), jnp.float32) * in_scale).astype(jnp.bfloat16)
    w_k = (jax.random.normal(key_k, (D_MODEL, KV_HEADS, HEAD_DIM), jnp.float32) * in_scale).astype(jnp.bfloat16)
    w_v = (jax.random.normal(key_v, (D_MODEL, KV_HEADS, HEAD_DIM), jnp.float32) * in_scale).astype(jnp.bfloat16)
    w_o = (jax.random.normal(key_o, (Q_HEADS, HEAD_DIM, D_MODEL), jnp.float32) * out_scale).astype(jnp.bfloat16)
    return {'x_in': x_in, 'dy_in': dy_in, 'doc_id': doc_id, 'w_q': w_q, 'w_k': w_k, 'w_v': w_v, 'w_o': w_o}


def reference(x_in, dy_in, doc_id, w_q, w_k, w_v, w_o):
    score_scale = HEAD_DIM ** -0.5
    all_pos = stored_positions()
    wq_flat = w_q.reshape(D_MODEL, Q_HEADS * HEAD_DIM)
    wk_flat = w_k.reshape(D_MODEL, KV_HEADS * HEAD_DIM)
    wv_flat = w_v.reshape(D_MODEL, KV_HEADS * HEAD_DIM)
    wo_flat = w_o.reshape(Q_HEADS * HEAD_DIM, D_MODEL)
    q_all = jnp.dot(x_in, wq_flat, preferred_element_type=jnp.float32).astype(jnp.bfloat16)
    q_all = q_all.reshape(SEQ_LEN, KV_HEADS, QUERY_GROUP, HEAD_DIM)
    k_all = jnp.dot(x_in, wk_flat, preferred_element_type=jnp.float32).astype(jnp.bfloat16)
    v_all = jnp.dot(x_in, wv_flat, preferred_element_type=jnp.float32).astype(jnp.bfloat16)
    k_wide = k_all.reshape(SEQ_LEN, KV_HEADS, HEAD_DIM).astype(jnp.float32)
    v_wide = v_all.reshape(SEQ_LEN, KV_HEADS, HEAD_DIM).astype(jnp.float32)
    do_all = jnp.dot(dy_in, wo_flat.T, preferred_element_type=jnp.float32).astype(jnp.bfloat16)
    do_all = do_all.reshape(SEQ_LEN, KV_HEADS, QUERY_GROUP, HEAD_DIM)

    def block_step(grad_acc, block_idx):
        dk_acc, dv_acc = grad_acc
        row_start = block_idx * TOK_DEV
        q_blk = lax.dynamic_slice_in_dim(q_all, row_start, TOK_DEV, 0).astype(jnp.float32)
        do_blk = lax.dynamic_slice_in_dim(do_all, row_start, TOK_DEV, 0).astype(jnp.float32)
        pos_blk = lax.dynamic_slice_in_dim(all_pos, row_start, TOK_DEV, 0)
        doc_blk = lax.dynamic_slice_in_dim(doc_id, row_start, TOK_DEV, 0)
        visible = (all_pos[None, :] <= pos_blk[:, None]) & (doc_id[None, :] == doc_blk[:, None])
        scores = jnp.einsum('tkge,ske->tkgs', q_blk, k_wide) * score_scale
        scores = jnp.where(visible[:, None, None, :], scores, NEG_BIG)
        log_norm = jax.nn.logsumexp(scores, axis=-1, keepdims=True)
        prob_blk = jnp.exp(scores - log_norm).astype(jnp.bfloat16).astype(jnp.float32)
        out_blk = jnp.einsum('tkgs,ske->tkge', prob_blk, v_wide).astype(jnp.bfloat16).astype(jnp.float32)
        delta_row = jnp.sum(do_blk * out_blk, axis=-1, keepdims=True)
        d_prob = jnp.einsum('tkge,ske->tkgs', do_blk, v_wide)
        d_score = (prob_blk * (d_prob - delta_row)).astype(jnp.bfloat16).astype(jnp.float32)
        dq_blk = (jnp.einsum('tkgs,ske->tkge', d_score, k_wide) * score_scale).astype(jnp.bfloat16)
        dk_acc = dk_acc + jnp.einsum('tkgs,tkge->ske', d_score, q_blk) * score_scale
        dv_acc = dv_acc + jnp.einsum('tkgs,tkge->ske', prob_blk, do_blk)
        return (dk_acc, dv_acc), (out_blk.astype(jnp.bfloat16), dq_blk)

    zero_grad = jnp.zeros((SEQ_LEN, KV_HEADS, HEAD_DIM), jnp.float32)
    grad_sums, block_outs = lax.scan(block_step, (zero_grad, zero_grad), jnp.arange(GROUP_DEVS))
    dk_sum, dv_sum = grad_sums
    out_blocks, dq_blocks = block_outs
    out_all = out_blocks.reshape(SEQ_LEN, Q_HEADS * HEAD_DIM)
    dq_all = dq_blocks.reshape(SEQ_LEN, Q_HEADS * HEAD_DIM)
    y_out = jnp.dot(out_all, wo_flat, preferred_element_type=jnp.float32).astype(jnp.bfloat16)
    dk_bf = dk_sum.astype(jnp.bfloat16).reshape(SEQ_LEN, KV_HEADS * HEAD_DIM)
    dv_bf = dv_sum.astype(jnp.bfloat16).reshape(SEQ_LEN, KV_HEADS * HEAD_DIM)
    dx_wide = (jnp.dot(dq_all, wq_flat.T, preferred_element_type=jnp.float32)
               + jnp.dot(dk_bf, wk_flat.T, preferred_element_type=jnp.float32)
               + jnp.dot(dv_bf, wv_flat.T, preferred_element_type=jnp.float32))
    dx_out = dx_wide.astype(jnp.bfloat16)
    return y_out, dx_out
```

```python
import functools
import math

import jax
import jax.numpy as jnp
from jax import lax
from jax.experimental import pallas as pl
from jax.experimental.pallas import tpu as pltpu
from jax.sharding import PartitionSpec as P

NEG_BIG = -1.0e30
F32 = jnp.float32
BF16 = jnp.bfloat16

NDEV = 8
HEADS = 7
E = 128
PIECE = 96
TOK = 192
D = 3584
HE = HEADS * E
ROWS = HEADS * PIECE
HALF = NDEV * PIECE
CH = 256

NT = (((1,), (1,)), ((), ()))
NN = (((1,), (0,)), ((), ()))


def dot(a, b, dims=NN):
    return lax.dot_general(a, b, dims, preferred_element_type=F32)


def kernel(x_hbm, dy_hbm, doc_ref, wq_hbm, wk_hbm, wv_hbm, wo_hbm,
           y_hbm, dx_hbm,
           x_s, dy_s, wq_s, wkv_s, wo_s,
           kv_s, doc_s, q_s, do_s, qt_s, dot_s, cap_s,
           s_s, p_s, dp_s, ds_s, o_s, dq_s, delta_s,
           accv_t, acck_t, acc_s, rb1, comb, rb2,
           y_s, dx_s, dxo_s,
           in_sem, wq_sem, wo_sem, out_sem,
           doc_send, doc_recv, kv_send, kv_recv,
           d2d_send, d2d_recv, rs_send, rs_recv):
    me = lax.axis_index('cp')
    core = lax.rem(me, 2)
    chip = me // 2
    cx = lax.rem(chip, 2)
    cy = chip // 2

    def dev(r):
        yy = lax.rem(cy + (r // 4), 2)
        xx = lax.rem(cx + ((r // 2) % 2), 2)
        cc = lax.rem(core + (r % 2), 2)
        return yy * 4 + xx * 2 + cc

    def rcopy(src, dst, ssem, rsem, r):
        return pltpu.make_async_remote_copy(src_ref=src, dst_ref=dst, send_sem=ssem, recv_sem=rsem,
                                            device_id={'cp': dev(r)}, device_id_type=pl.DeviceIdType.MESH)

    barrier = pltpu.get_barrier_semaphore()
    for r in range(1, NDEV):
        pl.semaphore_signal(barrier, inc=1, device_id={'cp': dev(r)}, device_id_type=pl.DeviceIdType.MESH)

    ld_x = pltpu.make_async_copy(x_hbm, x_s, in_sem.at[0])
    ld_wk = pltpu.make_async_copy(wk_hbm, wkv_s.at[:, 0:E], in_sem.at[1])
    ld_wv = pltpu.make_async_copy(wv_hbm, wkv_s.at[:, E:2 * E], in_sem.at[2])
    ld_dy = pltpu.make_async_copy(dy_hbm, dy_s, in_sem.at[3])
    ld_wq = [pltpu.make_async_copy(wq_hbm.at[h], wq_s.at[:, h * E:(h + 1) * E], wq_sem.at[h]) for h in range(HEADS)]
    ld_wo = [pltpu.make_async_copy(wo_hbm.at[h * E:(h + 1) * E], wo_s.at[h * E:(h + 1) * E], wo_sem.at[h])
             for h in range(HEADS)]
    for c in [ld_x, ld_wk, ld_wv] + ld_wq + [ld_dy] + ld_wo:
        c.start()

    my_off = pl.multiple_of(me * PIECE, 32)
    ld_x.wait()
    ld_wk.wait()
    ld_wv.wait()
    kv_own = dot(x_s[...], wkv_s[...]).astype(BF16)
    for t in range(2):
        for half in range(2):
            kv_s[t, half, pl.ds(my_off, PIECE), :] = kv_own[half * PIECE:(half + 1) * PIECE, t * E:(t + 1) * E]
    doc_s[me] = doc_ref[...]

    def kv_blk(owner):
        return kv_s.at[:, :, pl.ds(pl.multiple_of(owner * PIECE, 32), PIECE), :]

    pl.semaphore_wait(barrier, NDEV - 1)
    kv_out = {}
    for r in (2, 4, 6, 1):
        kv_out[r] = rcopy(kv_blk(me), kv_blk(me), kv_send.at[r], kv_recv.at[r], r)
        kv_out[r].start()
    doc_out = {}
    for r in range(1, NDEV):
        doc_out[r] = rcopy(doc_ref, doc_s.at[me], doc_send.at[r], doc_recv.at[r], r)
        doc_out[r].start()

    def kv_in(r):
        return rcopy(kv_blk(dev(r)), kv_blk(dev(r)), kv_send.at[r], kv_recv.at[r], r)

    def put_rows(dst, val, h):
        dst[0, h * PIECE:(h + 1) * PIECE, :] = val[0:PIECE]
        dst[1, h * PIECE:(h + 1) * PIECE, :] = val[PIECE:TOK]

    for h0 in range(0, HEADS, 2):
        n = min(2, HEADS - h0)
        for h in range(h0, h0 + n):
            ld_wq[h].wait()
        val = dot(x_s[...], wq_s[:, h0 * E:(h0 + n) * E]).astype(BF16)
        for j in range(n):
            put_rows(q_s, val[:, j * E:(j + 1) * E], h0 + j)

    def forward(r):
        kv_in(r).wait_recv()
        kv_out[r + 1] = rcopy(kv_blk(dev(r)), kv_blk(dev(r)), kv_send.at[r + 1], kv_recv.at[r + 1], 1)
        kv_out[r + 1].start()

    forward(2)
    forward(4)

    ld_dy.wait()
    for h0 in range(0, HEADS, 2):
        n = min(2, HEADS - h0)
        for h in range(h0, h0 + n):
            ld_wo[h].wait()
        val = dot(dy_s[...], wo_s[h0 * E:(h0 + n) * E, :], NT).astype(BF16)
        for j in range(n):
            put_rows(do_s, val[:, j * E:(j + 1) * E], h0 + j)
    forward(6)

    for piece in range(2):
        qt_s[piece] = q_s[piece].T
        dot_s[piece] = do_s[piece].T

    for r in range(1, NDEV):
        rcopy(doc_ref, doc_s.at[dev(r)], doc_send.at[r], doc_recv.at[r], r).wait_recv()
    my_doc = doc_ref[...].astype(F32)
    eye = (lax.broadcasted_iota(jnp.int32, (TOK, TOK), 0) == lax.broadcasted_iota(jnp.int32, (TOK, TOK), 1))
    doc_col = jnp.sum(jnp.where(eye, jnp.broadcast_to(my_doc, (TOK, TOK)), 0.0), axis=1, keepdims=True)
    less = jnp.zeros((TOK, TOK), F32)
    for d in range(NDEV):
        less = less + jnp.where(doc_s[d].astype(F32) < doc_col, 1.0, 0.0)
    first = jnp.sum(less, axis=1, keepdims=True)
    rowi = lax.broadcasted_iota(jnp.int32, (PIECE, 1), 0)
    pos_lo = (me * PIECE + rowi).astype(F32)
    pos_hi = ((2 * NDEV - 1 - me) * PIECE + rowi).astype(F32)
    lane = lax.broadcasted_iota(jnp.int32, (1, HALF), 1).astype(F32)
    kpos_lo = lane
    kpos_hi = (2 * NDEV - 1) * PIECE + lane - 2 * PIECE * jnp.floor((lane + 0.5) * (1.0 / PIECE))

    def cap_of(kpos, lo, hi):
        return jnp.where((kpos >= lo) & (kpos <= hi), jnp.inf, NEG_BIG)

    cap_s[:, 0:HALF] = cap_of(kpos_lo, first[PIECE:TOK], pos_hi)
    cap_s[:, HALF:2 * HALF] = cap_of(kpos_hi, first[PIECE:TOK], pos_hi)
    cap_s[:, 2 * HALF:3 * HALF] = cap_of(kpos_lo, first[0:PIECE], pos_lo)

    for r in (1, 3, 5, 7):
        kv_in(r).wait_recv()

    k_scale = E ** -0.5
    exp_scale = k_scale * math.log2(math.e)
    plan = ((1, 2, 0), (0, 1, 2))

    def key_chunks(halves):
        return [(half, c) for half in range(halves) for c in range(HALF // CH)]

    for piece, halves, col0 in plan:
        n = halves * HALF
        base = col0 * HALF
        for half, c in key_chunks(halves):
            col = base + half * HALF + c * CH
            s_s[:, col:col + CH] = dot(q_s[piece], kv_s[0, half, c * CH:(c + 1) * CH, :], NT)
        rb = 16 if halves == 2 else 32
        for h in range(HEADS):
            for b in range(PIECE // rb):
                r0 = h * PIECE + b * rb
                s = jnp.minimum(s_s[r0:r0 + rb, base:base + n], cap_s[b * rb:(b + 1) * rb, base:base + n])
                m = jnp.max(s, axis=1, keepdims=True)
                e = jnp.exp2((s - m) * exp_scale)
                l = jnp.sum(e, axis=1, keepdims=True)
                p_s[r0:r0 + rb, base:base + n] = (e * (1.0 / l)).astype(BF16)
        o = jnp.zeros((ROWS, E), F32)
        for half in range(halves):
            o = o + dot(p_s[:, base + half * HALF:base + (half + 1) * HALF], kv_s[1, half])
        o_bf = o.astype(BF16)
        delta_s[piece] = jnp.sum(do_s[piece].astype(F32) * o_bf.astype(F32), axis=1, keepdims=True)
        for h in range(HEADS):
            o_s[piece * PIECE:(piece + 1) * PIECE, h * E:(h + 1) * E] = o_bf[h * PIECE:(h + 1) * PIECE]
        for half, c in key_chunks(halves):
            col = base + half * HALF + c * CH
            dst = half * HALF + c * CH
            val = dot(dot_s[piece], p_s[:, col:col + CH])
            if piece == 0:
                val = val + accv_t[:, dst:dst + CH]
            accv_t[:, dst:dst + CH] = val

    def blk(t, owner):
        return acc_s.at[t, :, pl.ds(pl.multiple_of(owner * PIECE, 32), PIECE), :]

    def d2d(t, g):
        return rcopy(blk(t, dev(2 * g + 1)), rb1.at[t, g], d2d_send.at[t, g], d2d_recv.at[t, g], 1)

    def rs(t, g):
        return rcopy(comb.at[t, g], rb2.at[t, g], rs_send.at[t, g], rs_recv.at[t, g], 2 * g)

    def start_d2d(t, acc_t):
        for half in range(2):
            for c in range(HALF // CH):
                col = half * HALF + c * CH
                acc_s[t, half, c * CH:(c + 1) * CH, :] = acc_t[:, col:col + CH].T
        for g in (1, 2, 3, 0):
            d2d(t, g).start()

    def combine(t):
        for g in (1, 2, 3, 0):
            d2d(t, g).wait_recv()
            comb[t, g] = acc_s[t, :, pl.ds(pl.multiple_of(dev(2 * g) * PIECE, 32), PIECE), :] + rb1[t, g]
            if g:
                rs(t, g).start()

    start_d2d(1, accv_t)

    dq_parts = {}
    for piece, halves, col0 in plan:
        base = col0 * HALF
        for half, c in key_chunks(halves):
            col = base + half * HALF + c * CH
            dst = half * HALF + c * CH
            dp_s[...] = dot(do_s[piece], kv_s[1, half, c * CH:(c + 1) * CH, :], NT)
            for h in range(HEADS):
                r0 = h * PIECE
                ds_s[r0:r0 + PIECE, col:col + CH] = (
                    p_s[r0:r0 + PIECE, col:col + CH].astype(F32)
                    * (dp_s[r0:r0 + PIECE, :] - delta_s[piece, r0:r0 + PIECE, :])).astype(BF16)
            val = dot(qt_s[piece], ds_s[:, col:col + CH])
            if piece == 0:
                val = val + acck_t[:, dst:dst + CH]
            acck_t[:, dst:dst + CH] = val
        if piece == 1:
            combine(1)
        dq = jnp.zeros((ROWS, E), F32)
        for half in range(halves):
            dq = dq + dot(ds_s[:, base + half * HALF:base + (half + 1) * HALF], kv_s[0, half])
        dq_bf = (dq * k_scale).astype(BF16)
        for h in range(HEADS):
            dq_s[piece * PIECE:(piece + 1) * PIECE, h * E:(h + 1) * E] = dq_bf[h * PIECE:(h + 1) * PIECE]

    start_d2d(0, acck_t)

    NY = 512
    y_out = []
    for i in range(D // NY):
        if i == 2:
            combine(0)
        y_s[:, i * NY:(i + 1) * NY] = dot(o_s[...], wo_s[:, i * NY:(i + 1) * NY]).astype(BF16)
        cp = pltpu.make_async_copy(y_s.at[:, i * NY:(i + 1) * NY], y_hbm.at[:, i * NY:(i + 1) * NY], out_sem.at[0, i])
        cp.start()
        y_out.append(cp)
    for i in range(D // NY):
        dx_s[:, i * NY:(i + 1) * NY] = dot(dq_s[...], wq_s[i * NY:(i + 1) * NY, :], NT)

    dkv = []
    for t in range(2):
        for g in (1, 2, 3):
            rs(t, g).wait_recv()
        tot = (comb[t, 0] + rb2[t, 1]) + (rb2[t, 2] + rb2[t, 3])
        if t == 0:
            tot = tot * k_scale
        dkv.append(tot.reshape(TOK, E).astype(BF16))
    dkv = jnp.concatenate(dkv, axis=1)
    dx_out = []
    for i in range(D // NY):
        val = dx_s[:, i * NY:(i + 1) * NY] + dot(dkv, wkv_s[i * NY:(i + 1) * NY, :], NT)
        dxo_s[:, i * NY:(i + 1) * NY] = val.astype(BF16)
        cp = pltpu.make_async_copy(dxo_s.at[:, i * NY:(i + 1) * NY], dx_hbm.at[:, i * NY:(i + 1) * NY],
                                   out_sem.at[1, i])
        cp.start()
        dx_out.append(cp)

    for c in y_out + dx_out:
        c.wait()
    for r in range(1, NDEV):
        kv_out[r].wait_send()
        doc_out[r].wait_send()
    for t in range(2):
        for g in range(4):
            d2d(t, g).wait_send()
            if g:
                rs(t, g).wait_send()


def solution(mesh):
    row_spec = P(('dp', 'cp'))
    full_spec = P()
    any_spec = pl.BlockSpec(memory_space=pl.ANY)
    vmem_spec = pl.BlockSpec(memory_space=pltpu.VMEM)

    def local_layer(x_in, dy_in, doc_id, w_q, w_k, w_v, w_o):
        V = pltpu.VMEM
        dma = pltpu.SemaphoreType.DMA
        return pl.pallas_call(
            kernel,
            out_shape=(jax.ShapeDtypeStruct((TOK, D), BF16), jax.ShapeDtypeStruct((TOK, D), BF16)),
            in_specs=[any_spec, any_spec, vmem_spec, any_spec, any_spec, any_spec, any_spec],
            out_specs=(any_spec, any_spec),
            scratch_shapes=[
                V((TOK, D), BF16), V((TOK, D), BF16), V((D, HE), BF16), V((D, 2 * E), BF16), V((HE, D), BF16),
                V((2, 2, HALF, E), BF16), V((NDEV, 1, TOK), jnp.int32),
                V((2, ROWS, E), BF16), V((2, ROWS, E), BF16), V((2, E, ROWS), BF16), V((2, E, ROWS), BF16),
                V((PIECE, 3 * HALF), F32),
                V((ROWS, 3 * HALF), F32), V((ROWS, 3 * HALF), BF16), V((ROWS, CH), F32), V((ROWS, 3 * HALF), BF16),
                V((TOK, HE), BF16), V((TOK, HE), BF16), V((2, ROWS, 1), F32),
                V((E, 2 * HALF), F32), V((E, 2 * HALF), F32), V((2, 2, HALF, E), F32),
                V((2, 4, 2, PIECE, E), F32), V((2, 4, 2, PIECE, E), F32), V((2, 4, 2, PIECE, E), F32),
                V((TOK, D), BF16), V((TOK, D), F32), V((TOK, D), BF16),
                dma((4,)), dma((HEADS,)), dma((HEADS,)), dma((2, 7)),
                dma((NDEV,)), dma((NDEV,)), dma((NDEV,)), dma((NDEV,)),
                dma((2, 4)), dma((2, 4)), dma((2, 4)), dma((2, 4)),
            ],
            compiler_params=pltpu.CompilerParams(collective_id=0, has_side_effects=True,
                                                 vmem_limit_bytes=62 * 1024 * 1024),
        )(x_in, dy_in, doc_id.reshape(1, TOK), jnp.transpose(w_q, (1, 0, 2)), w_k.reshape(D, E), w_v.reshape(D, E),
          w_o.reshape(HE, D))

    return jax.shard_map(local_layer, mesh=mesh,
                         in_specs=(row_spec, row_spec, row_spec, full_spec, full_spec, full_spec, full_spec),
                         out_specs=(row_spec, row_spec), check_vma=False)
```

```python
import math

import jax
import jax.numpy as jnp
from jax import lax
from jax.experimental import pallas as pl
from jax.experimental.pallas import tpu as pltpu
from jax.sharding import PartitionSpec as P

NEG_BIG = -1.0e30
F32 = jnp.float32
BF16 = jnp.bfloat16

NDEV = 8
HEADS = 7
E = 128
PIECE = 96
TOK = 192
D = 3584
HE = HEADS * E
ROWS = HEADS * PIECE
HALF = NDEV * PIECE
SEQ = 2 * HALF
KSPLIT = 2

NT = (((1,), (1,)), ((), ()))
NN = (((1,), (0,)), ((), ()))
UNITS = ((1, 1), (1, 0), (0, 1), (0, 0))
GROUPS = ((0, 4), (4, 7))


def dot(a, b, dims=NN):
    return lax.dot_general(a, b, dims, preferred_element_type=F32)


def main_kernel(x_hbm, dy_hbm, doc_ref, wq_hbm, wk_hbm, wv_hbm, wo_hbm,
                y_s, dx_s, dkv_s, wkv_s,
                x_s, dy_s, wq_s, wo_s,
                kv_s, doc_s, q_s, do_s, qt_s, dot_s, cap_s,
                s_s, p_s, dp_s, ds_s, o_s, dq_s, delta_s,
                acc_s, rb1, comb, rb2,
                in_sem, wq_sem, wo_sem, dy_sem,
                doc_send, doc_recv, kv_send, kv_recv,
                d2d_send, d2d_recv, rs_send, rs_recv):
    me = lax.axis_index('cp')
    core = lax.rem(me, 2)
    chip = me // 2
    cx = lax.rem(chip, 2)
    cy = chip // 2

    def dev(r):
        yy = lax.rem(cy + (r // 4), 2)
        xx = lax.rem(cx + ((r // 2) % 2), 2)
        cc = lax.rem(core + (r % 2), 2)
        return yy * 4 + xx * 2 + cc

    def rcopy(src, dst, ssem, rsem, r):
        return pltpu.make_async_remote_copy(src_ref=src, dst_ref=dst, send_sem=ssem, recv_sem=rsem,
                                            device_id={'cp': dev(r)}, device_id_type=pl.DeviceIdType.MESH)

    kd = D // KSPLIT
    ld_in = []
    for i in range(KSPLIT):
        ks = slice(i * kd, (i + 1) * kd)
        ld_in.append([pltpu.make_async_copy(x_hbm.at[:, ks], x_s.at[:, ks], in_sem.at[i, 0]),
                      pltpu.make_async_copy(wk_hbm.at[ks], wkv_s.at[ks, 0:E], in_sem.at[i, 1]),
                      pltpu.make_async_copy(wv_hbm.at[ks], wkv_s.at[ks, E:2 * E], in_sem.at[i, 2])])
    ld_dy = pltpu.make_async_copy(dy_hbm, dy_s, dy_sem)
    ld_wq = [pltpu.make_async_copy(wq_hbm.at[h], wq_s.at[:, h * E:(h + 1) * E], wq_sem.at[h]) for h in range(HEADS)]
    ld_wo = [pltpu.make_async_copy(wo_hbm.at[h * E:(h + 1) * E], wo_s.at[h * E:(h + 1) * E], wo_sem.at[h])
             for h in range(HEADS)]
    for part in ld_in:
        for c in part:
            c.start()

    barrier = pltpu.get_barrier_semaphore()
    for r in range(1, NDEV):
        pl.semaphore_signal(barrier, inc=1, device_id={'cp': dev(r)}, device_id_type=pl.DeviceIdType.MESH)

    kv_own = jnp.zeros((TOK, 2 * E), F32)
    for i in range(KSPLIT):
        for c in ld_in[i]:
            c.wait()
        if i == 0:
            for c in ld_wq[:4]:
                c.start()
        else:
            for c in ld_wq[4:]:
                c.start()
        kv_own = kv_own + dot(x_s[:, i * kd:(i + 1) * kd], wkv_s[i * kd:(i + 1) * kd, :])
    kv_own = kv_own.astype(BF16)
    my_off = pl.multiple_of(me * PIECE, 32)
    for t in range(2):
        for half in range(2):
            kv_s[t, half, pl.ds(my_off, PIECE), :] = kv_own[half * PIECE:(half + 1) * PIECE, t * E:(t + 1) * E]
    doc_s[me] = doc_ref[...]

    def kv_blk(t, owner):
        return kv_s.at[t, :, pl.ds(pl.multiple_of(owner * PIECE, 32), PIECE), :]

    pl.semaphore_wait(barrier, NDEV - 1)
    kv_out = {}
    for t in range(2):
        for r in (6, 2, 4, 1):
            kv_out[t, r] = rcopy(kv_blk(t, me), kv_blk(t, me), kv_send.at[t, r], kv_recv.at[t, r], r)
            kv_out[t, r].start()
        if t == 0:
            doc_out = {}
            for r in range(1, NDEV):
                doc_out[r] = rcopy(doc_ref, doc_s.at[me], doc_send.at[r], doc_recv.at[r], r)
                doc_out[r].start()

    def kv_in(t, r):
        return rcopy(kv_blk(t, dev(r)), kv_blk(t, dev(r)), kv_send.at[t, r], kv_recv.at[t, r], r)

    def forward(t, r):
        kv_in(t, r).wait_recv()
        kv_out[t, r + 1] = rcopy(kv_blk(t, dev(r)), kv_blk(t, dev(r)), kv_send.at[t, r + 1], kv_recv.at[t, r + 1], 1)
        kv_out[t, r + 1].start()

    def put_rows(dst, val, h):
        dst[0, h * PIECE:(h + 1) * PIECE, :] = val[0:PIECE]
        dst[1, h * PIECE:(h + 1) * PIECE, :] = val[PIECE:TOK]

    for h0, h1 in GROUPS:
        for h in range(h0, h1):
            ld_wq[h].wait()
        for c in ([ld_dy] + ld_wo[:4] if h0 == 0 else ld_wo[4:]):
            c.start()
        val = dot(x_s[...], wq_s[:, h0 * E:h1 * E]).astype(BF16)
        for h in range(h0, h1):
            put_rows(q_s, val[:, (h - h0) * E:(h - h0 + 1) * E], h)
    ld_dy.wait()
    for h0, h1 in GROUPS:
        for h in range(h0, h1):
            ld_wo[h].wait()
        val = dot(dy_s[...], wo_s[h0 * E:h1 * E, :], NT).astype(BF16)
        for h in range(h0, h1):
            put_rows(do_s, val[:, (h - h0) * E:(h - h0 + 1) * E], h)
    for r in (6, 2, 4):
        forward(0, r)

    for piece in range(2):
        qt_s[piece] = q_s[piece].T
        dot_s[piece] = do_s[piece].T

    for r in range(1, NDEV):
        rcopy(doc_ref, doc_s.at[dev(r)], doc_send.at[r], doc_recv.at[r], r).wait_recv()
    my_doc = doc_ref[...].astype(F32)
    eye = (lax.broadcasted_iota(jnp.int32, (TOK, TOK), 0) == lax.broadcasted_iota(jnp.int32, (TOK, TOK), 1))
    doc_col = jnp.sum(jnp.where(eye, jnp.broadcast_to(my_doc, (TOK, TOK)), 0.0), axis=1, keepdims=True)
    less = jnp.zeros((TOK, TOK), F32)
    for d in range(NDEV):
        less = less + jnp.where(doc_s[d].astype(F32) < doc_col, 1.0, 0.0)
    first = jnp.sum(less, axis=1, keepdims=True)
    rowi = lax.broadcasted_iota(jnp.int32, (PIECE, 1), 0)
    pos_lo = (me * PIECE + rowi).astype(F32)
    pos_hi = ((2 * NDEV - 1 - me) * PIECE + rowi).astype(F32)
    lane = lax.broadcasted_iota(jnp.int32, (1, HALF), 1).astype(F32)
    kpos_lo = lane
    kpos_hi = (2 * NDEV - 1) * PIECE + lane - 2 * PIECE * jnp.floor((lane + 0.5) * (1.0 / PIECE))

    def cap_of(kpos, lo, hi):
        return jnp.where((kpos >= lo) & (kpos <= hi), jnp.inf, NEG_BIG)

    cap_s[:, 0:HALF] = cap_of(kpos_lo, first[PIECE:TOK], pos_hi)
    cap_s[:, HALF:2 * HALF] = cap_of(kpos_hi, first[PIECE:TOK], pos_hi)
    cap_s[:, 2 * HALF:3 * HALF] = cap_of(kpos_lo, first[0:PIECE], pos_lo)

    for r in (1, 7, 3, 5):
        kv_in(0, r).wait_recv()

    k_scale = E ** -0.5
    exp_scale = k_scale * math.log2(math.e)
    plan = ((1, SEQ, 0), (0, HALF, SEQ))

    def spans(n, step=512):
        return [(h + a, h + min(a + step, HALF)) for h in range(0, n, HALF) for a in range(0, HALF, step)]

    def keys(t, a, b):
        return kv_s[t, a // HALF, a % HALF:a % HALF + (b - a), :]

    def over_keys(src, t, r0, r1, base, n):
        acc = dot(src[r0:r1, base:base + HALF], kv_s[t, 0])
        if n == SEQ:
            acc = acc + dot(src[r0:r1, base + HALF:base + SEQ], kv_s[t, 1])
        return acc

    def softmax(piece, n, base, h):
        rb = 16 if n == SEQ else 32
        for b in range(PIECE // rb):
            r0 = h * PIECE + b * rb
            s = jnp.minimum(s_s[r0:r0 + rb, base:base + n], cap_s[b * rb:(b + 1) * rb, base:base + n])
            m = jnp.max(s, axis=1, keepdims=True)
            e = jnp.exp2((s - m) * exp_scale)
            l = jnp.sum(e, axis=1, keepdims=True)
            p_s[r0:r0 + rb, base:base + n] = (e * (1.0 / l)).astype(BF16)

    def blk(t, half, owner):
        return acc_s.at[t, half, pl.ds(pl.multiple_of(owner * PIECE, 32), PIECE), :]

    def d2d(t, half, g):
        return rcopy(blk(t, half, dev(2 * g + 1)), rb1.at[t, half, g], d2d_send.at[t, half, g],
                     d2d_recv.at[t, half, g], 1)

    def rs(t, half, g):
        return rcopy(comb.at[t, half, g], rb2.at[t, half, g], rs_send.at[t, half, g], rs_recv.at[t, half, g], 2 * g)

    def start_d2d(t, half):
        for g in (3, 1, 2, 0):
            d2d(t, half, g).start()

    def combine(t, half):
        for g in (3, 1, 2, 0):
            d2d(t, half, g).wait_recv()
            comb[t, half, g] = acc_s[t, half, pl.ds(pl.multiple_of(dev(2 * g) * PIECE, 32), PIECE), :] + rb1[t, half, g]
            if g:
                rs(t, half, g).start()

    def grad(t, half, lhs_t, src):
        for a, b in spans(HALF, 256):
            val = dot(lhs_t[1], src[:, half * HALF + a:half * HALF + b])
            if half == 0:
                val = val + dot(lhs_t[0], src[:, SEQ + a:SEQ + b])
            acc_s[t, half, a:b, :] = val.T

    def s_part(piece, base, a, b):
        s_s[:, base + a:base + b] = dot(q_s[piece], keys(0, a, b), NT)

    def dp_part(piece, base, a, b):
        dp_s[:, base + a:base + b] = dot(do_s[piece], keys(1, a, b), NT)

    def o_part(piece, base, n, r0, r1):
        h0, h1 = r0 // PIECE, r1 // PIECE
        o_bf = over_keys(p_s, 1, r0, r1, base, n).astype(BF16)
        delta_s[piece, r0:r1, :] = jnp.sum(do_s[piece, r0:r1, :].astype(F32) * o_bf.astype(F32), axis=1, keepdims=True)
        for h in range(h0, h1):
            o_s[piece * PIECE:(piece + 1) * PIECE, h * E:(h + 1) * E] = o_bf[(h - h0) * PIECE:(h - h0 + 1) * PIECE]

    def ds_rows(piece, base, a, b):
        for h in range(HEADS):
            for c in range(PIECE // 32):
                r0 = h * PIECE + c * 32
                ds_s[r0:r0 + 32, base + a:base + b] = (
                    p_s[r0:r0 + 32, base + a:base + b].astype(F32)
                    * (dp_s[r0:r0 + 32, base + a:base + b] - delta_s[piece, r0:r0 + 32, :])).astype(BF16)

    def dq_part(piece, base, n):
        dq_bf = (over_keys(ds_s, 0, 0, ROWS, base, n) * k_scale).astype(BF16)
        for h in range(HEADS):
            dq_s[piece * PIECE:(piece + 1) * PIECE, h * E:(h + 1) * E] = dq_bf[h * PIECE:(h + 1) * PIECE]

    def softmax_with(piece, n, base, others):
        others = list(others)
        for h in range(HEADS):
            softmax(piece, n, base, h)
            left = HEADS - h
            take = -(-len(others) // left)
            for fn in others[:take]:
                fn()
            others = others[take:]

    for a, b in spans(SEQ):
        s_part(1, 0, a, b)
    for r in (6, 2, 4):
        forward(1, r)
    for r in (1, 7, 3, 5):
        kv_in(1, r).wait_recv()
    softmax_with(1, SEQ, 0, [lambda a=a, b=b: s_part(0, SEQ, a, b) for a, b in spans(HALF, 256)]
                 + [lambda a=a, b=b: dp_part(1, 0, a, b) for a, b in spans(SEQ, 256)])
    grad(1, 1, dot_s, p_s)
    start_d2d(1, 1)
    softmax_with(0, HALF, SEQ, [lambda: o_part(1, 0, SEQ, 0, 192), lambda: o_part(1, 0, SEQ, 192, 384),
                                lambda: o_part(1, 0, SEQ, 384, 672)]
                 + [lambda a=a, b=b: dp_part(0, SEQ, a, b) for a, b in spans(HALF, 256)])
    grad(1, 0, dot_s, p_s)
    start_d2d(1, 0)
    combine(1, 1)
    ds_rows(1, 0, HALF, SEQ)
    grad(0, 1, qt_s, ds_s)
    start_d2d(0, 1)
    o_part(0, SEQ, HALF, 0, ROWS)
    ds_rows(1, 0, 0, HALF)
    combine(1, 0)
    ds_rows(0, SEQ, 0, HALF)
    grad(0, 0, qt_s, ds_s)
    start_d2d(0, 0)
    combine(0, 1)
    for piece, n, base in plan:
        dq_part(piece, base, n)

    NY = 512

    def y_part(i):
        y_s[:, i * NY:(i + 1) * NY] = dot(o_s[...], wo_s[:, i * NY:(i + 1) * NY]).astype(BF16)

    for i in range(2):
        y_part(i)
    combine(0, 0)
    for i in range(2, D // NY):
        y_part(i)
    for i in range(D // NY):
        dx_s[:, i * NY:(i + 1) * NY] = dot(dq_s[...], wq_s[i * NY:(i + 1) * NY, :], NT)

    for t, half in UNITS:
        for g in (1, 2, 3):
            rs(t, half, g).wait_recv()
        tot = (comb[t, half, 0] + rb2[t, half, 1]) + (rb2[t, half, 2] + rb2[t, half, 3])
        if t == 0:
            tot = tot * k_scale
        dkv_s[half * PIECE:(half + 1) * PIECE, t * E:(t + 1) * E] = tot.astype(BF16)

    for r in range(1, NDEV):
        kv_out[0, r].wait_send()
        kv_out[1, r].wait_send()
        doc_out[r].wait_send()
    for t, half in UNITS:
        for g in range(4):
            d2d(t, half, g).wait_send()
            if g:
                rs(t, half, g).wait_send()


FIN = ((0, 1536), (1536, 2560), (2560, 3584))


def final_kernel(y_s, dx_s, dkv_s, wkv_s, y_hbm, dx_hbm, dxo_s, y_sem, dx_sem):
    y_cp = pltpu.make_async_copy(y_s, y_hbm, y_sem)
    y_cp.start()
    copies = [y_cp]
    for i, (a, b) in enumerate(FIN):
        dxo_s[:, a:b] = (dx_s[:, a:b] + dot(dkv_s[...], wkv_s[a:b, :], NT)).astype(BF16)
        cp = pltpu.make_async_copy(dxo_s.at[:, a:b], dx_hbm.at[:, a:b], dx_sem.at[i])
        cp.start()
        copies.append(cp)
    for cp in copies:
        cp.wait()


def solution(mesh):
    row_spec = P(('dp', 'cp'))
    full_spec = P()
    hbm_spec = pl.BlockSpec(memory_space=pltpu.HBM)
    vmem_spec = pl.BlockSpec(memory_space=pltpu.VMEM)

    def local_layer(x_in, dy_in, doc_id, w_q, w_k, w_v, w_o):
        V = pltpu.VMEM
        dma = pltpu.SemaphoreType.DMA
        sds = jax.ShapeDtypeStruct
        hbm = lambda a: pltpu.with_memory_space_constraint(a, pltpu.HBM)
        parts = pl.pallas_call(
            main_kernel,
            out_shape=(V((TOK, D), BF16), V((TOK, D), F32), V((TOK, 2 * E), BF16), V((D, 2 * E), BF16)),
            in_specs=[hbm_spec, hbm_spec, vmem_spec, hbm_spec, hbm_spec, hbm_spec, hbm_spec],
            out_specs=(vmem_spec,) * 4,
            scratch_shapes=[
                V((TOK, D), BF16), V((TOK, D), BF16), V((D, HE), BF16), V((HE, D), BF16),
                V((2, 2, HALF, E), BF16), V((NDEV, 1, TOK), jnp.int32),
                V((2, ROWS, E), BF16), V((2, ROWS, E), BF16), V((2, E, ROWS), BF16), V((2, E, ROWS), BF16),
                V((PIECE, 3 * HALF), F32),
                V((ROWS, 3 * HALF), F32), V((ROWS, 3 * HALF), BF16), V((ROWS, 3 * HALF), F32),
                V((ROWS, 3 * HALF), BF16),
                V((TOK, HE), BF16), V((TOK, HE), BF16), V((2, ROWS, 1), F32),
                V((2, 2, HALF, E), F32),
                V((2, 2, 4, PIECE, E), F32), V((2, 2, 4, PIECE, E), F32), V((2, 2, 4, PIECE, E), F32),
                dma((KSPLIT, 3)), dma((HEADS,)), dma((HEADS,)), dma,
                dma((NDEV,)), dma((NDEV,)), dma((2, NDEV)), dma((2, NDEV)),
                dma((2, 2, 4)), dma((2, 2, 4)), dma((2, 2, 4)), dma((2, 2, 4)),
            ],
            compiler_params=pltpu.CompilerParams(collective_id=0, has_side_effects=True,
                                                 vmem_limit_bytes=50 * 1024 * 1024),
        )(hbm(x_in), hbm(dy_in), doc_id.reshape(1, TOK), hbm(jnp.transpose(w_q, (1, 0, 2))), hbm(w_k.reshape(D, E)),
          hbm(w_v.reshape(D, E)), hbm(w_o.reshape(HE, D)))
        return pl.pallas_call(
            final_kernel,
            out_shape=(sds((TOK, D), BF16), sds((TOK, D), BF16)),
            in_specs=[vmem_spec] * 4,
            out_specs=(hbm_spec, hbm_spec),
            scratch_shapes=[V((TOK, D), BF16), dma, dma((len(FIN),))],
            compiler_params=pltpu.CompilerParams(vmem_limit_bytes=12 * 1024 * 1024),
        )(*[pltpu.with_memory_space_constraint(a, pltpu.VMEM) for a in parts])

    return jax.shard_map(local_layer, mesh=mesh,
                         in_specs=(row_spec, row_spec, row_spec, full_spec, full_spec, full_spec, full_spec),
                         out_specs=(row_spec, row_spec), check_vma=False)
```

```python
import math

import jax
import jax.numpy as jnp
from jax import lax
from jax.experimental import pallas as pl
from jax.experimental.pallas import tpu as pltpu
from jax.sharding import PartitionSpec as P

NEG_BIG = -1.0e30
F32 = jnp.float32
BF16 = jnp.bfloat16

NDEV = 8
HEADS = 7
E = 128
PIECE = 96
TOK = 192
D = 3584
HE = HEADS * E
ROWS = HEADS * PIECE
HALF = NDEV * PIECE
SEQ = 2 * HALF
KSPLIT = 2

NT = (((1,), (1,)), ((), ()))
NN = (((1,), (0,)), ((), ()))
UNITS = ((1, 1), (1, 0), (0, 1), (0, 0))
GROUPS = ((0, 4), (4, 7))


def dot(a, b, dims=NN):
    return lax.dot_general(a, b, dims, preferred_element_type=F32)


def side_by_side(ref, h0, h1, r0, r1):
    return jnp.concatenate([ref[h, r0:r1, :] for h in range(h0, h1)], axis=1)


def main_kernel(x_hbm, dy_hbm, doc_ref, wq_hbm, wk_hbm, wv_hbm, wo_hbm,
                y_s, dx_s, dkv_s, wkv_s,
                x_s, dy_s, wq_s, wo_s,
                kv_s, doc_s, q_s, do_s, qt_s, dot_s, cap_s,
                s_s, p_s, dp_s, ds_s, o_s, dq_s, delta_s,
                acc_s, rb1, comb, rb2,
                in_sem, wq_sem, wo_sem, dy_sem,
                doc_send, doc_recv, kv_send, kv_recv,
                d2d_send, d2d_recv, rs_send, rs_recv):
    me = lax.axis_index('cp')
    core = lax.rem(me, 2)
    chip = me // 2
    cx = lax.rem(chip, 2)
    cy = chip // 2

    def dev(r):
        yy = lax.rem(cy + (r // 4), 2)
        xx = lax.rem(cx + ((r // 2) % 2), 2)
        cc = lax.rem(core + (r % 2), 2)
        return yy * 4 + xx * 2 + cc

    def rcopy(src, dst, ssem, rsem, r):
        return pltpu.make_async_remote_copy(src_ref=src, dst_ref=dst, send_sem=ssem, recv_sem=rsem,
                                            device_id={'cp': dev(r)}, device_id_type=pl.DeviceIdType.MESH)

    kd = D // KSPLIT
    ld_in = []
    for i in range(KSPLIT):
        ks = slice(i * kd, (i + 1) * kd)
        ld_in.append([pltpu.make_async_copy(x_hbm.at[:, ks], x_s.at[:, ks], in_sem.at[i, 0]),
                      pltpu.make_async_copy(wk_hbm.at[ks], wkv_s.at[0, ks], in_sem.at[i, 1]),
                      pltpu.make_async_copy(wv_hbm.at[ks], wkv_s.at[1, ks], in_sem.at[i, 2])])
    ld_dy = pltpu.make_async_copy(dy_hbm, dy_s, dy_sem)
    ld_wq = [pltpu.make_async_copy(wq_hbm.at[h], wq_s.at[h], wq_sem.at[h]) for h in range(HEADS)]
    ld_wo = [pltpu.make_async_copy(wo_hbm.at[h * E:(h + 1) * E], wo_s.at[h * E:(h + 1) * E], wo_sem.at[h])
             for h in range(HEADS)]
    for part in ld_in + [ld_wq[:1]]:
        for c in part:
            c.start()
    LATER = (ld_wq[1:], [ld_dy] + ld_wo[:4])

    barrier = pltpu.get_barrier_semaphore()
    for r in range(1, NDEV):
        pl.semaphore_signal(barrier, inc=1, device_id={'cp': dev(r)}, device_id_type=pl.DeviceIdType.MESH)

    for i in range(KSPLIT):
        for c in ld_in[i]:
            c.wait()
        for c in LATER[i]:
            c.start()
        kv_part = dot(x_s[:, i * kd:(i + 1) * kd], side_by_side(wkv_s, 0, 2, i * kd, (i + 1) * kd))
        if i == 0:
            s_s[0:TOK, 0:2 * E] = kv_part
            pl.semaphore_wait(barrier, NDEV - 1)
            doc_s[me] = doc_ref[...]
            doc_out = {}
            for r in range(1, NDEV):
                doc_out[r] = rcopy(doc_ref, doc_s.at[me], doc_send.at[r], doc_recv.at[r], r)
                doc_out[r].start()
    kv_own = (s_s[0:TOK, 0:2 * E] + kv_part).astype(BF16)
    my_off = pl.multiple_of(me * PIECE, 32)
    for t in range(2):
        for half in range(2):
            kv_s[t, half, pl.ds(my_off, PIECE), :] = kv_own[half * PIECE:(half + 1) * PIECE, t * E:(t + 1) * E]

    def kv_blk(t, owner):
        return kv_s.at[t, :, pl.ds(pl.multiple_of(owner * PIECE, 32), PIECE), :]

    kv_out = {}
    for t in range(2):
        for r in (6, 2, 4, 1):
            kv_out[t, r] = rcopy(kv_blk(t, me), kv_blk(t, me), kv_send.at[t, r], kv_recv.at[t, r], r)
            kv_out[t, r].start()

    def kv_in(t, r):
        return rcopy(kv_blk(t, dev(r)), kv_blk(t, dev(r)), kv_send.at[t, r], kv_recv.at[t, r], r)

    def forward(t, r):
        kv_in(t, r).wait_recv()
        kv_out[t, r + 1] = rcopy(kv_blk(t, dev(r)), kv_blk(t, dev(r)), kv_send.at[t, r + 1], kv_recv.at[t, r + 1], 1)
        kv_out[t, r + 1].start()

    def put_rows(dst, val, h):
        dst[0, h * PIECE:(h + 1) * PIECE, :] = val[0:PIECE]
        dst[1, h * PIECE:(h + 1) * PIECE, :] = val[PIECE:TOK]

    for h0, h1 in GROUPS:
        for h in range(h0, h1):
            ld_wq[h].wait()
        for c in (ld_wo[4:] if h0 == 0 else []):
            c.start()
        val = dot(x_s[...], side_by_side(wq_s, h0, h1, 0, D)).astype(BF16)
        for h in range(h0, h1):
            put_rows(q_s, val[:, (h - h0) * E:(h - h0 + 1) * E], h)
    for r in range(1, NDEV):
        rcopy(doc_ref, doc_s.at[dev(r)], doc_send.at[r], doc_recv.at[r], r).wait_recv()
    my_doc = doc_ref[...].astype(F32)
    eye = (lax.broadcasted_iota(jnp.int32, (TOK, TOK), 0) == lax.broadcasted_iota(jnp.int32, (TOK, TOK), 1))
    doc_col = jnp.sum(jnp.where(eye, jnp.broadcast_to(my_doc, (TOK, TOK)), 0.0), axis=1, keepdims=True)
    less = jnp.zeros((TOK, TOK), F32)
    for d in range(NDEV):
        less = less + jnp.where(doc_s[d].astype(F32) < doc_col, 1.0, 0.0)
    first = jnp.sum(less, axis=1, keepdims=True)
    rowi = lax.broadcasted_iota(jnp.int32, (PIECE, 1), 0)
    pos_lo = (me * PIECE + rowi).astype(F32)
    pos_hi = ((2 * NDEV - 1 - me) * PIECE + rowi).astype(F32)
    lane = lax.broadcasted_iota(jnp.int32, (1, HALF), 1).astype(F32)
    kpos_lo = lane
    kpos_hi = (2 * NDEV - 1) * PIECE + lane - 2 * PIECE * jnp.floor((lane + 0.5) * (1.0 / PIECE))

    def cap_of(kpos, lo, hi):
        return jnp.where((kpos >= lo) & (kpos <= hi), jnp.inf, NEG_BIG)

    cap_s[:, 0:HALF] = cap_of(kpos_lo, first[PIECE:TOK], pos_hi)
    cap_s[:, HALF:2 * HALF] = cap_of(kpos_hi, first[PIECE:TOK], pos_hi)
    cap_s[:, 2 * HALF:3 * HALF] = cap_of(kpos_lo, first[0:PIECE], pos_lo)

    ld_dy.wait()
    for h0, h1 in GROUPS:
        for h in range(h0, h1):
            ld_wo[h].wait()
        val = dot(dy_s[...], wo_s[h0 * E:h1 * E, :], NT).astype(BF16)
        for h in range(h0, h1):
            put_rows(do_s, val[:, (h - h0) * E:(h - h0 + 1) * E], h)
    for r in (6, 2, 4):
        forward(0, r)

    for piece in range(2):
        qt_s[piece] = q_s[piece].T
        dot_s[piece] = do_s[piece].T

    for r in (1, 7, 3, 5):
        kv_in(0, r).wait_recv()

    k_scale = E ** -0.5
    exp_scale = k_scale * math.log2(math.e)
    plan = ((1, SEQ, 0), (0, HALF, SEQ))

    def spans(n, step=512):
        return [(h + a, h + min(a + step, HALF)) for h in range(0, n, HALF) for a in range(0, HALF, step)]

    def keys(t, a, b):
        return kv_s[t, a // HALF, a % HALF:a % HALF + (b - a), :]

    def over_keys(src, t, r0, r1, base, n):
        parts = []
        for a, b in ((r0, (r0 + r1) // 2), ((r0 + r1) // 2, r1)):
            acc = dot(src[a:b, base:base + HALF], kv_s[t, 0])
            if n == SEQ:
                acc = acc + dot(src[a:b, base + HALF:base + SEQ], kv_s[t, 1])
            parts.append(acc)
        return jnp.concatenate(parts, axis=0)

    def softmax(piece, n, base, h):
        rb = 16 if n == SEQ else 32
        for b in range(PIECE // rb):
            r0 = h * PIECE + b * rb
            s = jnp.minimum(s_s[r0:r0 + rb, base:base + n], cap_s[b * rb:(b + 1) * rb, base:base + n])
            m = jnp.max(s, axis=1, keepdims=True)
            e = jnp.exp2((s - m) * exp_scale)
            l = jnp.sum(e, axis=1, keepdims=True)
            p_s[r0:r0 + rb, base:base + n] = (e * (1.0 / l)).astype(BF16)

    def blk(t, half, owner):
        return acc_s.at[t, half, pl.ds(pl.multiple_of(owner * PIECE, 32), PIECE), :]

    def d2d(t, half, g):
        return rcopy(blk(t, half, dev(2 * g + 1)), rb1.at[t, half, g], d2d_send.at[t, half, g],
                     d2d_recv.at[t, half, g], 1)

    def rs(t, half, g):
        return rcopy(comb.at[t, half, g], rb2.at[t, half, g], rs_send.at[t, half, g], rs_recv.at[t, half, g], 2 * g)

    def start_d2d(t, half):
        for g in (3, 1, 2, 0):
            d2d(t, half, g).start()

    def combine(t, half):
        for g in (3, 1, 2, 0):
            d2d(t, half, g).wait_recv()
            comb[t, half, g] = acc_s[t, half, pl.ds(pl.multiple_of(dev(2 * g) * PIECE, 32), PIECE), :] + rb1[t, half, g]
            if g:
                rs(t, half, g).start()

    def grad(t, half, lhs_t, src):
        for a, b in spans(HALF, 256):
            val = dot(lhs_t[1], src[:, half * HALF + a:half * HALF + b])
            if half == 0:
                val = val + dot(lhs_t[0], src[:, SEQ + a:SEQ + b])
            acc_s[t, half, a:b, :] = val.T

    def s_part(piece, base, a, b):
        s_s[:, base + a:base + b] = dot(q_s[piece], keys(0, a, b), NT)

    def dp_part(piece, base, a, b):
        dp_s[:, base + a:base + b] = dot(do_s[piece], keys(1, a, b), NT)

    def o_part(piece, base, n, r0, r1):
        h0, h1 = r0 // PIECE, r1 // PIECE
        o_bf = over_keys(p_s, 1, r0, r1, base, n).astype(BF16)
        delta_s[piece, r0:r1, :] = jnp.sum(do_s[piece, r0:r1, :].astype(F32) * o_bf.astype(F32), axis=1, keepdims=True)
        for h in range(h0, h1):
            o_s[piece * PIECE:(piece + 1) * PIECE, h * E:(h + 1) * E] = o_bf[(h - h0) * PIECE:(h - h0 + 1) * PIECE]

    def ds_rows(piece, base, a, b):
        for h in range(HEADS):
            for c in range(PIECE // 32):
                r0 = h * PIECE + c * 32
                ds_s[r0:r0 + 32, base + a:base + b] = (
                    p_s[r0:r0 + 32, base + a:base + b].astype(F32)
                    * (dp_s[r0:r0 + 32, base + a:base + b] - delta_s[piece, r0:r0 + 32, :])).astype(BF16)

    def dq_part(piece, base, n):
        dq_bf = (over_keys(ds_s, 0, 0, ROWS, base, n) * k_scale).astype(BF16)
        for h in range(HEADS):
            dq_s[piece * PIECE:(piece + 1) * PIECE, h * E:(h + 1) * E] = dq_bf[h * PIECE:(h + 1) * PIECE]

    def softmax_with(piece, n, base, h0, h1, others):
        for h in range(h0, h1):
            softmax(piece, n, base, h)
            left = h1 - h
            take = -(-len(others) // left)
            for fn in others[:take]:
                fn()
            others = others[take:]

    for a, b in spans(SEQ):
        s_part(1, 0, a, b)
    softmax_with(1, SEQ, 0, 0, 4, [lambda a=a, b=b: s_part(0, SEQ, a, b) for a, b in spans(HALF, 256)])
    for r in (6, 2, 4):
        forward(1, r)
    softmax_with(1, SEQ, 0, 4, HEADS, [])
    grad(1, 1, dot_s, p_s)
    start_d2d(1, 1)
    for r in (1, 7, 3, 5):
        kv_in(1, r).wait_recv()
    softmax_with(0, HALF, SEQ, 0, HEADS, [lambda a=a, b=b: dp_part(1, 0, a, b) for a, b in spans(SEQ, 256)])
    combine(1, 1)
    grad(1, 0, dot_s, p_s)
    start_d2d(1, 0)
    o_part(1, 0, SEQ, 0, ROWS)
    ds_rows(1, 0, HALF, SEQ)
    for a, b in spans(HALF):
        dp_part(0, SEQ, a, b)
    grad(0, 1, qt_s, ds_s)
    start_d2d(0, 1)
    combine(1, 0)
    o_part(0, SEQ, HALF, 0, ROWS)
    ds_rows(1, 0, 0, HALF)
    ds_rows(0, SEQ, 0, HALF)
    grad(0, 0, qt_s, ds_s)
    start_d2d(0, 0)
    combine(0, 1)
    for piece, n, base in plan:
        dq_part(piece, base, n)

    NY = 896

    def y_part(i):
        y_s[:, i * NY:(i + 1) * NY] = dot(o_s[...], wo_s[:, i * NY:(i + 1) * NY]).astype(BF16)

    for i in range(2):
        y_part(i)
    combine(0, 0)
    for i in range(2, D // NY):
        y_part(i)
    for i in range(D // NY):
        dx_s[:, i * NY:(i + 1) * NY] = dot(dq_s[...], side_by_side(wq_s, 0, HEADS, i * NY, (i + 1) * NY), NT)

    for t, half in UNITS:
        for g in (1, 2, 3):
            rs(t, half, g).wait_recv()
        tot = (comb[t, half, 0] + rb2[t, half, 1]) + (rb2[t, half, 2] + rb2[t, half, 3])
        if t == 0:
            tot = tot * k_scale
        dkv_s[half * PIECE:(half + 1) * PIECE, t * E:(t + 1) * E] = tot.astype(BF16)

    for r in range(1, NDEV):
        kv_out[0, r].wait_send()
        kv_out[1, r].wait_send()
        doc_out[r].wait_send()
    for t, half in UNITS:
        for g in range(4):
            d2d(t, half, g).wait_send()
            if g:
                rs(t, half, g).wait_send()


FIN = ((0, 1536), (1536, 2560), (2560, 3584))


def final_kernel(y_s, dx_s, dkv_s, wkv_s, y_hbm, dx_hbm, dxo_s, y_sem, dx_sem):
    y_cp = pltpu.make_async_copy(y_s, y_hbm, y_sem)
    y_cp.start()
    copies = [y_cp]
    for i, (a, b) in enumerate(FIN):
        dxo_s[:, a:b] = (dx_s[:, a:b] + dot(dkv_s[...], side_by_side(wkv_s, 0, 2, a, b), NT)).astype(BF16)
        cp = pltpu.make_async_copy(dxo_s.at[:, a:b], dx_hbm.at[:, a:b], dx_sem.at[i])
        cp.start()
        copies.append(cp)
    for cp in copies:
        cp.wait()


def solution(mesh):
    row_spec = P(('dp', 'cp'))
    full_spec = P()
    hbm_spec = pl.BlockSpec(memory_space=pltpu.HBM)
    vmem_spec = pl.BlockSpec(memory_space=pltpu.VMEM)

    def local_layer(x_in, dy_in, doc_id, w_q, w_k, w_v, w_o):
        V = pltpu.VMEM
        dma = pltpu.SemaphoreType.DMA
        sds = jax.ShapeDtypeStruct
        hbm = lambda a: pltpu.with_memory_space_constraint(a, pltpu.HBM)
        parts = pl.pallas_call(
            main_kernel,
            out_shape=(V((TOK, D), BF16), V((TOK, D), F32), V((TOK, 2 * E), BF16), V((2, D, E), BF16)),
            in_specs=[hbm_spec, hbm_spec, vmem_spec, hbm_spec, hbm_spec, hbm_spec, hbm_spec],
            out_specs=(vmem_spec,) * 4,
            scratch_shapes=[
                V((TOK, D), BF16), V((TOK, D), BF16), V((HEADS, D, E), BF16), V((HE, D), BF16),
                V((2, 2, HALF, E), BF16), V((NDEV, 1, TOK), jnp.int32),
                V((2, ROWS, E), BF16), V((2, ROWS, E), BF16), V((2, E, ROWS), BF16), V((2, E, ROWS), BF16),
                V((PIECE, 3 * HALF), F32),
                V((ROWS, 3 * HALF), F32), V((ROWS, 3 * HALF), BF16), V((ROWS, 3 * HALF), F32),
                V((ROWS, 3 * HALF), BF16),
                V((TOK, HE), BF16), V((TOK, HE), BF16), V((2, ROWS, 1), F32),
                V((2, 2, HALF, E), F32),
                V((2, 2, 4, PIECE, E), F32), V((2, 2, 4, PIECE, E), F32), V((2, 2, 4, PIECE, E), F32),
                dma((KSPLIT, 3)), dma((HEADS,)), dma((HEADS,)), dma,
                dma((NDEV,)), dma((NDEV,)), dma((2, NDEV)), dma((2, NDEV)),
                dma((2, 2, 4)), dma((2, 2, 4)), dma((2, 2, 4)), dma((2, 2, 4)),
            ],
            compiler_params=pltpu.CompilerParams(collective_id=0, has_side_effects=True,
                                                 vmem_limit_bytes=50 * 1024 * 1024),
        )(hbm(x_in), hbm(dy_in), doc_id.reshape(1, TOK), hbm(jnp.transpose(w_q, (1, 0, 2))), hbm(w_k.reshape(D, E)),
          hbm(w_v.reshape(D, E)), hbm(w_o.reshape(HE, D)))
        return pl.pallas_call(
            final_kernel,
            out_shape=(sds((TOK, D), BF16), sds((TOK, D), BF16)),
            in_specs=[vmem_spec] * 4,
            out_specs=(hbm_spec, hbm_spec),
            scratch_shapes=[V((TOK, D), BF16), dma, dma((len(FIN),))],
            compiler_params=pltpu.CompilerParams(vmem_limit_bytes=12 * 1024 * 1024),
        )(*[pltpu.with_memory_space_constraint(a, pltpu.VMEM) for a in parts])

    return jax.shard_map(local_layer, mesh=mesh,
                         in_specs=(row_spec, row_spec, row_spec, full_spec, full_spec, full_spec, full_spec),
                         out_specs=(row_spec, row_spec), check_vma=False)
```

```python
import math

import jax
import jax.numpy as jnp
from jax import lax
from jax.experimental import pallas as pl
from jax.experimental.pallas import tpu as pltpu
from jax.sharding import PartitionSpec as P

NEG_BIG = -1.0e30
F32 = jnp.float32
BF16 = jnp.bfloat16

NDEV = 8
HEADS = 7
E = 128
PIECE = 96
TOK = 192
D = 3584
HE = HEADS * E
ROWS = HEADS * PIECE
HALF = NDEV * PIECE
SEQ = 2 * HALF
KPARTS = ((0, 1024), (1024, 2048), (2048, 3072), (3072, D))

NT = (((1,), (1,)), ((), ()))
NN = (((1,), (0,)), ((), ()))
UNITS = ((1, 1), (1, 0), (0, 1), (0, 0))
GROUPS = ((0, 4), (4, 7))


def dot(a, b, dims=NN):
    return lax.dot_general(a, b, dims, preferred_element_type=F32)


def side_by_side(ref, h0, h1, r0, r1):
    return jnp.concatenate([ref[h, r0:r1, :] for h in range(h0, h1)], axis=1)


def main_kernel(x_hbm, dy_hbm, doc_ref, wq_hbm, wk_hbm, wv_hbm, wo_hbm,
                y_s, dx_s, dkv_s, wkv_s,
                x_s, dy_s, wq_s, wo_s,
                kv_s, doc_s, q_s, do_s, qt_s, dot_s, cap_s,
                s_s, p_s, dp_s, ds_s, o_s, dq_s, delta_s,
                acc_s, rb1, comb, rb2, relay,
                in_sem, wq_sem, wo_sem, dy_sem,
                doc_send, doc_recv, kv_send, kv_recv,
                d2d_send, d2d_recv, rs_send, rs_recv):
    me = lax.axis_index('cp')
    core = lax.rem(me, 2)
    chip = me // 2
    cx = lax.rem(chip, 2)
    cy = chip // 2

    def dev(r):
        yy = lax.rem(cy + (r // 4), 2)
        xx = lax.rem(cx + ((r // 2) % 2), 2)
        cc = lax.rem(core + (r % 2), 2)
        return yy * 4 + xx * 2 + cc

    def rcopy(src, dst, ssem, rsem, r):
        return pltpu.make_async_remote_copy(src_ref=src, dst_ref=dst, send_sem=ssem, recv_sem=rsem,
                                            device_id={'cp': dev(r)}, device_id_type=pl.DeviceIdType.MESH)

    ld_in = []
    for i, (ka, kb) in enumerate(KPARTS):
        ks = slice(ka, kb)
        ld_in.append([pltpu.make_async_copy(x_hbm.at[:, ks], x_s.at[:, ks], in_sem.at[i, 0]),
                      pltpu.make_async_copy(wk_hbm.at[ks], wkv_s.at[0, ks], in_sem.at[i, 1]),
                      pltpu.make_async_copy(wv_hbm.at[ks], wkv_s.at[1, ks], in_sem.at[i, 2])])
    ld_dy = pltpu.make_async_copy(dy_hbm, dy_s, dy_sem)
    ld_wq = [pltpu.make_async_copy(wq_hbm.at[h], wq_s.at[h], wq_sem.at[h]) for h in range(HEADS)]
    ld_wo = [pltpu.make_async_copy(wo_hbm.at[h * E:(h + 1) * E], wo_s.at[h * E:(h + 1) * E], wo_sem.at[h])
             for h in range(HEADS)]
    for part in ld_in + [ld_wq[:1]]:
        for c in part:
            c.start()
    LATER = (ld_wq[1:3], ld_wq[3:4], ld_wq[4:], [])

    barrier = pltpu.get_barrier_semaphore()
    for r in range(1, NDEV):
        pl.semaphore_signal(barrier, inc=1, device_id={'cp': dev(r)}, device_id_type=pl.DeviceIdType.MESH)

    for i, (ka, kb) in enumerate(KPARTS):
        for c in ld_in[i]:
            c.wait()
        for c in LATER[i]:
            c.start()
        kv_part = dot(x_s[:, ka:kb], side_by_side(wkv_s, 0, 2, ka, kb))
        if i:
            kv_part = s_s[0:TOK, 0:2 * E] + kv_part
        if i < len(KPARTS) - 1:
            s_s[0:TOK, 0:2 * E] = kv_part
        if i == 1:
            pl.semaphore_wait(barrier, NDEV - 1)
            doc_s[me] = doc_ref[...]
            doc_out = {}
            for r in range(1, NDEV):
                doc_out[r] = rcopy(doc_ref, doc_s.at[me], doc_send.at[r], doc_recv.at[r], r)
                doc_out[r].start()
    kv_own = kv_part.astype(BF16)
    my_off = pl.multiple_of(me * PIECE, 32)
    for t in range(2):
        for half in range(2):
            kv_s[t, half, pl.ds(my_off, PIECE), :] = kv_own[half * PIECE:(half + 1) * PIECE, t * E:(t + 1) * E]

    def kv_blk(t, owner):
        return kv_s.at[t, :, pl.ds(pl.multiple_of(owner * PIECE, 32), PIECE), :]

    kv_out = {}
    for t in range(2):
        for r in (6, 2, 4, 1):
            kv_out[t, r] = rcopy(kv_blk(t, me), kv_blk(t, me), kv_send.at[t, r], kv_recv.at[t, r], r)
            kv_out[t, r].start()

    def kv_in(t, r):
        return rcopy(kv_blk(t, dev(r)), kv_blk(t, dev(r)), kv_send.at[t, r], kv_recv.at[t, r], r)

    def forward(t, r):
        kv_in(t, r).wait_recv()
        kv_out[t, r + 1] = rcopy(kv_blk(t, dev(r)), kv_blk(t, dev(r)), kv_send.at[t, r + 1], kv_recv.at[t, r + 1], 1)
        kv_out[t, r + 1].start()

    def put_rows(dst, val, h):
        dst[0, h * PIECE:(h + 1) * PIECE, :] = val[0:PIECE]
        dst[1, h * PIECE:(h + 1) * PIECE, :] = val[PIECE:TOK]

    for h0, h1 in GROUPS:
        for h in range(h0, h1):
            ld_wq[h].wait()
        for c in ([ld_dy] + ld_wo[:4] if h0 == 0 else ld_wo[4:]):
            c.start()
        val = dot(x_s[...], side_by_side(wq_s, h0, h1, 0, D)).astype(BF16)
        for h in range(h0, h1):
            put_rows(q_s, val[:, (h - h0) * E:(h - h0 + 1) * E], h)
    for r in range(1, NDEV):
        rcopy(doc_ref, doc_s.at[dev(r)], doc_send.at[r], doc_recv.at[r], r).wait_recv()
    ld_dy.wait()
    for h0, h1 in GROUPS:
        for h in range(h0, h1):
            ld_wo[h].wait()
        val = dot(dy_s[...], wo_s[h0 * E:h1 * E, :], NT).astype(BF16)
        for h in range(h0, h1):
            put_rows(do_s, val[:, (h - h0) * E:(h - h0 + 1) * E], h)
        if h0 == 0:
            my_doc = doc_ref[...].astype(F32)
            eye = (lax.broadcasted_iota(jnp.int32, (TOK, TOK), 0) == lax.broadcasted_iota(jnp.int32, (TOK, TOK), 1))
            doc_col = jnp.sum(jnp.where(eye, jnp.broadcast_to(my_doc, (TOK, TOK)), 0.0), axis=1, keepdims=True)
            less = jnp.zeros((TOK, TOK), F32)
            for d in range(NDEV):
                less = less + jnp.where(doc_s[d].astype(F32) < doc_col, 1.0, 0.0)
            first = jnp.sum(less, axis=1, keepdims=True)
            rowi = lax.broadcasted_iota(jnp.int32, (PIECE, 1), 0)
            pos_lo = (me * PIECE + rowi).astype(F32)
            pos_hi = ((2 * NDEV - 1 - me) * PIECE + rowi).astype(F32)
            lane = lax.broadcasted_iota(jnp.int32, (1, HALF), 1).astype(F32)
            kpos_lo = lane
            kpos_hi = (2 * NDEV - 1) * PIECE + lane - 2 * PIECE * jnp.floor((lane + 0.5) * (1.0 / PIECE))

            def cap_of(kpos, lo, hi):
                return jnp.where((kpos >= lo) & (kpos <= hi), jnp.inf, NEG_BIG)

            cap_s[:, 0:HALF] = cap_of(kpos_lo, first[PIECE:TOK], pos_hi)
            cap_s[:, HALF:2 * HALF] = cap_of(kpos_hi, first[PIECE:TOK], pos_hi)
            cap_s[:, 2 * HALF:3 * HALF] = cap_of(kpos_lo, first[0:PIECE], pos_lo)
            for r in (6, 2, 4):
                forward(0, r)
        else:
            for piece in range(2):
                qt_s[piece] = q_s[piece].T

    for r in (1, 7, 3, 5):
        kv_in(0, r).wait_recv()

    k_scale = E ** -0.5
    exp_scale = k_scale * math.log2(math.e)
    plan = ((1, SEQ, 0), (0, HALF, SEQ))

    def spans(n, step=512):
        return [(h + a, h + min(a + step, HALF)) for h in range(0, n, HALF) for a in range(0, HALF, step)]

    def keys(t, a, b):
        return kv_s[t, a // HALF, a % HALF:a % HALF + (b - a), :]

    def over_keys(src, t, r0, r1, base, n):
        parts = []
        for a, b in ((r0, (r0 + r1) // 2), ((r0 + r1) // 2, r1)):
            acc = dot(src[a:b, base:base + HALF], kv_s[t, 0])
            if n == SEQ:
                acc = acc + dot(src[a:b, base + HALF:base + SEQ], kv_s[t, 1])
            parts.append(acc)
        return jnp.concatenate(parts, axis=0)

    def softmax(piece, n, base, h):
        rb = 16 if n == SEQ else 32
        for b in range(PIECE // rb):
            r0 = h * PIECE + b * rb
            s = jnp.minimum(s_s[r0:r0 + rb, base:base + n], cap_s[b * rb:(b + 1) * rb, base:base + n])
            m = jnp.max(s, axis=1, keepdims=True)
            e = jnp.exp2((s - m) * exp_scale)
            l = jnp.sum(e, axis=1, keepdims=True)
            p_s[r0:r0 + rb, base:base + n] = (e * (1.0 / l)).astype(BF16)

    def blk(t, half, owner):
        return acc_s.at[t, half, pl.ds(pl.multiple_of(owner * PIECE, 32), PIECE), :]

    def d2d(t, half, g):
        return rcopy(blk(t, half, dev(2 * g + 1)), rb1.at[t, half, g], d2d_send.at[t, half, g],
                     d2d_recv.at[t, half, g], 1)

    def rs(t, half, g):
        return rcopy(comb.at[t, half, g], rb2.at[t, half, g], rs_send.at[t, half, g], rs_recv.at[t, half, g], 2 * g)

    def start_d2d(t, half):
        for g in (3, 1, 2, 0):
            d2d(t, half, g).start()

    def add_peer(t, half, g):
        d2d(t, half, g).wait_recv()
        comb[t, half, g] = (acc_s[t, half, pl.ds(pl.multiple_of(dev(2 * g) * PIECE, 32), PIECE), :]
                            + rb1[t, half, g])

    def combine_direct(t, half):
        for g in (3, 1, 2, 0):
            add_peer(t, half, g)
            if g:
                rs(t, half, g).start()

    first_dev = lax.rem(cy + core, 2) * 4 + lax.rem(cx + 1 - core, 2) * 2 + core
    second_dev = lax.rem(cy + 1 - core, 2) * 4 + lax.rem(cx + core, 2) * 2 + core
    first_g, second_g = 1 + core, 2 - core

    def to_first(t, half, i):
        if i == 0:
            src, dst = comb.at[t, half, 3], relay.at[t, half]
        else:
            src, dst = comb.at[t, half, first_g], rb2.at[t, half, 1]
        return pltpu.make_async_remote_copy(
            src_ref=src, dst_ref=dst, send_sem=rs_send.at[t, half, i], recv_sem=rs_recv.at[t, half, i],
            device_id={'cp': first_dev}, device_id_type=pl.DeviceIdType.MESH)

    def to_second(t, half):
        return pltpu.make_async_remote_copy(
            src_ref=comb.at[t, half, second_g], dst_ref=rb2.at[t, half, 2], send_sem=rs_send.at[t, half, 2],
            recv_sem=rs_recv.at[t, half, 2], device_id={'cp': second_dev}, device_id_type=pl.DeviceIdType.MESH)

    def combine_relayed(t, half):
        add_peer(t, half, 3)
        to_first(t, half, 0).start()
        add_peer(t, half, 1)
        add_peer(t, half, 2)
        to_first(t, half, 1).start()
        add_peer(t, half, 0)

    def pass_on(t, half):
        to_first(t, half, 0).wait_recv()
        comb[t, half, second_g] = comb[t, half, second_g] + relay[t, half]
        to_second(t, half).start()

    def grad(t, half, lhs_t, src):
        for a, b in spans(HALF, 256):
            val = dot(lhs_t[1], src[:, half * HALF + a:half * HALF + b])
            if half == 0:
                val = val + dot(lhs_t[0], src[:, SEQ + a:SEQ + b])
            acc_s[t, half, a:b, :] = val.T

    def s_part(piece, base, a, b):
        s_s[:, base + a:base + b] = dot(q_s[piece], keys(0, a, b), NT)

    def dp_part(piece, base, a, b):
        dp_s[:, base + a:base + b] = dot(do_s[piece], keys(1, a, b), NT)

    def o_part(piece, base, n, r0, r1):
        h0, h1 = r0 // PIECE, r1 // PIECE
        o_bf = over_keys(p_s, 1, r0, r1, base, n).astype(BF16)
        delta_s[piece, r0:r1, :] = jnp.sum(do_s[piece, r0:r1, :].astype(F32) * o_bf.astype(F32), axis=1, keepdims=True)
        for h in range(h0, h1):
            o_s[piece * PIECE:(piece + 1) * PIECE, h * E:(h + 1) * E] = o_bf[(h - h0) * PIECE:(h - h0 + 1) * PIECE]

    def ds_rows(piece, base, a, b):
        for h in range(HEADS):
            for c in range(PIECE // 32):
                r0 = h * PIECE + c * 32
                ds_s[r0:r0 + 32, base + a:base + b] = (
                    p_s[r0:r0 + 32, base + a:base + b].astype(F32)
                    * (dp_s[r0:r0 + 32, base + a:base + b] - delta_s[piece, r0:r0 + 32, :])).astype(BF16)

    def dq_part(piece, base, n):
        dq_bf = (over_keys(ds_s, 0, 0, ROWS, base, n) * k_scale).astype(BF16)
        for h in range(HEADS):
            dq_s[piece * PIECE:(piece + 1) * PIECE, h * E:(h + 1) * E] = dq_bf[h * PIECE:(h + 1) * PIECE]

    def softmax_with(piece, n, base, h0, h1, others):
        for h in range(h0, h1):
            softmax(piece, n, base, h)
            left = h1 - h
            take = -(-len(others) // left)
            for fn in others[:take]:
                fn()
            others = others[take:]

    for a, b in spans(SEQ):
        s_part(1, 0, a, b)
    for piece in range(2):
        dot_s[piece] = do_s[piece].T
    softmax_with(1, SEQ, 0, 0, 4, [lambda a=a, b=b: s_part(0, SEQ, a, b) for a, b in spans(HALF, 256)])
    for r in (6, 2, 4):
        forward(1, r)
    softmax_with(1, SEQ, 0, 4, HEADS, [])
    grad(1, 1, dot_s, p_s)
    start_d2d(1, 1)
    for r in (1, 7, 3, 5):
        kv_in(1, r).wait_recv()
    softmax_with(0, HALF, SEQ, 0, HEADS, [lambda a=a, b=b: dp_part(1, 0, a, b) for a, b in spans(SEQ, 256)])
    combine_relayed(1, 1)
    grad(1, 0, dot_s, p_s)
    start_d2d(1, 0)
    o_part(1, 0, SEQ, 0, ROWS)
    ds_rows(1, 0, HALF, SEQ)
    for a, b in spans(HALF):
        dp_part(0, SEQ, a, b)
    grad(0, 1, qt_s, ds_s)
    start_d2d(0, 1)
    combine_relayed(1, 0)
    o_part(0, SEQ, HALF, 0, ROWS)
    ds_rows(1, 0, 0, HALF)
    ds_rows(0, SEQ, 0, HALF)
    grad(0, 0, qt_s, ds_s)
    start_d2d(0, 0)
    pass_on(1, 1)
    combine_relayed(0, 1)
    for piece, n, base in plan:
        dq_part(piece, base, n)

    combine_direct(0, 0)
    NY = 896

    def y_part(a, b):
        y_s[:, a:b] = dot(o_s[...], wo_s[:, a:b]).astype(BF16)

    y_part(0, 1792)
    pass_on(1, 0)
    y_part(1792, D)
    pass_on(0, 1)
    for i in range(D // NY):
        dx_s[:, i * NY:(i + 1) * NY] = dot(dq_s[...], side_by_side(wq_s, 0, HEADS, i * NY, (i + 1) * NY), NT)

    def put_total(t, half, tot):
        if t == 0:
            tot = tot * k_scale
        dkv_s[half * PIECE:(half + 1) * PIECE, t * E:(t + 1) * E] = tot.astype(BF16)

    for t, half in UNITS[:3]:
        to_first(t, half, 1).wait_recv()
        to_second(t, half).wait_recv()
        put_total(t, half, comb[t, half, 0] + (rb2[t, half, 1] + rb2[t, half, 2]))
    for g in (3, 1, 2):
        rs(0, 0, g).wait_recv()
    put_total(0, 0, (comb[0, 0, 0] + rb2[0, 0, 1]) + (rb2[0, 0, 2] + rb2[0, 0, 3]))

    for r in range(1, NDEV):
        kv_out[0, r].wait_send()
        kv_out[1, r].wait_send()
        doc_out[r].wait_send()
    for t, half in UNITS:
        for g in range(4):
            d2d(t, half, g).wait_send()
    for t, half in UNITS[:3]:
        to_first(t, half, 0).wait_send()
        to_first(t, half, 1).wait_send()
        to_second(t, half).wait_send()
    for g in (1, 2, 3):
        rs(0, 0, g).wait_send()


FIN = ((0, 1536), (1536, 2560), (2560, 3584))


def final_kernel(y_s, dx_s, dkv_s, wkv_s, y_hbm, dx_hbm, dxo_s, y_sem, dx_sem):
    y_cp = pltpu.make_async_copy(y_s, y_hbm, y_sem)
    y_cp.start()
    copies = [y_cp]
    for i, (a, b) in enumerate(FIN):
        dxo_s[:, a:b] = (dx_s[:, a:b] + dot(dkv_s[...], side_by_side(wkv_s, 0, 2, a, b), NT)).astype(BF16)
        cp = pltpu.make_async_copy(dxo_s.at[:, a:b], dx_hbm.at[:, a:b], dx_sem.at[i])
        cp.start()
        copies.append(cp)
    for cp in copies:
        cp.wait()


def solution(mesh):
    row_spec = P(('dp', 'cp'))
    full_spec = P()
    hbm_spec = pl.BlockSpec(memory_space=pltpu.HBM)
    vmem_spec = pl.BlockSpec(memory_space=pltpu.VMEM)

    def local_layer(x_in, dy_in, doc_id, w_q, w_k, w_v, w_o):
        V = pltpu.VMEM
        dma = pltpu.SemaphoreType.DMA
        sds = jax.ShapeDtypeStruct
        hbm = lambda a: pltpu.with_memory_space_constraint(a, pltpu.HBM)
        parts = pl.pallas_call(
            main_kernel,
            out_shape=(V((TOK, D), BF16), V((TOK, D), F32), V((TOK, 2 * E), BF16), V((2, D, E), BF16)),
            in_specs=[hbm_spec, hbm_spec, vmem_spec, hbm_spec, hbm_spec, hbm_spec, hbm_spec],
            out_specs=(vmem_spec,) * 4,
            scratch_shapes=[
                V((TOK, D), BF16), V((TOK, D), BF16), V((HEADS, D, E), BF16), V((HE, D), BF16),
                V((2, 2, HALF, E), BF16), V((NDEV, 1, TOK), jnp.int32),
                V((2, ROWS, E), BF16), V((2, ROWS, E), BF16), V((2, E, ROWS), BF16), V((2, E, ROWS), BF16),
                V((PIECE, 3 * HALF), F32),
                V((ROWS, 3 * HALF), F32), V((ROWS, 3 * HALF), BF16), V((ROWS, 3 * HALF), F32),
                V((ROWS, 3 * HALF), BF16),
                V((TOK, HE), BF16), V((TOK, HE), BF16), V((2, ROWS, 1), F32),
                V((2, 2, HALF, E), F32),
                V((2, 2, 4, PIECE, E), F32), V((2, 2, 4, PIECE, E), F32), V((2, 2, 4, PIECE, E), F32), V((2, 2, PIECE, E), F32),
                dma((len(KPARTS), 3)), dma((HEADS,)), dma((HEADS,)), dma,
                dma((NDEV,)), dma((NDEV,)), dma((2, NDEV)), dma((2, NDEV)),
                dma((2, 2, 4)), dma((2, 2, 4)), dma((2, 2, 4)), dma((2, 2, 4)),
            ],
            compiler_params=pltpu.CompilerParams(collective_id=0, has_side_effects=True,
                                                 vmem_limit_bytes=50 * 1024 * 1024),
        )(hbm(x_in), hbm(dy_in), doc_id.reshape(1, TOK), hbm(jnp.transpose(w_q, (1, 0, 2))), hbm(w_k.reshape(D, E)),
          hbm(w_v.reshape(D, E)), hbm(w_o.reshape(HE, D)))
        return pl.pallas_call(
            final_kernel,
            out_shape=(sds((TOK, D), BF16), sds((TOK, D), BF16)),
            in_specs=[vmem_spec] * 4,
            out_specs=(hbm_spec, hbm_spec),
            scratch_shapes=[V((TOK, D), BF16), dma, dma((len(FIN),))],
            compiler_params=pltpu.CompilerParams(vmem_limit_bytes=12 * 1024 * 1024),
        )(*[pltpu.with_memory_space_constraint(a, pltpu.VMEM) for a in parts])

    return jax.shard_map(local_layer, mesh=mesh,
                         in_specs=(row_spec, row_spec, row_spec, full_spec, full_spec, full_spec, full_spec),
                         out_specs=(row_spec, row_spec), check_vma=False)
```

```python
import math

import jax
import jax.numpy as jnp
from jax import lax
from jax.experimental import pallas as pl
from jax.experimental.pallas import tpu as pltpu
from jax.sharding import PartitionSpec as P

NEG_BIG = -1.0e30
F32 = jnp.float32
BF16 = jnp.bfloat16

NDEV = 8
HEADS = 7
E = 128
PIECE = 96
TOK = 192
D = 3584
HE = HEADS * E
ROWS = HEADS * PIECE
HALF = NDEV * PIECE
SEQ = 2 * HALF
KPARTS = ((0, 1024), (1024, 2048), (2048, 3072), (3072, D))

NT = (((1,), (1,)), ((), ()))
NN = (((1,), (0,)), ((), ()))
UNITS = ((1, 1), (1, 0), (0, 1), (0, 0))
GROUPS = ((0, 4), (4, 7))


def dot(a, b, dims=NN):
    return lax.dot_general(a, b, dims, preferred_element_type=F32)


def side_by_side(ref, h0, h1, r0, r1):
    return jnp.concatenate([ref[h, r0:r1, :] for h in range(h0, h1)], axis=1)


def main_kernel(x_hbm, dy_hbm, doc_ref, wq_hbm, wk_hbm, wv_hbm, wo_hbm,
                y_s, dx_s, dkv_s, wkv_s,
                x_s, dy_s, wq_s, wo_s,
                kv_s, doc_s, q_s, do_s, qt_s, dot_s, cap_s,
                s_s, p_s, dp_s, ds_s, o_s, dq_s, delta_s,
                acc_s, rb1, comb, rb2, relay,
                in_sem, wq_sem, wo_sem, dy_sem,
                doc_send, doc_recv, kv_send, kv_recv, kv_pass,
                d2d_send, d2d_recv, rs_send, rs_recv):
    me = lax.axis_index('cp')
    core = lax.rem(me, 2)
    chip = me // 2
    cx = lax.rem(chip, 2)
    cy = chip // 2

    def dev(r):
        yy = lax.rem(cy + (r // 4), 2)
        xx = lax.rem(cx + ((r // 2) % 2), 2)
        cc = lax.rem(core + (r % 2), 2)
        return yy * 4 + xx * 2 + cc

    def rcopy(src, dst, ssem, rsem, r):
        return pltpu.make_async_remote_copy(src_ref=src, dst_ref=dst, send_sem=ssem, recv_sem=rsem,
                                            device_id={'cp': dev(r)}, device_id_type=pl.DeviceIdType.MESH)

    ld_in = []
    for i, (ka, kb) in enumerate(KPARTS):
        ks = slice(ka, kb)
        ld_in.append([pltpu.make_async_copy(x_hbm.at[:, ks], x_s.at[:, ks], in_sem.at[i, 0]),
                      pltpu.make_async_copy(wk_hbm.at[ks], wkv_s.at[0, ks], in_sem.at[i, 1]),
                      pltpu.make_async_copy(wv_hbm.at[ks], wkv_s.at[1, ks], in_sem.at[i, 2])])
    ld_dy = pltpu.make_async_copy(dy_hbm, dy_s, dy_sem)
    ld_wq = [pltpu.make_async_copy(wq_hbm.at[h], wq_s.at[h], wq_sem.at[h]) for h in range(HEADS)]
    ld_wo = [pltpu.make_async_copy(wo_hbm.at[h * E:(h + 1) * E], wo_s.at[h * E:(h + 1) * E], wo_sem.at[h])
             for h in range(HEADS)]
    for part in ld_in + [ld_wq[:2]]:
        for c in part:
            c.start()
    LATER = (ld_wq[2:4], ld_wq[4:], [ld_dy], ld_wo[:4])

    barrier = pltpu.get_barrier_semaphore()
    for r in range(1, NDEV):
        pl.semaphore_signal(barrier, inc=1, device_id={'cp': dev(r)}, device_id_type=pl.DeviceIdType.MESH)

    for i, (ka, kb) in enumerate(KPARTS):
        for c in ld_in[i]:
            c.wait()
        for c in LATER[i]:
            c.start()
        kv_part = jnp.concatenate([dot(x_s[a:a + PIECE, ka:kb], side_by_side(wkv_s, 0, 2, ka, kb))
                                   for a in (0, PIECE)], axis=0)
        if i:
            kv_part = s_s[0:TOK, 0:2 * E] + kv_part
        if i < len(KPARTS) - 1:
            s_s[0:TOK, 0:2 * E] = kv_part
        if i == 1:
            pl.semaphore_wait(barrier, NDEV - 1)
            doc_s[me] = doc_ref[...]
            doc_out = {}
            for r in range(1, NDEV):
                doc_out[r] = rcopy(doc_ref, doc_s.at[me], doc_send.at[r], doc_recv.at[r], r)
                doc_out[r].start()
    kv_own = kv_part.astype(BF16)
    my_off = pl.multiple_of(me * PIECE, 32)
    for t in range(2):
        for half in range(2):
            kv_s[t, half, pl.ds(my_off, PIECE), :] = kv_own[half * PIECE:(half + 1) * PIECE, t * E:(t + 1) * E]

    def kv_blk(t, owner):
        return kv_s.at[t, :, pl.ds(pl.multiple_of(owner * PIECE, 32), PIECE), :]

    def kv_send_own(t, g):
        blk = kv_blk(t, me)
        to = dev(2 * g) + 1 - core if g else dev(1)
        return pltpu.make_async_remote_copy(
            src_ref=blk, dst_ref=blk, send_sem=kv_send.at[t, g], recv_sem=kv_recv.at[t, 2 * g + core],
            device_id={'cp': to}, device_id_type=pl.DeviceIdType.MESH)

    def kv_hand_on(t, g, c):
        blk = kv_blk(t, dev(2 * g) - core + c)
        return pltpu.make_async_remote_copy(
            src_ref=blk, dst_ref=blk, send_sem=kv_pass.at[t, 2 * g + c], recv_sem=kv_recv.at[t, 2 * g + c],
            device_id={'cp': dev(1)}, device_id_type=pl.DeviceIdType.MESH)

    REMOTE = [(g, c) for g in (3, 1, 2) for c in (1, 0)]

    for t in range(2):
        for g in (3, 1, 2, 0):
            kv_send_own(t, g).start()

    def hand_on(t):
        @pl.when(core == 1)
        def _():
            for g, c in REMOTE:
                kv_hand_on(t, g, c).wait_recv()
                kv_hand_on(t, g, c).start()

    def wait_blocks(t):
        @pl.when(core == 0)
        def _():
            for g, c in REMOTE:
                kv_hand_on(t, g, c).wait_recv()
            kv_hand_on(t, 0, 1).wait_recv()

        @pl.when(core == 1)
        def _():
            kv_hand_on(t, 0, 0).wait_recv()

    def put_rows(dst, val, h):
        dst[0, h * PIECE:(h + 1) * PIECE, :] = val[0:PIECE]
        dst[1, h * PIECE:(h + 1) * PIECE, :] = val[PIECE:TOK]

    for h0, h1 in GROUPS:
        for h in range(h0, h1):
            ld_wq[h].wait()
        for c in ld_wo[4:] if h0 == 0 else []:
            c.start()
        val = dot(x_s[...], side_by_side(wq_s, h0, h1, 0, D)).astype(BF16)
        for h in range(h0, h1):
            put_rows(q_s, val[:, (h - h0) * E:(h - h0 + 1) * E], h)
    for r in range(1, NDEV):
        rcopy(doc_ref, doc_s.at[dev(r)], doc_send.at[r], doc_recv.at[r], r).wait_recv()
    ld_dy.wait()
    for h0, h1 in GROUPS:
        for h in range(h0, h1):
            ld_wo[h].wait()
        val = dot(dy_s[...], wo_s[h0 * E:h1 * E, :], NT).astype(BF16)
        for h in range(h0, h1):
            put_rows(do_s, val[:, (h - h0) * E:(h - h0 + 1) * E], h)
        if h0 == 0:
            my_doc = doc_ref[...].astype(F32)
            eye = (lax.broadcasted_iota(jnp.int32, (TOK, TOK), 0) == lax.broadcasted_iota(jnp.int32, (TOK, TOK), 1))
            doc_col = jnp.sum(jnp.where(eye, jnp.broadcast_to(my_doc, (TOK, TOK)), 0.0), axis=1, keepdims=True)
            less = jnp.zeros((TOK, TOK), F32)
            for d in range(NDEV):
                less = less + jnp.where(doc_s[d].astype(F32) < doc_col, 1.0, 0.0)
            first = jnp.sum(less, axis=1, keepdims=True)
            rowi = lax.broadcasted_iota(jnp.int32, (PIECE, 1), 0)
            pos_lo = (me * PIECE + rowi).astype(F32)
            pos_hi = ((2 * NDEV - 1 - me) * PIECE + rowi).astype(F32)
            lane = lax.broadcasted_iota(jnp.int32, (1, HALF), 1).astype(F32)
            kpos_lo = lane
            kpos_hi = (2 * NDEV - 1) * PIECE + lane - 2 * PIECE * jnp.floor((lane + 0.5) * (1.0 / PIECE))

            def cap_of(kpos, lo, hi):
                return jnp.where((kpos >= lo) & (kpos <= hi), jnp.inf, NEG_BIG)

            cap_s[:, 0:HALF] = cap_of(kpos_lo, first[PIECE:TOK], pos_hi)
            cap_s[:, HALF:2 * HALF] = cap_of(kpos_hi, first[PIECE:TOK], pos_hi)
            cap_s[:, 2 * HALF:3 * HALF] = cap_of(kpos_lo, first[0:PIECE], pos_lo)
            hand_on(0)
        else:
            for piece in range(2):
                qt_s[piece] = q_s[piece].T

    wait_blocks(0)

    k_scale = E ** -0.5
    exp_scale = k_scale * math.log2(math.e)
    def keys(t, a, b):
        return kv_s[t, a // HALF, a % HALF:a % HALF + (b - a), :]

    def over_keys(src, t, base, segs):
        parts = []
        for a, b in ((0, ROWS // 2), (ROWS // 2, ROWS)):
            acc = None
            for c, d in segs:
                val = dot(src[a:b, base + c:base + d], keys(t, c, d))
                acc = val if acc is None else acc + val
            parts.append(acc)
        return jnp.concatenate(parts, axis=0)

    def side(ref, rows, base, segs):
        return jnp.concatenate([ref[rows, base + c:base + d] for c, d in segs], axis=1)

    def softmax(base, segs, h):
        rb = 16 if sum(d - c for c, d in segs) > HALF else 32
        for b in range(PIECE // rb):
            rows = slice(h * PIECE + b * rb, h * PIECE + (b + 1) * rb)
            s = jnp.minimum(side(s_s, rows, base, segs), side(cap_s, slice(b * rb, (b + 1) * rb), base, segs))
            m = jnp.max(s, axis=1, keepdims=True)
            e = jnp.exp2((s - m) * exp_scale)
            l = jnp.sum(e, axis=1, keepdims=True)
            p = (e * (1.0 / l)).astype(BF16)
            at = 0
            for c, d in segs:
                p_s[rows, base + c:base + d] = p[:, at:at + d - c]
                at += d - c

    def blk(t, half, owner):
        return acc_s.at[t, half, pl.ds(pl.multiple_of(owner * PIECE, 32), PIECE), :]

    def d2d(t, half, g):
        return rcopy(blk(t, half, dev(2 * g + 1)), rb1.at[t, half, g], d2d_send.at[t, half, g],
                     d2d_recv.at[t, half, g], 1)

    def rs(t, half, g):
        return rcopy(comb.at[t, half, g], rb2.at[t, half, g], rs_send.at[t, half, g], rs_recv.at[t, half, g], 2 * g)

    def start_d2d(t, half, gs):
        for g in gs:
            d2d(t, half, g).start()

    def add_peer(t, half, g, late):
        if half and late and g >= 2:
            comb[t, half, g] = jnp.zeros((PIECE, E), F32)
            return
        d2d(t, half, g).wait_recv()
        comb[t, half, g] = (acc_s[t, half, pl.ds(pl.multiple_of(dev(2 * g) * PIECE, 32), PIECE), :]
                            + rb1[t, half, g])

    def combine_direct(t, half, late):
        for g in (3, 1, 2, 0):
            if not (half and late and g >= 2):
                add_peer(t, half, g, late)
                if g:
                    rs(t, half, g).start()

    first_dev = lax.rem(cy + core, 2) * 4 + lax.rem(cx + 1 - core, 2) * 2 + core
    second_dev = lax.rem(cy + 1 - core, 2) * 4 + lax.rem(cx + core, 2) * 2 + core
    first_g, second_g = 1 + core, 2 - core

    def to_first(t, half, i):
        if i == 0:
            src, dst = comb.at[t, half, 3], relay.at[t, half]
        else:
            src, dst = comb.at[t, half, first_g], rb2.at[t, half, 1]
        return pltpu.make_async_remote_copy(
            src_ref=src, dst_ref=dst, send_sem=rs_send.at[t, half, i], recv_sem=rs_recv.at[t, half, i],
            device_id={'cp': first_dev}, device_id_type=pl.DeviceIdType.MESH)

    def to_second(t, half):
        return pltpu.make_async_remote_copy(
            src_ref=comb.at[t, half, second_g], dst_ref=rb2.at[t, half, 2], send_sem=rs_send.at[t, half, 2],
            recv_sem=rs_recv.at[t, half, 2], device_id={'cp': second_dev}, device_id_type=pl.DeviceIdType.MESH)

    def combine_relayed(t, half, late):
        add_peer(t, half, 3, late)
        to_first(t, half, 0).start()
        add_peer(t, half, 1, late)
        add_peer(t, half, 2, late)
        to_first(t, half, 1).start()
        add_peer(t, half, 0, late)

    def pass_on(t, half):
        to_first(t, half, 0).wait_recv()
        comb[t, half, second_g] = comb[t, half, second_g] + relay[t, half]
        to_second(t, half).start()

    QUART = HALF // 2

    def attention(late):
        hi = ((0, HALF), (HALF + QUART, SEQ)) if late else ((0, HALF), (HALF, SEQ))
        lo = ((0, HALF),) if late else ((0, QUART),)
        hi_blocks = [(a, min(a + 512, d)) for c, d in hi for a in range(c, d, 512)]
        lo_blocks = [(a, min(a + 512, d)) for c, d in lo for a in range(c, d, 512)]

        def grad(t, half, lhs_t, src):
            cuts = ((QUART, 512), (512, HALF)) if half and late else ((0, 256), (256, 512), (512, HALF))
            for a, b in cuts:
                val = dot(lhs_t[1], src[:, half * HALF + a:half * HALF + b])
                c = b if late else min(b, QUART)
                if not half and c > a:
                    more = dot(lhs_t[0], src[:, SEQ + a:SEQ + c])
                    val = val + more if c == b else jnp.concatenate([val[:, :c - a] + more, val[:, c - a:]], axis=1)
                acc_s[t, half, a:b, :] = val.T
            start_d2d(t, half, (1, 0) if half and late else (3, 1, 2, 0))

        def s_part(piece, base, a, b, r0=0, r1=ROWS):
            s_s[r0:r1, base + a:base + b] = dot(q_s[piece, r0:r1, :], keys(0, a, b), NT)

        def dp_part(piece, base, a, b):
            dp_s[:, base + a:base + b] = dot(do_s[piece], keys(1, a, b), NT)

        def o_part(piece, base, segs):
            o_bf = over_keys(p_s, 1, base, segs).astype(BF16)
            delta_s[piece] = jnp.sum(do_s[piece].astype(F32) * o_bf.astype(F32), axis=1, keepdims=True)
            for h in range(HEADS):
                o_s[piece * PIECE:(piece + 1) * PIECE, h * E:(h + 1) * E] = o_bf[h * PIECE:(h + 1) * PIECE]

        def ds_rows(piece, base, segs):
            for h in range(HEADS):
                for c in range(PIECE // 32):
                    r0 = h * PIECE + c * 32
                    for a, b in segs:
                        ds_s[r0:r0 + 32, base + a:base + b] = (
                            p_s[r0:r0 + 32, base + a:base + b].astype(F32)
                            * (dp_s[r0:r0 + 32, base + a:base + b] - delta_s[piece, r0:r0 + 32, :])).astype(BF16)

        def dq_part(piece, base, segs):
            dq_bf = (over_keys(ds_s, 0, base, segs) * k_scale).astype(BF16)
            for h in range(HEADS):
                dq_s[piece * PIECE:(piece + 1) * PIECE, h * E:(h + 1) * E] = dq_bf[h * PIECE:(h + 1) * PIECE]

        def softmax_with(base, segs, h0, h1, others):
            for h in range(h0, h1):
                softmax(base, segs, h)
                left = h1 - h
                take = -(-len(others) // left)
                for fn in others[:take]:
                    fn()
                others = others[take:]

        for a, b in hi_blocks:
            s_part(1, 0, a, b, 0, 336)
        for piece in range(2):
            dot_s[piece] = do_s[piece].T
        softmax_with(0, hi, 0, 3, [lambda a=a, b=b: s_part(1, 0, a, b, 336, ROWS) for a, b in hi_blocks])
        hand_on(1)
        softmax_with(0, hi, 3, HEADS, [lambda a=a, b=b: s_part(0, SEQ, a, b) for a, b in lo_blocks])
        grad(1, 1, dot_s, p_s)
        wait_blocks(1)
        softmax_with(SEQ, lo, 0, HEADS, [lambda a=a, b=b: dp_part(1, 0, a, b) for a, b in hi_blocks])
        combine_direct(1, 1, late)
        grad(1, 0, dot_s, p_s)
        o_part(1, 0, hi)
        ds_rows(1, 0, hi[1:])
        for a, b in lo_blocks:
            dp_part(0, SEQ, a, b)
        grad(0, 1, qt_s, ds_s)
        combine_relayed(1, 0, late)
        o_part(0, SEQ, lo)
        ds_rows(1, 0, hi[:1])
        ds_rows(0, SEQ, lo)
        grad(0, 0, qt_s, ds_s)
        combine_relayed(0, 1, late)
        dq_part(1, 0, hi)
        dq_part(0, SEQ, lo)

    for late in range(2):
        pl.when(cy == late)(lambda late=late: attention(late))

    combine_direct(0, 0, 0)
    NY = 896

    def y_part(a, b):
        y_s[:, a:b] = dot(o_s[...], wo_s[:, a:b]).astype(BF16)

    y_part(0, 1792)
    pass_on(1, 0)
    y_part(1792, D)
    pass_on(0, 1)
    for i in range(D // NY):
        dx_s[:, i * NY:(i + 1) * NY] = dot(dq_s[...], side_by_side(wq_s, 0, HEADS, i * NY, (i + 1) * NY), NT)

    def put_total(t, half, tot):
        if t == 0:
            tot = tot * k_scale
        dkv_s[half * PIECE:(half + 1) * PIECE, t * E:(t + 1) * E] = tot.astype(BF16)

    @pl.when(cy == 0)
    def _():
        rs(1, 1, 1).wait_recv()
        put_total(1, 1, comb[1, 1, 0] + rb2[1, 1, 1])

    @pl.when(cy == 1)
    def _():
        for g in (1, 2, 3):
            rs(1, 1, g).wait_recv()
        put_total(1, 1, (comb[1, 1, 0] + rb2[1, 1, 1]) + (rb2[1, 1, 2] + rb2[1, 1, 3]))

    for t, half in UNITS[1:3]:
        to_first(t, half, 1).wait_recv()
        to_second(t, half).wait_recv()
        put_total(t, half, comb[t, half, 0] + (rb2[t, half, 1] + rb2[t, half, 2]))
    for g in (3, 1, 2):
        rs(0, 0, g).wait_recv()
    put_total(0, 0, (comb[0, 0, 0] + rb2[0, 0, 1]) + (rb2[0, 0, 2] + rb2[0, 0, 3]))

    for r in range(1, NDEV):
        doc_out[r].wait_send()
    for t in range(2):
        for g in range(4):
            kv_send_own(t, g).wait_send()

    @pl.when(core == 1)
    def _():
        for t in range(2):
            for g, c in REMOTE:
                kv_hand_on(t, g, c).wait_send()

    for t, half in UNITS:
        for g in range(2):
            d2d(t, half, g).wait_send()
        if not half:
            for g in range(2, 4):
                d2d(t, half, g).wait_send()
    rs(1, 1, 1).wait_send()

    @pl.when(cy == 0)
    def _():
        for t in range(2):
            for g in range(2, 4):
                d2d(t, 1, g).wait_send()
        for g in range(2, 4):
            rs(1, 1, g).wait_send()

    for t, half in UNITS[1:3]:
        to_first(t, half, 0).wait_send()
        to_first(t, half, 1).wait_send()
        to_second(t, half).wait_send()
    for g in (1, 2, 3):
        rs(0, 0, g).wait_send()


FIN = ((0, 1536), (1536, 2560), (2560, 3584))


def final_kernel(y_s, dx_s, dkv_s, wkv_s, y_hbm, dx_hbm, dxo_s, y_sem, dx_sem):
    y_cp = pltpu.make_async_copy(y_s, y_hbm, y_sem)
    y_cp.start()
    copies = [y_cp]
    for i, (a, b) in enumerate(FIN):
        dxo_s[:, a:b] = (dx_s[:, a:b] + dot(dkv_s[...], side_by_side(wkv_s, 0, 2, a, b), NT)).astype(BF16)
        cp = pltpu.make_async_copy(dxo_s.at[:, a:b], dx_hbm.at[:, a:b], dx_sem.at[i])
        cp.start()
        copies.append(cp)
    for cp in copies:
        cp.wait()


def solution(mesh):
    row_spec = P(('dp', 'cp'))
    full_spec = P()
    hbm_spec = pl.BlockSpec(memory_space=pltpu.HBM)
    vmem_spec = pl.BlockSpec(memory_space=pltpu.VMEM)

    def local_layer(x_in, dy_in, doc_id, w_q, w_k, w_v, w_o):
        V = pltpu.VMEM
        dma = pltpu.SemaphoreType.DMA
        sds = jax.ShapeDtypeStruct
        hbm = lambda a: pltpu.with_memory_space_constraint(a, pltpu.HBM)
        parts = pl.pallas_call(
            main_kernel,
            out_shape=(V((TOK, D), BF16), V((TOK, D), F32), V((TOK, 2 * E), BF16), V((2, D, E), BF16)),
            in_specs=[hbm_spec, hbm_spec, vmem_spec, hbm_spec, hbm_spec, hbm_spec, hbm_spec],
            out_specs=(vmem_spec,) * 4,
            scratch_shapes=[
                V((TOK, D), BF16), V((TOK, D), BF16), V((HEADS, D, E), BF16), V((HE, D), BF16),
                V((2, 2, HALF, E), BF16), V((NDEV, 1, TOK), jnp.int32),
                V((2, ROWS, E), BF16), V((2, ROWS, E), BF16), V((2, E, ROWS), BF16), V((2, E, ROWS), BF16),
                V((PIECE, 3 * HALF), F32),
                V((ROWS, 3 * HALF), F32), V((ROWS, 3 * HALF), BF16), V((ROWS, 3 * HALF), F32),
                V((ROWS, 3 * HALF), BF16),
                V((TOK, HE), BF16), V((TOK, HE), BF16), V((2, ROWS, 1), F32),
                V((2, 2, HALF, E), F32),
                V((2, 2, 4, PIECE, E), F32), V((2, 2, 4, PIECE, E), F32), V((2, 2, 4, PIECE, E), F32), V((2, 2, PIECE, E), F32),
                dma((len(KPARTS), 3)), dma((HEADS,)), dma((HEADS,)), dma,
                dma((NDEV,)), dma((NDEV,)), dma((2, 4)), dma((2, NDEV)), dma((2, NDEV)),
                dma((2, 2, 4)), dma((2, 2, 4)), dma((2, 2, 4)), dma((2, 2, 4)),
            ],
            compiler_params=pltpu.CompilerParams(collective_id=0, has_side_effects=True,
                                                 vmem_limit_bytes=50 * 1024 * 1024),
        )(hbm(x_in), hbm(dy_in), doc_id.reshape(1, TOK), hbm(jnp.transpose(w_q, (1, 0, 2))), hbm(w_k.reshape(D, E)),
          hbm(w_v.reshape(D, E)), hbm(w_o.reshape(HE, D)))
        return pl.pallas_call(
            final_kernel,
            out_shape=(sds((TOK, D), BF16), sds((TOK, D), BF16)),
            in_specs=[vmem_spec] * 4,
            out_specs=(hbm_spec, hbm_spec),
            scratch_shapes=[V((TOK, D), BF16), dma, dma((len(FIN),))],
            compiler_params=pltpu.CompilerParams(vmem_limit_bytes=12 * 1024 * 1024),
        )(*[pltpu.with_memory_space_constraint(a, pltpu.VMEM) for a in parts])

    return jax.shard_map(local_layer, mesh=mesh,
                         in_specs=(row_spec, row_spec, row_spec, full_spec, full_spec, full_spec, full_spec),
                         out_specs=(row_spec, row_spec), check_vma=False)
```

```python
import math

import jax
import jax.numpy as jnp
from jax import lax
from jax.experimental import pallas as pl
from jax.experimental.pallas import tpu as pltpu
from jax.sharding import PartitionSpec as P

NEG_BIG = -1.0e30
F32 = jnp.float32
BF16 = jnp.bfloat16

NDEV = 8
HEADS = 7
E = 128
PIECE = 96
TOK = 192
D = 3584
HE = HEADS * E
ROWS = HEADS * PIECE
HALF = NDEV * PIECE
SEQ = 2 * HALF
KPARTS = ((0, 1024), (1024, 2048), (2048, 3072), (3072, D))

NT = (((1,), (1,)), ((), ()))
NN = (((1,), (0,)), ((), ()))
UNITS = ((1, 1), (1, 0), (0, 1), (0, 0))
GROUPS = ((0, 4), (4, 7))


def dot(a, b, dims=NN):
    return lax.dot_general(a, b, dims, preferred_element_type=F32)


def side_by_side(ref, h0, h1, r0, r1):
    return jnp.concatenate([ref[h, r0:r1, :] for h in range(h0, h1)], axis=1)


def main_kernel(x_hbm, dy_hbm, doc_hbm, wq_hbm, wk_hbm, wv_hbm, wo_hbm,
                y_s, dx_s, dkv_s, wkv_s,
                x_s, dy_s, wq_s, wo_s, doc_ref,
                kv_s, doc_s, q_s, do_s, qt_s, dot_s, cap_s,
                s_s, p_s, dp_s, ds_s, o_s, dq_s, delta_s,
                acc_s, rb1, comb, rb2, relay,
                in_sem, wq_sem, wo_sem, dy_sem, doc_sem,
                doc_send, doc_recv, kv_send, kv_recv, kv_pass,
                d2d_send, d2d_recv, rs_send, rs_recv):
    me = lax.axis_index('cp')
    core = lax.rem(me, 2)
    chip = me // 2
    cx = lax.rem(chip, 2)
    cy = chip // 2

    def dev(r):
        yy = lax.rem(cy + (r // 4), 2)
        xx = lax.rem(cx + ((r // 2) % 2), 2)
        cc = lax.rem(core + (r % 2), 2)
        return yy * 4 + xx * 2 + cc

    def rcopy(src, dst, ssem, rsem, r):
        return pltpu.make_async_remote_copy(src_ref=src, dst_ref=dst, send_sem=ssem, recv_sem=rsem,
                                            device_id={'cp': dev(r)}, device_id_type=pl.DeviceIdType.MESH)

    ld_in = []
    for i, (ka, kb) in enumerate(KPARTS):
        ks = slice(ka, kb)
        ld_in.append([pltpu.make_async_copy(x_hbm.at[:, ks], x_s.at[:, ks], in_sem.at[i, 0]),
                      pltpu.make_async_copy(wk_hbm.at[ks], wkv_s.at[0, ks], in_sem.at[i, 1]),
                      pltpu.make_async_copy(wv_hbm.at[ks], wkv_s.at[1, ks], in_sem.at[i, 2])])
    ld_dy = pltpu.make_async_copy(dy_hbm, dy_s, dy_sem)
    ld_doc = pltpu.make_async_copy(doc_hbm, doc_ref, doc_sem)
    ld_wq = [pltpu.make_async_copy(wq_hbm.at[h], wq_s.at[h], wq_sem.at[h]) for h in range(HEADS)]
    ld_wo = [pltpu.make_async_copy(wo_hbm.at[h * E:(h + 1) * E], wo_s.at[h * E:(h + 1) * E], wo_sem.at[h])
             for h in range(HEADS)]
    for part in ld_in + [[ld_doc], ld_wq[:2]]:
        for c in part:
            c.start()
    LATER = (ld_wq[2:4], ld_wq[4:], [ld_dy], ld_wo[:4])

    barrier = pltpu.get_barrier_semaphore()
    for r in range(1, NDEV):
        pl.semaphore_signal(barrier, inc=1, device_id={'cp': dev(r)}, device_id_type=pl.DeviceIdType.MESH)

    for i, (ka, kb) in enumerate(KPARTS):
        for c in ld_in[i]:
            c.wait()
        for c in LATER[i]:
            c.start()
        kv_part = jnp.concatenate([dot(x_s[a:a + PIECE, ka:kb], side_by_side(wkv_s, 0, 2, ka, kb))
                                   for a in (0, PIECE)], axis=0)
        if i:
            kv_part = s_s[0:TOK, 0:2 * E] + kv_part
        if i < len(KPARTS) - 1:
            s_s[0:TOK, 0:2 * E] = kv_part
        if i == 1:
            pl.semaphore_wait(barrier, NDEV - 1)
            ld_doc.wait()
            doc_s[me] = doc_ref[...]
            doc_out = {}
            for r in range(1, NDEV):
                doc_out[r] = rcopy(doc_ref, doc_s.at[me], doc_send.at[r], doc_recv.at[r], r)
                doc_out[r].start()
    kv_own = kv_part.astype(BF16)
    my_off = pl.multiple_of(me * PIECE, 32)
    for t in range(2):
        for half in range(2):
            kv_s[t, half, pl.ds(my_off, PIECE), :] = kv_own[half * PIECE:(half + 1) * PIECE, t * E:(t + 1) * E]

    def kv_blk(t, owner):
        return kv_s.at[t, :, pl.ds(pl.multiple_of(owner * PIECE, 32), PIECE), :]

    def kv_send_own(t, g):
        blk = kv_blk(t, me)
        to = dev(2 * g) + 1 - core if g else dev(1)
        return pltpu.make_async_remote_copy(
            src_ref=blk, dst_ref=blk, send_sem=kv_send.at[t, g], recv_sem=kv_recv.at[t, 2 * g + core],
            device_id={'cp': to}, device_id_type=pl.DeviceIdType.MESH)

    def kv_hand_on(t, g, c):
        blk = kv_blk(t, dev(2 * g) - core + c)
        return pltpu.make_async_remote_copy(
            src_ref=blk, dst_ref=blk, send_sem=kv_pass.at[t, 2 * g + c], recv_sem=kv_recv.at[t, 2 * g + c],
            device_id={'cp': dev(1)}, device_id_type=pl.DeviceIdType.MESH)

    REMOTE = [(g, c) for g in (3, 1, 2) for c in (1, 0)]

    for t in range(2):
        for g in (3, 1, 2, 0):
            kv_send_own(t, g).start()

    def hand_on(t):
        @pl.when(core == 1)
        def _():
            for g, c in REMOTE:
                kv_hand_on(t, g, c).wait_recv()
                kv_hand_on(t, g, c).start()

    def wait_blocks(t):
        @pl.when(core == 0)
        def _():
            for g, c in REMOTE:
                kv_hand_on(t, g, c).wait_recv()
            kv_hand_on(t, 0, 1).wait_recv()

        @pl.when(core == 1)
        def _():
            kv_hand_on(t, 0, 0).wait_recv()

    def put_rows(dst, val, h):
        dst[0, h * PIECE:(h + 1) * PIECE, :] = val[0:PIECE]
        dst[1, h * PIECE:(h + 1) * PIECE, :] = val[PIECE:TOK]

    for h0, h1 in GROUPS:
        for h in range(h0, h1):
            ld_wq[h].wait()
        for c in ld_wo[4:] if h0 == 0 else []:
            c.start()
        val = dot(x_s[...], side_by_side(wq_s, h0, h1, 0, D)).astype(BF16)
        for h in range(h0, h1):
            put_rows(q_s, val[:, (h - h0) * E:(h - h0 + 1) * E], h)
    for r in range(1, NDEV):
        rcopy(doc_ref, doc_s.at[dev(r)], doc_send.at[r], doc_recv.at[r], r).wait_recv()
    ld_dy.wait()
    for h0, h1 in GROUPS:
        for h in range(h0, h1):
            ld_wo[h].wait()
        val = dot(dy_s[...], wo_s[h0 * E:h1 * E, :], NT).astype(BF16)
        for h in range(h0, h1):
            put_rows(do_s, val[:, (h - h0) * E:(h - h0 + 1) * E], h)
        if h0 == 0:
            my_doc = doc_ref[...].astype(F32)
            eye = (lax.broadcasted_iota(jnp.int32, (TOK, TOK), 0) == lax.broadcasted_iota(jnp.int32, (TOK, TOK), 1))
            doc_col = jnp.sum(jnp.where(eye, jnp.broadcast_to(my_doc, (TOK, TOK)), 0.0), axis=1, keepdims=True)
            less = jnp.zeros((TOK, TOK), F32)
            for d in range(NDEV):
                less = less + jnp.where(doc_s[d].astype(F32) < doc_col, 1.0, 0.0)
            first = jnp.sum(less, axis=1, keepdims=True)
            rowi = lax.broadcasted_iota(jnp.int32, (PIECE, 1), 0)
            pos_lo = (me * PIECE + rowi).astype(F32)
            pos_hi = ((2 * NDEV - 1 - me) * PIECE + rowi).astype(F32)
            lane = lax.broadcasted_iota(jnp.int32, (1, HALF), 1).astype(F32)
            kpos_lo = lane
            kpos_hi = (2 * NDEV - 1) * PIECE + lane - 2 * PIECE * jnp.floor((lane + 0.5) * (1.0 / PIECE))

            def cap_of(kpos, lo, hi):
                return jnp.where((kpos >= lo) & (kpos <= hi), jnp.inf, NEG_BIG)

            cap_s[:, 0:HALF] = cap_of(kpos_lo, first[PIECE:TOK], pos_hi)
            cap_s[:, HALF:2 * HALF] = cap_of(kpos_hi, first[PIECE:TOK], pos_hi)
            cap_s[:, 2 * HALF:3 * HALF] = cap_of(kpos_lo, first[0:PIECE], pos_lo)
            hand_on(0)
        else:
            for piece in range(2):
                qt_s[piece] = q_s[piece].T

    wait_blocks(0)

    k_scale = E ** -0.5
    exp_scale = k_scale * math.log2(math.e)
    def keys(t, a, b):
        return kv_s[t, a // HALF, a % HALF:a % HALF + (b - a), :]

    def over_keys(src, t, base, segs):
        parts = []
        for a, b in ((0, ROWS // 2), (ROWS // 2, ROWS)):
            acc = None
            for c, d in segs:
                val = dot(src[a:b, base + c:base + d], keys(t, c, d))
                acc = val if acc is None else acc + val
            parts.append(acc)
        return jnp.concatenate(parts, axis=0)

    def side(ref, rows, base, segs):
        return jnp.concatenate([ref[rows, base + c:base + d] for c, d in segs], axis=1)

    def softmax(base, segs, h):
        rb = 16 if sum(d - c for c, d in segs) > HALF else 32
        for b in range(PIECE // rb):
            rows = slice(h * PIECE + b * rb, h * PIECE + (b + 1) * rb)
            s = jnp.minimum(side(s_s, rows, base, segs), side(cap_s, slice(b * rb, (b + 1) * rb), base, segs))
            m = jnp.max(s, axis=1, keepdims=True)
            e = jnp.exp2((s - m) * exp_scale)
            l = jnp.sum(e, axis=1, keepdims=True)
            p = (e * (1.0 / l)).astype(BF16)
            at = 0
            for c, d in segs:
                p_s[rows, base + c:base + d] = p[:, at:at + d - c]
                at += d - c

    def blk(t, half, owner):
        return acc_s.at[t, half, pl.ds(pl.multiple_of(owner * PIECE, 32), PIECE), :]

    def d2d(t, half, g):
        return rcopy(blk(t, half, dev(2 * g + 1)), rb1.at[t, half, g], d2d_send.at[t, half, g],
                     d2d_recv.at[t, half, g], 1)

    def rs(t, half, g):
        return rcopy(comb.at[t, half, g], rb2.at[t, half, g], rs_send.at[t, half, g], rs_recv.at[t, half, g], 2 * g)

    def start_d2d(t, half, gs):
        for g in gs:
            d2d(t, half, g).start()

    def add_peer(t, half, g, late):
        if half and late and g >= 2:
            comb[t, half, g] = jnp.zeros((PIECE, E), F32)
            return
        d2d(t, half, g).wait_recv()
        comb[t, half, g] = (acc_s[t, half, pl.ds(pl.multiple_of(dev(2 * g) * PIECE, 32), PIECE), :]
                            + rb1[t, half, g])

    def combine_direct(t, half, late):
        for g in (3, 1, 2, 0):
            if not (half and late and g >= 2):
                add_peer(t, half, g, late)
                if g:
                    rs(t, half, g).start()

    first_dev = lax.rem(cy + core, 2) * 4 + lax.rem(cx + 1 - core, 2) * 2 + core
    second_dev = lax.rem(cy + 1 - core, 2) * 4 + lax.rem(cx + core, 2) * 2 + core
    first_g, second_g = 1 + core, 2 - core

    def to_first(t, half, i):
        if i == 0:
            src, dst = comb.at[t, half, 3], relay.at[t, half]
        else:
            src, dst = comb.at[t, half, first_g], rb2.at[t, half, 1]
        return pltpu.make_async_remote_copy(
            src_ref=src, dst_ref=dst, send_sem=rs_send.at[t, half, i], recv_sem=rs_recv.at[t, half, i],
            device_id={'cp': first_dev}, device_id_type=pl.DeviceIdType.MESH)

    def to_second(t, half):
        return pltpu.make_async_remote_copy(
            src_ref=comb.at[t, half, second_g], dst_ref=rb2.at[t, half, 2], send_sem=rs_send.at[t, half, 2],
            recv_sem=rs_recv.at[t, half, 2], device_id={'cp': second_dev}, device_id_type=pl.DeviceIdType.MESH)

    def combine_relayed(t, half, late):
        add_peer(t, half, 3, late)
        to_first(t, half, 0).start()
        add_peer(t, half, 1, late)
        add_peer(t, half, 2, late)
        to_first(t, half, 1).start()
        add_peer(t, half, 0, late)

    def pass_on(t, half):
        to_first(t, half, 0).wait_recv()
        comb[t, half, second_g] = comb[t, half, second_g] + relay[t, half]
        to_second(t, half).start()

    QUART = HALF // 2

    def attention(late):
        hi = ((0, HALF), (HALF + QUART, SEQ)) if late else ((0, HALF), (HALF, SEQ))
        lo = ((0, HALF),) if late else ((0, QUART),)
        hi_blocks = [(a, min(a + 512, d)) for c, d in hi for a in range(c, d, 512)]
        lo_blocks = [(a, min(a + 512, d)) for c, d in lo for a in range(c, d, 512)]

        def grad(t, half, lhs_t, src):
            cuts = ((QUART, 512), (512, HALF)) if half and late else ((0, 256), (256, 512), (512, HALF))
            for a, b in cuts:
                c = b if late else min(b, QUART)
                if t == 0:
                    ds_rows(1, 0, ((half * HALF + a, half * HALF + b),))
                    if not half and c > a:
                        ds_rows(0, SEQ, ((a, c),))
                val = dot(lhs_t[1], src[:, half * HALF + a:half * HALF + b])
                if not half and c > a:
                    more = dot(lhs_t[0], src[:, SEQ + a:SEQ + c])
                    val = val + more if c == b else jnp.concatenate([val[:, :c - a] + more, val[:, c - a:]], axis=1)
                acc_s[t, half, a:b, :] = val.T
            start_d2d(t, half, (1, 0) if half and late else (3, 1, 2, 0))

        def s_part(piece, base, a, b, r0=0, r1=ROWS):
            s_s[r0:r1, base + a:base + b] = dot(q_s[piece, r0:r1, :], keys(0, a, b), NT)

        def dp_part(piece, base, a, b):
            dp_s[:, base + a:base + b] = dot(do_s[piece], keys(1, a, b), NT)

        def o_part(piece, base, segs):
            o_bf = over_keys(p_s, 1, base, segs).astype(BF16)
            delta_s[piece] = jnp.sum(do_s[piece].astype(F32) * o_bf.astype(F32), axis=1, keepdims=True)
            for h in range(HEADS):
                o_s[piece * PIECE:(piece + 1) * PIECE, h * E:(h + 1) * E] = o_bf[h * PIECE:(h + 1) * PIECE]

        def ds_rows(piece, base, segs):
            for h in range(HEADS):
                for c in range(PIECE // 32):
                    r0 = h * PIECE + c * 32
                    for a, b in segs:
                        ds_s[r0:r0 + 32, base + a:base + b] = (
                            p_s[r0:r0 + 32, base + a:base + b].astype(F32)
                            * (dp_s[r0:r0 + 32, base + a:base + b] - delta_s[piece, r0:r0 + 32, :])).astype(BF16)

        def dq_part(piece, base, segs):
            dq_bf = (over_keys(ds_s, 0, base, segs) * k_scale).astype(BF16)
            for h in range(HEADS):
                dq_s[piece * PIECE:(piece + 1) * PIECE, h * E:(h + 1) * E] = dq_bf[h * PIECE:(h + 1) * PIECE]

        def softmax_with(base, segs, h0, h1, others):
            for h in range(h0, h1):
                softmax(base, segs, h)
                left = h1 - h
                take = -(-len(others) // left)
                for fn in others[:take]:
                    fn()
                others = others[take:]

        for a, b in hi_blocks:
            s_part(1, 0, a, b, 0, 336)
        for piece in range(2):
            dot_s[piece] = do_s[piece].T
        softmax_with(0, hi, 0, 3, [lambda a=a, b=b: s_part(1, 0, a, b, 336, ROWS) for a, b in hi_blocks])
        hand_on(1)
        softmax_with(0, hi, 3, HEADS, [lambda a=a, b=b: s_part(0, SEQ, a, b) for a, b in lo_blocks])
        grad(1, 1, dot_s, p_s)
        wait_blocks(1)
        softmax_with(SEQ, lo, 0, HEADS, [lambda a=a, b=b: dp_part(1, 0, a, b) for a, b in hi_blocks])
        grad(1, 0, dot_s, p_s)
        combine_direct(1, 1, late)
        o_part(1, 0, hi)
        for a, b in lo_blocks:
            dp_part(0, SEQ, a, b)
        grad(0, 1, qt_s, ds_s)
        combine_relayed(1, 0, late)
        o_part(0, SEQ, lo)
        grad(0, 0, qt_s, ds_s)
        combine_relayed(0, 1, late)
        dq_part(1, 0, hi)
        dq_part(0, SEQ, lo)

    for late in range(2):
        pl.when(cy == late)(lambda late=late: attention(late))

    combine_direct(0, 0, 0)
    NY = 896

    def y_part(a, b):
        y_s[:, a:b] = dot(o_s[...], wo_s[:, a:b]).astype(BF16)

    y_part(0, 1792)
    pass_on(1, 0)
    y_part(1792, D)
    pass_on(0, 1)
    for i in range(D // NY):
        dx_s[:, i * NY:(i + 1) * NY] = dot(dq_s[...], side_by_side(wq_s, 0, HEADS, i * NY, (i + 1) * NY), NT)

    def put_total(t, half, tot):
        if t == 0:
            tot = tot * k_scale
        dkv_s[half * PIECE:(half + 1) * PIECE, t * E:(t + 1) * E] = tot.astype(BF16)

    @pl.when(cy == 0)
    def _():
        rs(1, 1, 1).wait_recv()
        put_total(1, 1, comb[1, 1, 0] + rb2[1, 1, 1])

    @pl.when(cy == 1)
    def _():
        for g in (1, 2, 3):
            rs(1, 1, g).wait_recv()
        put_total(1, 1, (comb[1, 1, 0] + rb2[1, 1, 1]) + (rb2[1, 1, 2] + rb2[1, 1, 3]))

    for t, half in UNITS[1:3]:
        to_first(t, half, 1).wait_recv()
        to_second(t, half).wait_recv()
        put_total(t, half, comb[t, half, 0] + (rb2[t, half, 1] + rb2[t, half, 2]))
    for g in (3, 1, 2):
        rs(0, 0, g).wait_recv()
    put_total(0, 0, (comb[0, 0, 0] + rb2[0, 0, 1]) + (rb2[0, 0, 2] + rb2[0, 0, 3]))

    for r in range(1, NDEV):
        doc_out[r].wait_send()
    for t in range(2):
        for g in range(4):
            kv_send_own(t, g).wait_send()

    @pl.when(core == 1)
    def _():
        for t in range(2):
            for g, c in REMOTE:
                kv_hand_on(t, g, c).wait_send()

    for t, half in UNITS:
        for g in range(2):
            d2d(t, half, g).wait_send()
        if not half:
            for g in range(2, 4):
                d2d(t, half, g).wait_send()
    rs(1, 1, 1).wait_send()

    @pl.when(cy == 0)
    def _():
        for t in range(2):
            for g in range(2, 4):
                d2d(t, 1, g).wait_send()
        for g in range(2, 4):
            rs(1, 1, g).wait_send()

    for t, half in UNITS[1:3]:
        to_first(t, half, 0).wait_send()
        to_first(t, half, 1).wait_send()
        to_second(t, half).wait_send()
    for g in (1, 2, 3):
        rs(0, 0, g).wait_send()


FIN = ((0, 1536), (1536, 2560), (2560, 3584))


def final_kernel(y_s, dx_s, dkv_s, wkv_s, y_hbm, dx_hbm, dxo_s, y_sem, dx_sem):
    y_cp = pltpu.make_async_copy(y_s, y_hbm, y_sem)
    y_cp.start()
    copies = [y_cp]
    for i, (a, b) in enumerate(FIN):
        dxo_s[:, a:b] = (dx_s[:, a:b] + dot(dkv_s[...], side_by_side(wkv_s, 0, 2, a, b), NT)).astype(BF16)
        cp = pltpu.make_async_copy(dxo_s.at[:, a:b], dx_hbm.at[:, a:b], dx_sem.at[i])
        cp.start()
        copies.append(cp)
    for cp in copies:
        cp.wait()


def solution(mesh):
    row_spec = P(('dp', 'cp'))
    full_spec = P()
    hbm_spec = pl.BlockSpec(memory_space=pltpu.HBM)
    vmem_spec = pl.BlockSpec(memory_space=pltpu.VMEM)

    def local_layer(x_in, dy_in, doc_id, w_q, w_k, w_v, w_o):
        V = pltpu.VMEM
        dma = pltpu.SemaphoreType.DMA
        sds = jax.ShapeDtypeStruct
        hbm = lambda a: pltpu.with_memory_space_constraint(a, pltpu.HBM)
        parts = pl.pallas_call(
            main_kernel,
            out_shape=(V((TOK, D), BF16), V((TOK, D), F32), V((TOK, 2 * E), BF16), V((2, D, E), BF16)),
            in_specs=[hbm_spec, hbm_spec, hbm_spec, hbm_spec, hbm_spec, hbm_spec, hbm_spec],
            out_specs=(vmem_spec,) * 4,
            scratch_shapes=[
                V((TOK, D), BF16), V((TOK, D), BF16), V((HEADS, D, E), BF16), V((HE, D), BF16), V((1, TOK), jnp.int32),
                V((2, 2, HALF, E), BF16), V((NDEV, 1, TOK), jnp.int32),
                V((2, ROWS, E), BF16), V((2, ROWS, E), BF16), V((2, E, ROWS), BF16), V((2, E, ROWS), BF16),
                V((PIECE, 3 * HALF), F32),
                V((ROWS, 3 * HALF), F32), V((ROWS, 3 * HALF), BF16), V((ROWS, 3 * HALF), F32),
                V((ROWS, 3 * HALF), BF16),
                V((TOK, HE), BF16), V((TOK, HE), BF16), V((2, ROWS, 1), F32),
                V((2, 2, HALF, E), F32),
                V((2, 2, 4, PIECE, E), F32), V((2, 2, 4, PIECE, E), F32), V((2, 2, 4, PIECE, E), F32), V((2, 2, PIECE, E), F32),
                dma((len(KPARTS), 3)), dma((HEADS,)), dma((HEADS,)), dma, dma,
                dma((NDEV,)), dma((NDEV,)), dma((2, 4)), dma((2, NDEV)), dma((2, NDEV)),
                dma((2, 2, 4)), dma((2, 2, 4)), dma((2, 2, 4)), dma((2, 2, 4)),
            ],
            compiler_params=pltpu.CompilerParams(collective_id=0, has_side_effects=True,
                                                 vmem_limit_bytes=50 * 1024 * 1024),
        )(hbm(x_in), hbm(dy_in), hbm(doc_id.reshape(1, TOK)), hbm(jnp.transpose(w_q, (1, 0, 2))), hbm(w_k.reshape(D, E)),
          hbm(w_v.reshape(D, E)), hbm(w_o.reshape(HE, D)))
        return pl.pallas_call(
            final_kernel,
            out_shape=(sds((TOK, D), BF16), sds((TOK, D), BF16)),
            in_specs=[vmem_spec] * 4,
            out_specs=(hbm_spec, hbm_spec),
            scratch_shapes=[V((TOK, D), BF16), dma, dma((len(FIN),))],
            compiler_params=pltpu.CompilerParams(vmem_limit_bytes=12 * 1024 * 1024),
        )(*[pltpu.with_memory_space_constraint(a, pltpu.VMEM) for a in parts])

    return jax.shard_map(local_layer, mesh=mesh,
                         in_specs=(row_spec, row_spec, row_spec, full_spec, full_spec, full_spec, full_spec),
                         out_specs=(row_spec, row_spec), check_vma=False)
```

```python
import math

import jax
import jax.numpy as jnp
from jax import lax
from jax.experimental import pallas as pl
from jax.experimental.pallas import tpu as pltpu
from jax.sharding import PartitionSpec as P

NEG_BIG = -1.0e30
F32 = jnp.float32
BF16 = jnp.bfloat16

NDEV = 8
HEADS = 7
E = 128
PIECE = 96
TOK = 192
D = 3584
HE = HEADS * E
ROWS = HEADS * PIECE
HALF = NDEV * PIECE
SEQ = 2 * HALF
KPARTS = ((0, 2048), (2048, D))

NT = (((1,), (1,)), ((), ()))
NN = (((1,), (0,)), ((), ()))
UNITS = ((1, 1), (1, 0), (0, 1), (0, 0))
GROUPS = ((0, 4), (4, 7))


def dot(a, b, dims=NN):
    return lax.dot_general(a, b, dims, preferred_element_type=F32)


def side_by_side(ref, h0, h1, r0, r1):
    return jnp.concatenate([ref[h, r0:r1, :] for h in range(h0, h1)], axis=1)


def main_kernel(x_hbm, dy_hbm, doc_hbm, wq_hbm, wk_hbm, wv_hbm, wo_hbm,
                y_s, dx_s, dkv_s, wkv_s,
                x_s, dy_s, wq_s, wo_s, doc_ref,
                kv_s, doc_s, q_s, do_s, qt_s, dot_s, cap_s,
                s_s, p_s, dp_s, ds_s, o_s, dq_s, delta_s,
                acc_s, rb1, comb, rb2, relay,
                in_sem, wq_sem, wo_sem, dy_sem, doc_sem,
                doc_send, doc_recv, kv_send, kv_recv, kv_pass,
                d2d_send, d2d_recv, rs_send, rs_recv):
    me = lax.axis_index('cp')
    core = lax.rem(me, 2)
    chip = me // 2
    cx = lax.rem(chip, 2)
    cy = chip // 2

    def dev(r):
        yy = lax.rem(cy + (r // 4), 2)
        xx = lax.rem(cx + ((r // 2) % 2), 2)
        cc = lax.rem(core + (r % 2), 2)
        return yy * 4 + xx * 2 + cc

    def rcopy(src, dst, ssem, rsem, r):
        return pltpu.make_async_remote_copy(src_ref=src, dst_ref=dst, send_sem=ssem, recv_sem=rsem,
                                            device_id={'cp': dev(r)}, device_id_type=pl.DeviceIdType.MESH)

    ld_in = []
    for i, (ka, kb) in enumerate(KPARTS):
        ks = slice(ka, kb)
        ld_in.append([pltpu.make_async_copy(x_hbm.at[:, ks], x_s.at[:, ks], in_sem.at[i, 0]),
                      pltpu.make_async_copy(wk_hbm.at[ks], wkv_s.at[0, ks], in_sem.at[i, 1]),
                      pltpu.make_async_copy(wv_hbm.at[ks], wkv_s.at[1, ks], in_sem.at[i, 2])])
    ld_dy = pltpu.make_async_copy(dy_hbm, dy_s, dy_sem)
    ld_doc = pltpu.make_async_copy(doc_hbm, doc_ref, doc_sem)
    ld_wq = [pltpu.make_async_copy(wq_hbm.at[a:b], wq_s.at[a:b], wq_sem.at[i])
             for i, (a, b) in enumerate(((0, 2), (2, 4), (4, HEADS)))]
    ld_wo = [pltpu.make_async_copy(wo_hbm.at[a * E:b * E], wo_s.at[a * E:b * E], wo_sem.at[i])
             for i, (a, b) in enumerate(GROUPS)]
    for part in ld_in + [[ld_doc], ld_wq[:1]]:
        for c in part:
            c.start()
    LATER = (ld_wq[1:2], ld_wq[2:] + [ld_dy])

    barrier = pltpu.get_barrier_semaphore()
    for r in range(1, NDEV):
        pl.semaphore_signal(barrier, inc=1, device_id={'cp': dev(r)}, device_id_type=pl.DeviceIdType.MESH)

    for i, (ka, kb) in enumerate(KPARTS):
        for c in ld_in[i]:
            c.wait()
        for c in LATER[i]:
            c.start()
        kv_part = jnp.concatenate([dot(x_s[a:a + PIECE, ka:kb], side_by_side(wkv_s, 0, 2, ka, kb))
                                   for a in (0, PIECE)], axis=0)
        if i:
            kv_part = s_s[0:TOK, 0:2 * E] + kv_part
        if i < len(KPARTS) - 1:
            s_s[0:TOK, 0:2 * E] = kv_part
        if i == 0:
            pl.semaphore_wait(barrier, NDEV - 1)
            ld_doc.wait()
            doc_s[me] = doc_ref[...]
            doc_out = {}
            for r in range(1, NDEV):
                doc_out[r] = rcopy(doc_ref, doc_s.at[me], doc_send, doc_recv, r)
                doc_out[r].start()
    kv_own = kv_part.astype(BF16)
    my_off = pl.multiple_of(me * PIECE, 32)
    for t in range(2):
        for half in range(2):
            kv_s[t, half, pl.ds(my_off, PIECE), :] = kv_own[half * PIECE:(half + 1) * PIECE, t * E:(t + 1) * E]

    def kv_blk(t, owner):
        return kv_s.at[t, :, pl.ds(pl.multiple_of(owner * PIECE, 32), PIECE), :]

    def kv_send_own(t, g):
        blk = kv_blk(t, me)
        to = dev(2 * g) + 1 - core if g else dev(1)
        return pltpu.make_async_remote_copy(
            src_ref=blk, dst_ref=blk, send_sem=kv_send.at[t, g], recv_sem=kv_recv.at[t, 2 * g - 1 + core if g else 0],
            device_id={'cp': to}, device_id_type=pl.DeviceIdType.MESH)

    def kv_hand_on(t, g, c):
        blk = kv_blk(t, dev(2 * g) - core + c)
        return pltpu.make_async_remote_copy(
            src_ref=blk, dst_ref=blk, send_sem=kv_pass.at[t], recv_sem=kv_recv.at[t, 2 * g - 1 + c if g else 0],
            device_id={'cp': dev(1)}, device_id_type=pl.DeviceIdType.MESH)

    REMOTE = [(g, c) for g in (3, 1, 2) for c in (1, 0)]

    for t in range(2):
        for g in (3, 1, 2, 0):
            kv_send_own(t, g).start()

    def hand_on(t):
        @pl.when(core == 1)
        def _():
            for g, c in REMOTE:
                kv_hand_on(t, g, c).wait_recv()
                kv_hand_on(t, g, c).start()

    def wait_blocks(t):
        @pl.when(core == 0)
        def _():
            for g, c in REMOTE:
                kv_hand_on(t, g, c).wait_recv()
            kv_hand_on(t, 0, 1).wait_recv()

        @pl.when(core == 1)
        def _():
            kv_hand_on(t, 0, 0).wait_recv()

    def put_rows(dst, val, h):
        dst[0, h * PIECE:(h + 1) * PIECE, :] = val[0:PIECE]
        dst[1, h * PIECE:(h + 1) * PIECE, :] = val[PIECE:TOK]

    for h0, h1 in GROUPS:
        for c in ld_wq[:2] if h0 == 0 else ld_wq[2:]:
            c.wait()
        ld_wo[0 if h0 == 0 else 1].start()
        val = dot(x_s[...], side_by_side(wq_s, h0, h1, 0, D)).astype(BF16)
        for h in range(h0, h1):
            put_rows(q_s, val[:, (h - h0) * E:(h - h0 + 1) * E], h)
    doc_sum = rcopy(doc_s.at[1:NDEV], doc_s.at[1:NDEV], doc_send, doc_recv, 1)
    doc_sum.wait_recv()
    ld_dy.wait()
    for h0, h1 in GROUPS:
        ld_wo[0 if h0 == 0 else 1].wait()
        val = dot(dy_s[...], wo_s[h0 * E:h1 * E, :], NT).astype(BF16)
        for h in range(h0, h1):
            put_rows(do_s, val[:, (h - h0) * E:(h - h0 + 1) * E], h)
        if h0 == 0:
            my_doc = doc_ref[...].astype(F32)
            eye = (lax.broadcasted_iota(jnp.int32, (TOK, TOK), 0) == lax.broadcasted_iota(jnp.int32, (TOK, TOK), 1))
            doc_col = jnp.sum(jnp.where(eye, jnp.broadcast_to(my_doc, (TOK, TOK)), 0.0), axis=1, keepdims=True)
            less = jnp.zeros((TOK, TOK), F32)
            for d in range(NDEV):
                less = less + jnp.where(doc_s[d].astype(F32) < doc_col, 1.0, 0.0)
            first = jnp.sum(less, axis=1, keepdims=True)
            rowi = lax.broadcasted_iota(jnp.int32, (PIECE, 1), 0)
            pos_lo = (me * PIECE + rowi).astype(F32)
            pos_hi = ((2 * NDEV - 1 - me) * PIECE + rowi).astype(F32)
            lane = lax.broadcasted_iota(jnp.int32, (1, HALF), 1).astype(F32)
            kpos_lo = lane
            kpos_hi = (2 * NDEV - 1) * PIECE + lane - 2 * PIECE * jnp.floor((lane + 0.5) * (1.0 / PIECE))

            def cap_of(kpos, lo, hi):
                return jnp.where((kpos >= lo) & (kpos <= hi), jnp.inf, NEG_BIG)

            cap_s[:, 0:HALF] = cap_of(kpos_lo, first[PIECE:TOK], pos_hi)
            cap_s[:, HALF:2 * HALF] = cap_of(kpos_hi, first[PIECE:TOK], pos_hi)
            cap_s[:, 2 * HALF:3 * HALF] = cap_of(kpos_lo, first[0:PIECE], pos_lo)
            hand_on(0)
        else:
            for piece in range(2):
                qt_s[piece] = q_s[piece].T

    wait_blocks(0)

    k_scale = E ** -0.5
    exp_scale = k_scale * math.log2(math.e)
    def keys(t, a, b):
        return kv_s[t, a // HALF, a % HALF:a % HALF + (b - a), :]

    def over_keys(src, t, base, segs):
        parts = []
        for a, b in ((0, ROWS // 2), (ROWS // 2, ROWS)):
            acc = None
            for c, d in segs:
                val = dot(src[a:b, base + c:base + d], keys(t, c, d))
                acc = val if acc is None else acc + val
            parts.append(acc)
        return jnp.concatenate(parts, axis=0)

    def side(ref, rows, base, segs):
        return jnp.concatenate([ref[rows, base + c:base + d] for c, d in segs], axis=1)

    def softmax(base, segs, h):
        rb = 16 if sum(d - c for c, d in segs) > HALF else 32
        for b in range(PIECE // rb):
            rows = slice(h * PIECE + b * rb, h * PIECE + (b + 1) * rb)
            s = jnp.minimum(side(s_s, rows, base, segs), side(cap_s, slice(b * rb, (b + 1) * rb), base, segs))
            m = jnp.max(s, axis=1, keepdims=True)
            e = jnp.exp2((s - m) * exp_scale)
            l = jnp.sum(e, axis=1, keepdims=True)
            p = (e * (1.0 / l)).astype(BF16)
            at = 0
            for c, d in segs:
                p_s[rows, base + c:base + d] = p[:, at:at + d - c]
                at += d - c

    def d2d(t, half, late):
        q = slice(2 if half and late else 0, 4)
        return rcopy(acc_s.at[t, half, q, 1 - core], rb1.at[t, half, q], d2d_send.at[t, half], d2d_recv.at[t, half], 1)

    def rs(t, half, g):
        return rcopy(comb.at[t, half, g], rb2.at[t, half, g], rs_send.at[t, half, g - 1], rs_recv.at[t, half, g - 1], 2 * g)

    def add_peer(t, half, g, late):
        if half and late and g >= 2:
            comb[t, half, g] = jnp.zeros((PIECE, E), F32)
            return
        q = dev(2 * g) // 2
        comb[t, half, g] = acc_s[t, half, q, core] + rb1[t, half, q]

    def combine_direct(t, half, late):
        d2d(t, half, late).wait_recv()
        for g in (3, 1, 2, 0):
            if not (half and late and g >= 2):
                add_peer(t, half, g, late)
                if g:
                    rs(t, half, g).start()

    first_dev = lax.rem(cy + core, 2) * 4 + lax.rem(cx + 1 - core, 2) * 2 + core
    second_dev = lax.rem(cy + 1 - core, 2) * 4 + lax.rem(cx + core, 2) * 2 + core
    first_g, second_g = 1 + core, 2 - core

    def to_first(t, half, i):
        if i == 0:
            src, dst = comb.at[t, half, 3], relay.at[t, half]
        else:
            src, dst = comb.at[t, half, first_g], rb2.at[t, half, 1]
        return pltpu.make_async_remote_copy(
            src_ref=src, dst_ref=dst, send_sem=rs_send.at[t, half, i], recv_sem=rs_recv.at[t, half, i],
            device_id={'cp': first_dev}, device_id_type=pl.DeviceIdType.MESH)

    def to_second(t, half):
        return pltpu.make_async_remote_copy(
            src_ref=comb.at[t, half, second_g], dst_ref=rb2.at[t, half, 2], send_sem=rs_send.at[t, half, 2],
            recv_sem=rs_recv.at[t, half, 2], device_id={'cp': second_dev}, device_id_type=pl.DeviceIdType.MESH)

    def combine_relayed(t, half, late):
        d2d(t, half, late).wait_recv()
        add_peer(t, half, 3, late)
        to_first(t, half, 0).start()
        add_peer(t, half, 1, late)
        add_peer(t, half, 2, late)
        to_first(t, half, 1).start()
        add_peer(t, half, 0, late)

    def pass_on(t, half):
        to_first(t, half, 0).wait_recv()
        comb[t, half, second_g] = comb[t, half, second_g] + relay[t, half]
        to_second(t, half).start()

    QUART = HALF // 2

    def attention(late):
        hi = ((0, HALF), (HALF + QUART, SEQ)) if late else ((0, HALF), (HALF, SEQ))
        lo = ((0, HALF),) if late else ((0, QUART),)
        hi_blocks = [(a, min(a + 512, d)) for c, d in hi for a in range(c, d, 512)]
        lo_blocks = [(a, min(a + 512, d)) for c, d in lo for a in range(c, d, 512)]

        def grad(t, half, lhs_t, src):
            cuts = ((QUART, 512), (512, HALF)) if half and late else ((0, 256), (256, 512), (512, HALF))
            for a, b in cuts:
                c = b if late else min(b, QUART)
                if t == 0:
                    ds_rows(1, 0, ((half * HALF + a, half * HALF + b),))
                    if not half and c > a:
                        ds_rows(0, SEQ, ((a, c),))
                val = dot(lhs_t[1], src[:, half * HALF + a:half * HALF + b])
                if not half and c > a:
                    more = dot(lhs_t[0], src[:, SEQ + a:SEQ + c])
                    val = val + more if c == b else jnp.concatenate([val[:, :c - a] + more, val[:, c - a:]], axis=1)
                val = val.T
                for r in range(a - a % PIECE, b, PIECE):
                    c, d = max(a, r), min(b, r + PIECE)
                    slot = r // PIECE
                    acc_s[t, half, slot // 2, slot % 2, c - r:d - r, :] = val[c - a:d - a]
            d2d(t, half, late).start()

        def s_part(piece, base, a, b, r0=0, r1=ROWS):
            s_s[r0:r1, base + a:base + b] = dot(q_s[piece, r0:r1, :], keys(0, a, b), NT)

        def dp_part(piece, base, a, b):
            dp_s[:, base + a:base + b] = dot(do_s[piece], keys(1, a, b), NT)

        def o_part(piece, base, segs):
            o_bf = over_keys(p_s, 1, base, segs).astype(BF16)
            delta_s[piece] = jnp.sum(do_s[piece].astype(F32) * o_bf.astype(F32), axis=1, keepdims=True)
            for h in range(HEADS):
                o_s[piece * PIECE:(piece + 1) * PIECE, h * E:(h + 1) * E] = o_bf[h * PIECE:(h + 1) * PIECE]

        def ds_rows(piece, base, segs):
            for h in range(HEADS):
                for c in range(PIECE // 32):
                    r0 = h * PIECE + c * 32
                    for a, b in segs:
                        ds_s[r0:r0 + 32, base + a:base + b] = (
                            p_s[r0:r0 + 32, base + a:base + b].astype(F32)
                            * (dp_s[r0:r0 + 32, base + a:base + b] - delta_s[piece, r0:r0 + 32, :])).astype(BF16)

        def dq_part(piece, base, segs):
            dq_bf = (over_keys(ds_s, 0, base, segs) * k_scale).astype(BF16)
            for h in range(HEADS):
                dq_s[piece * PIECE:(piece + 1) * PIECE, h * E:(h + 1) * E] = dq_bf[h * PIECE:(h + 1) * PIECE]

        def softmax_with(base, segs, h0, h1, others):
            for h in range(h0, h1):
                softmax(base, segs, h)
                left = h1 - h
                take = -(-len(others) // left)
                for fn in others[:take]:
                    fn()
                others = others[take:]

        for a, b in hi_blocks:
            s_part(1, 0, a, b, 0, 192)
        for piece in range(2):
            dot_s[piece] = do_s[piece].T
        softmax_with(0, hi, 0, 2, [lambda a=a, b=b: s_part(1, 0, a, b, 192, ROWS) for a, b in hi_blocks])
        hand_on(1)
        softmax_with(0, hi, 2, HEADS, [lambda a=a, b=b: s_part(0, SEQ, a, b) for a, b in lo_blocks])
        grad(1, 1, dot_s, p_s)
        wait_blocks(1)
        softmax_with(SEQ, lo, 0, HEADS, [lambda a=a, b=b: dp_part(1, 0, a, b) for a, b in hi_blocks])
        grad(1, 0, dot_s, p_s)
        combine_direct(1, 1, late)
        o_part(1, 0, hi)
        for a, b in lo_blocks:
            dp_part(0, SEQ, a, b)
        grad(0, 1, qt_s, ds_s)
        combine_relayed(1, 0, late)
        o_part(0, SEQ, lo)
        grad(0, 0, qt_s, ds_s)
        combine_relayed(0, 1, late)
        dq_part(1, 0, hi)
        dq_part(0, SEQ, lo)

    for late in range(2):
        pl.when(cy == late)(lambda late=late: attention(late))

    combine_direct(0, 0, 0)
    NY = 896

    def y_part(a, b):
        y_s[:, a:b] = dot(o_s[...], wo_s[:, a:b]).astype(BF16)

    y_part(0, 1792)
    pass_on(1, 0)
    y_part(1792, D)
    pass_on(0, 1)
    for i in range(D // NY):
        dx_s[:, i * NY:(i + 1) * NY] = dot(dq_s[...], side_by_side(wq_s, 0, HEADS, i * NY, (i + 1) * NY), NT)

    def put_total(t, half, tot):
        if t == 0:
            tot = tot * k_scale
        dkv_s[half * PIECE:(half + 1) * PIECE, t * E:(t + 1) * E] = tot.astype(BF16)

    @pl.when(cy == 0)
    def _():
        rs(1, 1, 1).wait_recv()
        put_total(1, 1, comb[1, 1, 0] + rb2[1, 1, 1])

    @pl.when(cy == 1)
    def _():
        for g in (1, 2, 3):
            rs(1, 1, g).wait_recv()
        put_total(1, 1, (comb[1, 1, 0] + rb2[1, 1, 1]) + (rb2[1, 1, 2] + rb2[1, 1, 3]))

    for t, half in UNITS[1:3]:
        to_first(t, half, 1).wait_recv()
        to_second(t, half).wait_recv()
        put_total(t, half, comb[t, half, 0] + (rb2[t, half, 1] + rb2[t, half, 2]))
    for g in (3, 1, 2):
        rs(0, 0, g).wait_recv()
    put_total(0, 0, (comb[0, 0, 0] + rb2[0, 0, 1]) + (rb2[0, 0, 2] + rb2[0, 0, 3]))

    doc_sum.wait_send()
    for t in range(2):
        for g in range(4):
            kv_send_own(t, g).wait_send()

    @pl.when(core == 1)
    def _():
        for t in range(2):
            six = kv_s.at[t, :, 0:6 * PIECE, :]
            rcopy(six, six, kv_pass.at[t], kv_recv.at[t, 0], 1).wait_send()

    for t in range(2):
        d2d(t, 0, 0).wait_send()
    rs(1, 1, 1).wait_send()

    @pl.when(cy == 0)
    def _():
        for t in range(2):
            d2d(t, 1, 0).wait_send()
        for g in range(2, 4):
            rs(1, 1, g).wait_send()

    @pl.when(cy == 1)
    def _():
        for t in range(2):
            d2d(t, 1, 1).wait_send()

    for t, half in UNITS[1:3]:
        to_first(t, half, 0).wait_send()
        to_first(t, half, 1).wait_send()
        to_second(t, half).wait_send()
    for g in (1, 2, 3):
        rs(0, 0, g).wait_send()


FIN = ((0, 1536), (1536, 2560), (2560, 3584))


def final_kernel(y_s, dx_s, dkv_s, wkv_s, y_hbm, dx_hbm, dxo_s, y_sem, dx_sem):
    y_cp = pltpu.make_async_copy(y_s, y_hbm, y_sem)
    y_cp.start()
    copies = [y_cp]
    for i, (a, b) in enumerate(FIN):
        dxo_s[:, a:b] = (dx_s[:, a:b] + dot(dkv_s[...], side_by_side(wkv_s, 0, 2, a, b), NT)).astype(BF16)
        cp = pltpu.make_async_copy(dxo_s.at[:, a:b], dx_hbm.at[:, a:b], dx_sem.at[i])
        cp.start()
        copies.append(cp)
    for cp in copies:
        cp.wait()


def solution(mesh):
    row_spec = P(('dp', 'cp'))
    full_spec = P()
    hbm_spec = pl.BlockSpec(memory_space=pltpu.HBM)
    vmem_spec = pl.BlockSpec(memory_space=pltpu.VMEM)

    def local_layer(x_in, dy_in, doc_id, w_q, w_k, w_v, w_o):
        V = pltpu.VMEM
        dma = pltpu.SemaphoreType.DMA
        sds = jax.ShapeDtypeStruct
        hbm = lambda a: pltpu.with_memory_space_constraint(a, pltpu.HBM)
        parts = pl.pallas_call(
            main_kernel,
            out_shape=(V((TOK, D), BF16), V((TOK, D), F32), V((TOK, 2 * E), BF16), V((2, D, E), BF16)),
            in_specs=[hbm_spec, hbm_spec, hbm_spec, hbm_spec, hbm_spec, hbm_spec, hbm_spec],
            out_specs=(vmem_spec,) * 4,
            scratch_shapes=[
                V((TOK, D), BF16), V((TOK, D), BF16), V((HEADS, D, E), BF16), V((HE, D), BF16), V((1, TOK), jnp.int32),
                V((2, 2, HALF, E), BF16), V((NDEV, 1, TOK), jnp.int32),
                V((2, ROWS, E), BF16), V((2, ROWS, E), BF16), V((2, E, ROWS), BF16), V((2, E, ROWS), BF16),
                V((PIECE, 3 * HALF), F32),
                V((ROWS, 3 * HALF), F32), V((ROWS, 3 * HALF), BF16), V((ROWS, 3 * HALF), F32),
                V((ROWS, 3 * HALF), BF16),
                V((TOK, HE), BF16), V((TOK, HE), BF16), V((2, ROWS, 1), F32),
                V((2, 2, 4, 2, PIECE, E), F32),
                V((2, 2, 4, PIECE, E), F32), V((2, 2, 4, PIECE, E), F32), V((2, 2, 4, PIECE, E), F32), V((2, 2, PIECE, E), F32),
                dma((len(KPARTS), 3)), dma((3,)), dma((2,)), dma, dma,
                dma, dma, dma((2, 4)), dma((2, 7)), dma((2,)),
                dma((2, 2)), dma((2, 2)), dma((2, 2, 3)), dma((2, 2, 3)),
            ],
            compiler_params=pltpu.CompilerParams(collective_id=0, has_side_effects=True,
                                                 vmem_limit_bytes=50 * 1024 * 1024),
        )(hbm(x_in), hbm(dy_in), hbm(doc_id.reshape(1, TOK)), hbm(jnp.transpose(w_q, (1, 0, 2))), hbm(w_k.reshape(D, E)),
          hbm(w_v.reshape(D, E)), hbm(w_o.reshape(HE, D)))
        return pl.pallas_call(
            final_kernel,
            out_shape=(sds((TOK, D), BF16), sds((TOK, D), BF16)),
            in_specs=[vmem_spec] * 4,
            out_specs=(hbm_spec, hbm_spec),
            scratch_shapes=[V((TOK, D), BF16), dma, dma((len(FIN),))],
            compiler_params=pltpu.CompilerParams(vmem_limit_bytes=12 * 1024 * 1024),
        )(*[pltpu.with_memory_space_constraint(a, pltpu.VMEM) for a in parts])

    return jax.shard_map(local_layer, mesh=mesh,
                         in_specs=(row_spec, row_spec, row_spec, full_spec, full_spec, full_spec, full_spec),
                         out_specs=(row_spec, row_spec), check_vma=False)
```

```python
import math

import jax
import jax.numpy as jnp
from jax import lax
from jax.experimental import pallas as pl
from jax.experimental.pallas import tpu as pltpu
from jax.sharding import PartitionSpec as P

NEG_BIG = -1.0e30
F32 = jnp.float32
BF16 = jnp.bfloat16

NDEV = 8
HEADS = 7
E = 128
PIECE = 96
TOK = 192
D = 3584
HE = HEADS * E
ROWS = HEADS * PIECE
HALF = NDEV * PIECE
SEQ = 2 * HALF
KPARTS = ((0, 2048), (2048, D))

NT = (((1,), (1,)), ((), ()))
NN = (((1,), (0,)), ((), ()))
UNITS = ((1, 1), (1, 0), (0, 1), (0, 0))
GROUPS = ((0, 4), (4, 7))


def dot(a, b, dims=NN):
    return lax.dot_general(a, b, dims, preferred_element_type=F32)


def side_by_side(ref, h0, h1, r0, r1):
    return jnp.concatenate([ref[h, r0:r1, :] for h in range(h0, h1)], axis=1)


def main_kernel(x_hbm, dy_hbm, doc_hbm, wq_hbm, wk_hbm, wv_hbm, wo_hbm,
                y_s, dx_s, dkv_s, wkv_s,
                x_s, dy_s, wq_s, wo_s, doc_ref,
                kv_s, doc_s, q_s, do_s, qt_s, dot_s, cap_s,
                s_s, p_s, dp_s, ds_s, o_s, dq_s, delta_s,
                acc_s, rb1, comb, rb2, relay,
                in_sem, wq_sem, wo_sem, dy_sem, doc_sem,
                doc_send, doc_recv, kv_send, kv_recv, kv_pass,
                d2d_send, d2d_recv, rs_send, rs_recv, relay_recv):
    me = lax.axis_index('cp')
    core = lax.rem(me, 2)
    chip = me // 2
    cx = lax.rem(chip, 2)
    cy = chip // 2

    def dev(r):
        yy = lax.rem(cy + (r // 4), 2)
        xx = lax.rem(cx + ((r // 2) % 2), 2)
        cc = lax.rem(core + (r % 2), 2)
        return yy * 4 + xx * 2 + cc

    def rcopy(src, dst, ssem, rsem, r):
        return pltpu.make_async_remote_copy(src_ref=src, dst_ref=dst, send_sem=ssem, recv_sem=rsem,
                                            device_id={'cp': dev(r)}, device_id_type=pl.DeviceIdType.MESH)

    ld_in = []
    for i, (ka, kb) in enumerate(KPARTS):
        ks = slice(ka, kb)
        ld_in.append([pltpu.make_async_copy(x_hbm.at[:, ks], x_s.at[:, ks], in_sem.at[i, 0]),
                      pltpu.make_async_copy(wk_hbm.at[ks], wkv_s.at[0, ks], in_sem.at[i, 1]),
                      pltpu.make_async_copy(wv_hbm.at[ks], wkv_s.at[1, ks], in_sem.at[i, 2])])
    ld_dy = pltpu.make_async_copy(dy_hbm, dy_s, dy_sem)
    ld_doc = pltpu.make_async_copy(doc_hbm, doc_ref, doc_sem)
    ld_wq = [pltpu.make_async_copy(wq_hbm.at[a:b], wq_s.at[a:b], wq_sem.at[i])
             for i, (a, b) in enumerate(((0, 2), (2, 4), (4, HEADS)))]
    ld_wo = [pltpu.make_async_copy(wo_hbm.at[a * E:b * E], wo_s.at[a * E:b * E], wo_sem.at[i])
             for i, (a, b) in enumerate(GROUPS)]
    for part in ld_in + [[ld_doc], ld_wq[:1]]:
        for c in part:
            c.start()
    LATER = (ld_wq[1:2], ld_wq[2:] + [ld_dy])

    barrier = pltpu.get_barrier_semaphore()
    for r in range(1, NDEV):
        pl.semaphore_signal(barrier, inc=1, device_id={'cp': dev(r)}, device_id_type=pl.DeviceIdType.MESH)

    for i, (ka, kb) in enumerate(KPARTS):
        for c in ld_in[i]:
            c.wait()
        for c in LATER[i]:
            c.start()
        kv_part = jnp.concatenate([dot(x_s[a:a + PIECE, ka:kb], side_by_side(wkv_s, 0, 2, ka, kb))
                                   for a in (0, PIECE)], axis=0)
        if i:
            kv_part = s_s[0:TOK, 0:2 * E] + kv_part
        if i < len(KPARTS) - 1:
            s_s[0:TOK, 0:2 * E] = kv_part
        if i == 0:
            pl.semaphore_wait(barrier, NDEV - 1)
            ld_doc.wait()
            doc_s[me] = doc_ref[...]
            doc_out = {}
            for r in range(1, NDEV):
                doc_out[r] = rcopy(doc_ref, doc_s.at[me], doc_send, doc_recv, r)
                doc_out[r].start()
    kv_own = kv_part.astype(BF16)
    my_off = pl.multiple_of(me * PIECE, 32)
    for t in range(2):
        for half in range(2):
            kv_s[t, half, pl.ds(my_off, PIECE), :] = kv_own[half * PIECE:(half + 1) * PIECE, t * E:(t + 1) * E]

    def kv_blk(t, owner):
        return kv_s.at[t, :, pl.ds(pl.multiple_of(owner * PIECE, 32), PIECE), :]

    def kv_send_own(t, g):
        blk = kv_blk(t, me)
        to = dev(2 * g) + 1 - core if g else dev(1)
        return pltpu.make_async_remote_copy(
            src_ref=blk, dst_ref=blk, send_sem=kv_send.at[t], recv_sem=kv_recv.at[t, 1 if g else 0],
            device_id={'cp': to}, device_id_type=pl.DeviceIdType.MESH)

    def kv_sum(t, n):
        blks = kv_s.at[t, :, 0:n * PIECE, :]
        return rcopy(blks, blks, kv_pass.at[t], kv_recv.at[t, 1], 1)

    for t in range(2):
        for g in (3, 1, 2, 0):
            kv_send_own(t, g).start()

    def hand_on(t):
        @pl.when(core == 1)
        def _():
            kv_sum(t, 6).wait_recv()
            for g in (3, 1, 2):
                both = kv_s.at[t, :, pl.ds(pl.multiple_of((dev(2 * g) - core) * PIECE, 64), 2 * PIECE), :]
                rcopy(both, both, kv_pass.at[t], kv_recv.at[t, 1], 1).start()

    def wait_blocks(t):
        @pl.when(core == 0)
        def _():
            kv_sum(t, 6).wait_recv()
        rcopy(kv_blk(t, dev(1)), kv_blk(t, dev(1)), kv_send.at[t], kv_recv.at[t, 0], 1).wait_recv()

    def put_rows(dst, val, h):
        dst[0, h * PIECE:(h + 1) * PIECE, :] = val[0:PIECE]
        dst[1, h * PIECE:(h + 1) * PIECE, :] = val[PIECE:TOK]

    for h0, h1 in GROUPS:
        for c in ld_wq[:2] if h0 == 0 else ld_wq[2:]:
            c.wait()
        ld_wo[0 if h0 == 0 else 1].start()
        val = dot(x_s[...], side_by_side(wq_s, h0, h1, 0, D)).astype(BF16)
        for h in range(h0, h1):
            put_rows(q_s, val[:, (h - h0) * E:(h - h0 + 1) * E], h)
    doc_sum = rcopy(doc_s.at[1:NDEV], doc_s.at[1:NDEV], doc_send, doc_recv, 1)
    doc_sum.wait_recv()
    ld_dy.wait()
    for h0, h1 in GROUPS:
        ld_wo[0 if h0 == 0 else 1].wait()
        val = dot(dy_s[...], wo_s[h0 * E:h1 * E, :], NT).astype(BF16)
        for h in range(h0, h1):
            put_rows(do_s, val[:, (h - h0) * E:(h - h0 + 1) * E], h)
        if h0 == 0:
            my_doc = doc_ref[...].astype(F32)
            eye = (lax.broadcasted_iota(jnp.int32, (TOK, TOK), 0) == lax.broadcasted_iota(jnp.int32, (TOK, TOK), 1))
            doc_col = jnp.sum(jnp.where(eye, jnp.broadcast_to(my_doc, (TOK, TOK)), 0.0), axis=1, keepdims=True)
            less = jnp.zeros((TOK, TOK), F32)
            for d in range(NDEV):
                less = less + jnp.where(doc_s[d].astype(F32) < doc_col, 1.0, 0.0)
            first = jnp.sum(less, axis=1, keepdims=True)
            rowi = lax.broadcasted_iota(jnp.int32, (PIECE, 1), 0)
            pos_lo = (me * PIECE + rowi).astype(F32)
            pos_hi = ((2 * NDEV - 1 - me) * PIECE + rowi).astype(F32)
            lane = lax.broadcasted_iota(jnp.int32, (1, HALF), 1).astype(F32)
            kpos_lo = lane
            kpos_hi = (2 * NDEV - 1) * PIECE + lane - 2 * PIECE * jnp.floor((lane + 0.5) * (1.0 / PIECE))

            def cap_of(kpos, lo, hi):
                return jnp.where((kpos >= lo) & (kpos <= hi), jnp.inf, NEG_BIG)

            cap_s[:, 0:HALF] = cap_of(kpos_lo, first[PIECE:TOK], pos_hi)
            cap_s[:, HALF:2 * HALF] = cap_of(kpos_hi, first[PIECE:TOK], pos_hi)
            cap_s[:, 2 * HALF:3 * HALF] = cap_of(kpos_lo, first[0:PIECE], pos_lo)
            hand_on(0)
        else:
            for piece in range(2):
                qt_s[piece] = q_s[piece].T

    wait_blocks(0)

    k_scale = E ** -0.5
    exp_scale = k_scale * math.log2(math.e)
    def keys(t, a, b):
        return kv_s[t, a // HALF, a % HALF:a % HALF + (b - a), :]

    def over_keys(src, t, base, segs):
        parts = []
        for a, b in ((0, ROWS // 2), (ROWS // 2, ROWS)):
            acc = None
            for c, d in segs:
                val = dot(src[a:b, base + c:base + d], keys(t, c, d))
                acc = val if acc is None else acc + val
            parts.append(acc)
        return jnp.concatenate(parts, axis=0)

    def side(ref, rows, base, segs):
        return jnp.concatenate([ref[rows, base + c:base + d] for c, d in segs], axis=1)

    def softmax(base, segs, h):
        rb = 16 if sum(d - c for c, d in segs) > HALF else 32
        for b in range(PIECE // rb):
            rows = slice(h * PIECE + b * rb, h * PIECE + (b + 1) * rb)
            s = jnp.minimum(side(s_s, rows, base, segs), side(cap_s, slice(b * rb, (b + 1) * rb), base, segs))
            m = jnp.max(s, axis=1, keepdims=True)
            e = jnp.exp2((s - m) * exp_scale)
            l = jnp.sum(e, axis=1, keepdims=True)
            p = (e * (1.0 / l)).astype(BF16)
            at = 0
            for c, d in segs:
                p_s[rows, base + c:base + d] = p[:, at:at + d - c]
                at += d - c

    def d2d(t, half, late):
        q = slice(2 if half and late else 0, 4)
        return rcopy(acc_s.at[t, half, q, 1 - core], rb1.at[t, half, q], d2d_send.at[t, half], d2d_recv.at[t, half], 1)

    def rs(t, half, g):
        return rcopy(comb.at[t, half, g], rb2.at[t, half, g], rs_send.at[1 - t * half], rs_recv.at[t, half], 2 * g)

    def add_peer(t, half, g, late):
        if half and late and g >= 2:
            comb[t, half, g] = jnp.zeros((PIECE, E), F32)
            return
        q = dev(2 * g) // 2
        comb[t, half, g] = acc_s[t, half, q, core] + rb1[t, half, q]

    def rs_sum(t, half, n):
        blks = rb1.at[0, 0, 0:n]
        return rcopy(blks, blks, rs_send.at[1 - t * half], rs_recv.at[t, half], 2)

    def combine_direct(t, half, late):
        d2d(t, half, late).wait_recv()
        for g in (3, 1, 2, 0):
            if not (half and late and g >= 2):
                add_peer(t, half, g, late)
                if g:
                    rs(t, half, g).start()

    first_dev = lax.rem(cy + core, 2) * 4 + lax.rem(cx + 1 - core, 2) * 2 + core
    second_dev = lax.rem(cy + 1 - core, 2) * 4 + lax.rem(cx + core, 2) * 2 + core
    first_g, second_g = 1 + core, 2 - core

    def to_first(t, half, i):
        if i == 0:
            src, dst, sem = comb.at[t, half, 3], relay.at[t, half], relay_recv.at[t]
        else:
            src, dst, sem = comb.at[t, half, first_g], rb2.at[t, half, 1], rs_recv.at[t, half]
        return pltpu.make_async_remote_copy(
            src_ref=src, dst_ref=dst, send_sem=rs_send.at[1], recv_sem=sem,
            device_id={'cp': first_dev}, device_id_type=pl.DeviceIdType.MESH)

    def to_second(t, half):
        return pltpu.make_async_remote_copy(
            src_ref=comb.at[t, half, second_g], dst_ref=rb2.at[t, half, 2], send_sem=rs_send.at[1],
            recv_sem=rs_recv.at[t, half], device_id={'cp': second_dev}, device_id_type=pl.DeviceIdType.MESH)

    def combine_relayed(t, half, late):
        d2d(t, half, late).wait_recv()
        add_peer(t, half, 3, late)
        to_first(t, half, 0).start()
        add_peer(t, half, 1, late)
        add_peer(t, half, 2, late)
        to_first(t, half, 1).start()
        add_peer(t, half, 0, late)

    def pass_on(t, half):
        to_first(t, half, 0).wait_recv()
        comb[t, half, second_g] = comb[t, half, second_g] + relay[t, half]
        to_second(t, half).start()

    QUART = HALF // 2

    def attention(late):
        hi = ((0, HALF), (HALF + QUART, SEQ)) if late else ((0, HALF), (HALF, SEQ))
        lo = ((0, HALF),) if late else ((0, QUART),)
        hi_blocks = [(a, min(a + 512, d)) for c, d in hi for a in range(c, d, 512)]
        lo_blocks = [(a, min(a + 512, d)) for c, d in lo for a in range(c, d, 512)]

        def grad(t, half, lhs_t, src):
            cuts = ((QUART, 512), (512, HALF)) if half and late else ((0, 256), (256, 512), (512, HALF))
            for a, b in cuts:
                c = b if late else min(b, QUART)
                if t == 0:
                    ds_rows(1, 0, ((half * HALF + a, half * HALF + b),))
                    if not half and c > a:
                        ds_rows(0, SEQ, ((a, c),))
                val = dot(lhs_t[1], src[:, half * HALF + a:half * HALF + b])
                if not half and c > a:
                    more = dot(lhs_t[0], src[:, SEQ + a:SEQ + c])
                    val = val + more if c == b else jnp.concatenate([val[:, :c - a] + more, val[:, c - a:]], axis=1)
                val = val.T
                for r in range(a - a % PIECE, b, PIECE):
                    c, d = max(a, r), min(b, r + PIECE)
                    slot = r // PIECE
                    acc_s[t, half, slot // 2, slot % 2, c - r:d - r, :] = val[c - a:d - a]
            d2d(t, half, late).start()

        def s_part(piece, base, a, b, r0=0, r1=ROWS):
            s_s[r0:r1, base + a:base + b] = dot(q_s[piece, r0:r1, :], keys(0, a, b), NT)

        def dp_part(piece, base, a, b):
            dp_s[:, base + a:base + b] = dot(do_s[piece], keys(1, a, b), NT)

        def o_part(piece, base, segs):
            o_bf = over_keys(p_s, 1, base, segs).astype(BF16)
            delta_s[piece] = jnp.sum(do_s[piece].astype(F32) * o_bf.astype(F32), axis=1, keepdims=True)
            for h in range(HEADS):
                o_s[piece * PIECE:(piece + 1) * PIECE, h * E:(h + 1) * E] = o_bf[h * PIECE:(h + 1) * PIECE]

        def ds_rows(piece, base, segs):
            for h in range(HEADS):
                for c in range(PIECE // 32):
                    r0 = h * PIECE + c * 32
                    for a, b in segs:
                        ds_s[r0:r0 + 32, base + a:base + b] = (
                            p_s[r0:r0 + 32, base + a:base + b].astype(F32)
                            * (dp_s[r0:r0 + 32, base + a:base + b] - delta_s[piece, r0:r0 + 32, :])).astype(BF16)

        def dq_part(piece, base, segs):
            dq_bf = (over_keys(ds_s, 0, base, segs) * k_scale).astype(BF16)
            for h in range(HEADS):
                dq_s[piece * PIECE:(piece + 1) * PIECE, h * E:(h + 1) * E] = dq_bf[h * PIECE:(h + 1) * PIECE]

        def softmax_with(base, segs, h0, h1, others):
            for h in range(h0, h1):
                softmax(base, segs, h)
                left = h1 - h
                take = -(-len(others) // left)
                for fn in others[:take]:
                    fn()
                others = others[take:]

        for a, b in hi_blocks:
            s_part(1, 0, a, b, 0, 192)
        for piece in range(2):
            dot_s[piece] = do_s[piece].T
        softmax_with(0, hi, 0, 2, [lambda a=a, b=b: s_part(1, 0, a, b, 192, ROWS) for a, b in hi_blocks])
        hand_on(1)
        softmax_with(0, hi, 2, HEADS, [lambda a=a, b=b: s_part(0, SEQ, a, b) for a, b in lo_blocks])
        grad(1, 1, dot_s, p_s)
        wait_blocks(1)
        softmax_with(SEQ, lo, 0, HEADS, [lambda a=a, b=b: dp_part(1, 0, a, b) for a, b in hi_blocks])
        grad(1, 0, dot_s, p_s)
        combine_direct(1, 1, late)
        o_part(1, 0, hi)
        for a, b in lo_blocks:
            dp_part(0, SEQ, a, b)
        grad(0, 1, qt_s, ds_s)
        combine_relayed(1, 0, late)
        o_part(0, SEQ, lo)
        grad(0, 0, qt_s, ds_s)
        combine_relayed(0, 1, late)
        dq_part(1, 0, hi)
        dq_part(0, SEQ, lo)

    for late in range(2):
        pl.when(cy == late)(lambda late=late: attention(late))

    combine_direct(0, 0, 0)
    NY = 896

    def y_part(a, b):
        y_s[:, a:b] = dot(o_s[...], wo_s[:, a:b]).astype(BF16)

    y_part(0, 1792)
    pass_on(1, 0)
    y_part(1792, D)
    pass_on(0, 1)
    for i in range(D // NY):
        dx_s[:, i * NY:(i + 1) * NY] = dot(dq_s[...], side_by_side(wq_s, 0, HEADS, i * NY, (i + 1) * NY), NT)

    def put_total(t, half, tot):
        if t == 0:
            tot = tot * k_scale
        dkv_s[half * PIECE:(half + 1) * PIECE, t * E:(t + 1) * E] = tot.astype(BF16)

    @pl.when(cy == 0)
    def _():
        rs_sum(1, 1, 1).wait_recv()
        put_total(1, 1, comb[1, 1, 0] + rb2[1, 1, 1])

    @pl.when(cy == 1)
    def _():
        rs_sum(1, 1, 3).wait_recv()
        put_total(1, 1, (comb[1, 1, 0] + rb2[1, 1, 1]) + (rb2[1, 1, 2] + rb2[1, 1, 3]))

    for t, half in UNITS[1:3]:
        rs_sum(t, half, 2).wait_recv()
        put_total(t, half, comb[t, half, 0] + (rb2[t, half, 1] + rb2[t, half, 2]))
    rs_sum(0, 0, 3).wait_recv()
    put_total(0, 0, (comb[0, 0, 0] + rb2[0, 0, 1]) + (rb2[0, 0, 2] + rb2[0, 0, 3]))

    doc_sum.wait_send()
    for t in range(2):
        four = kv_s.at[t, :, 0:4 * PIECE, :]
        rcopy(four, four, kv_send.at[t], kv_recv.at[t, 0], 1).wait_send()

    @pl.when(core == 1)
    def _():
        for t in range(2):
            kv_sum(t, 6).wait_send()

    for t in range(2):
        d2d(t, 0, 0).wait_send()

    @pl.when(cy == 0)
    def _():
        for t in range(2):
            d2d(t, 1, 0).wait_send()
        rs_sum(1, 1, 3).wait_send()

    @pl.when(cy == 1)
    def _():
        for t in range(2):
            d2d(t, 1, 1).wait_send()
        rs_sum(1, 1, 1).wait_send()

    nine = s_s.at[0:9 * PIECE * E // (3 * HALF), :]
    rcopy(nine, nine, rs_send.at[1], rs_recv.at[0, 0], 2).wait_send()


FIN = ((0, 1536), (1536, 2560), (2560, 3584))


def final_kernel(y_s, dx_s, dkv_s, wkv_s, y_hbm, dx_hbm, dxo_s, y_sem, dx_sem):
    y_cp = pltpu.make_async_copy(y_s, y_hbm, y_sem)
    y_cp.start()
    copies = [y_cp]
    for i, (a, b) in enumerate(FIN):
        dxo_s[:, a:b] = (dx_s[:, a:b] + dot(dkv_s[...], side_by_side(wkv_s, 0, 2, a, b), NT)).astype(BF16)
        cp = pltpu.make_async_copy(dxo_s.at[:, a:b], dx_hbm.at[:, a:b], dx_sem.at[i])
        cp.start()
        copies.append(cp)
    for cp in copies:
        cp.wait()


def solution(mesh):
    row_spec = P(('dp', 'cp'))
    full_spec = P()
    hbm_spec = pl.BlockSpec(memory_space=pltpu.HBM)
    vmem_spec = pl.BlockSpec(memory_space=pltpu.VMEM)

    def local_layer(x_in, dy_in, doc_id, w_q, w_k, w_v, w_o):
        V = pltpu.VMEM
        dma = pltpu.SemaphoreType.DMA
        sds = jax.ShapeDtypeStruct
        hbm = lambda a: pltpu.with_memory_space_constraint(a, pltpu.HBM)
        parts = pl.pallas_call(
            main_kernel,
            out_shape=(V((TOK, D), BF16), V((TOK, D), F32), V((TOK, 2 * E), BF16), V((2, D, E), BF16)),
            in_specs=[hbm_spec, hbm_spec, hbm_spec, hbm_spec, hbm_spec, hbm_spec, hbm_spec],
            out_specs=(vmem_spec,) * 4,
            scratch_shapes=[
                V((TOK, D), BF16), V((TOK, D), BF16), V((HEADS, D, E), BF16), V((HE, D), BF16), V((1, TOK), jnp.int32),
                V((2, 2, HALF, E), BF16), V((NDEV, 1, TOK), jnp.int32),
                V((2, ROWS, E), BF16), V((2, ROWS, E), BF16), V((2, E, ROWS), BF16), V((2, E, ROWS), BF16),
                V((PIECE, 3 * HALF), F32),
                V((ROWS, 3 * HALF), F32), V((ROWS, 3 * HALF), BF16), V((ROWS, 3 * HALF), F32),
                V((ROWS, 3 * HALF), BF16),
                V((TOK, HE), BF16), V((TOK, HE), BF16), V((2, ROWS, 1), F32),
                V((2, 2, 4, 2, PIECE, E), F32),
                V((2, 2, 4, PIECE, E), F32), V((2, 2, 4, PIECE, E), F32), V((2, 2, 4, PIECE, E), F32), V((2, 2, PIECE, E), F32),
                dma((len(KPARTS), 3)), dma((3,)), dma((2,)), dma, dma,
                dma, dma, dma((2,)), dma((2, 2)), dma((2,)),
                dma((2, 2)), dma((2, 2)), dma((2,)), dma((2, 2)), dma((2,)),
            ],
            compiler_params=pltpu.CompilerParams(collective_id=0, has_side_effects=True,
                                                 vmem_limit_bytes=50 * 1024 * 1024),
        )(hbm(x_in), hbm(dy_in), hbm(doc_id.reshape(1, TOK)), hbm(jnp.transpose(w_q, (1, 0, 2))), hbm(w_k.reshape(D, E)),
          hbm(w_v.reshape(D, E)), hbm(w_o.reshape(HE, D)))
        return pl.pallas_call(
            final_kernel,
            out_shape=(sds((TOK, D), BF16), sds((TOK, D), BF16)),
            in_specs=[vmem_spec] * 4,
            out_specs=(hbm_spec, hbm_spec),
            scratch_shapes=[V((TOK, D), BF16), dma, dma((len(FIN),))],
            compiler_params=pltpu.CompilerParams(vmem_limit_bytes=12 * 1024 * 1024),
        )(*[pltpu.with_memory_space_constraint(a, pltpu.VMEM) for a in parts])

    return jax.shard_map(local_layer, mesh=mesh,
                         in_specs=(row_spec, row_spec, row_spec, full_spec, full_spec, full_spec, full_spec),
                         out_specs=(row_spec, row_spec), check_vma=False)
```

```python
import math

import jax
import jax.numpy as jnp
from jax import lax
from jax.experimental import pallas as pl
from jax.experimental.pallas import tpu as pltpu
from jax.sharding import PartitionSpec as P

NEG_BIG = -1.0e30
F32 = jnp.float32
BF16 = jnp.bfloat16

NDEV = 8
HEADS = 7
E = 128
PIECE = 96
TOK = 192
D = 3584
HE = HEADS * E
ROWS = HEADS * PIECE
HALF = NDEV * PIECE
SEQ = 2 * HALF
KPARTS = ((0, 2048), (2048, D))

NT = (((1,), (1,)), ((), ()))
NN = (((1,), (0,)), ((), ()))
UNITS = ((1, 1), (1, 0), (0, 1), (0, 0))
GROUPS = ((0, 4), (4, 7))


def dot(a, b, dims=NN):
    return lax.dot_general(a, b, dims, preferred_element_type=F32)


def side_by_side(ref, h0, h1, r0, r1):
    return jnp.concatenate([ref[h, r0:r1, :] for h in range(h0, h1)], axis=1)


def main_kernel(x_hbm, dy_hbm, doc_hbm, wq_hbm, wk_hbm, wv_hbm, wo_hbm,
                y_s, dx_s, dkv_s, wkv_s,
                x_s, dy_s, wq_s, wo_s, doc_ref,
                kv_s, doc_s, q_s, do_s, qt_s, dot_s, cap_s,
                s_s, p_s, dp_s, ds_s, o_s, dq_s, delta_s,
                acc_s, rb1, comb, rb2, relay,
                in_sem, wq_sem, wo_sem, dy_sem, doc_sem,
                doc_send, doc_recv, kv_send, kv_recv, kv_pass,
                d2d_send, d2d_recv, rs_send, rs_recv, relay_recv):
    me = lax.axis_index('cp')
    core = lax.rem(me, 2)
    chip = me // 2
    cx = lax.rem(chip, 2)
    cy = chip // 2

    def dev(r):
        yy = lax.rem(cy + (r // 4), 2)
        xx = lax.rem(cx + ((r // 2) % 2), 2)
        cc = lax.rem(core + (r % 2), 2)
        return yy * 4 + xx * 2 + cc

    def rcopy(src, dst, ssem, rsem, r):
        return pltpu.make_async_remote_copy(src_ref=src, dst_ref=dst, send_sem=ssem, recv_sem=rsem,
                                            device_id={'cp': dev(r)}, device_id_type=pl.DeviceIdType.MESH)

    ld_in = []
    for i, (ka, kb) in enumerate(KPARTS):
        ks = slice(ka, kb)
        ld_in.append([pltpu.make_async_copy(x_hbm.at[:, ks], x_s.at[:, ks], in_sem.at[i, 0]),
                      pltpu.make_async_copy(wk_hbm.at[ks], wkv_s.at[0, ks], in_sem.at[i, 1]),
                      pltpu.make_async_copy(wv_hbm.at[ks], wkv_s.at[1, ks], in_sem.at[i, 2])])
    ld_dy = pltpu.make_async_copy(dy_hbm, dy_s, dy_sem)
    ld_doc = pltpu.make_async_copy(doc_hbm, doc_ref, doc_sem)
    ld_wq = [pltpu.make_async_copy(wq_hbm.at[a:b], wq_s.at[a:b], wq_sem.at[i])
             for i, (a, b) in enumerate(((0, 2), (2, 4), (4, HEADS)))]
    ld_wo = [pltpu.make_async_copy(wo_hbm.at[a * E:b * E], wo_s.at[a * E:b * E], wo_sem.at[i])
             for i, (a, b) in enumerate(GROUPS)]
    for part in ld_in + [[ld_doc], ld_wq[:1]]:
        for c in part:
            c.start()
    LATER = (ld_wq[1:2], ld_wq[2:] + [ld_dy])

    barrier = pltpu.get_barrier_semaphore()
    for r in range(1, NDEV):
        pl.semaphore_signal(barrier, inc=1, device_id={'cp': dev(r)}, device_id_type=pl.DeviceIdType.MESH)

    for i, (ka, kb) in enumerate(KPARTS):
        for c in ld_in[i]:
            c.wait()
        for c in LATER[i]:
            c.start()
        kv_part = jnp.concatenate([dot(x_s[a:a + PIECE, ka:kb], side_by_side(wkv_s, 0, 2, ka, kb))
                                   for a in (0, PIECE)], axis=0)
        if i:
            kv_part = s_s[0:TOK, 0:2 * E] + kv_part
        if i < len(KPARTS) - 1:
            s_s[0:TOK, 0:2 * E] = kv_part
        if i == 0:
            pl.semaphore_wait(barrier, NDEV - 1)
            ld_doc.wait()
            doc_s[me] = doc_ref[...]
            doc_out = {}
            for r in range(1, NDEV):
                doc_out[r] = rcopy(doc_ref, doc_s.at[me], doc_send, doc_recv, r)
                doc_out[r].start()
    kv_own = kv_part.astype(BF16)
    my_off = pl.multiple_of(me * PIECE, 32)
    for t in range(2):
        for half in range(2):
            kv_s[t, half, pl.ds(my_off, PIECE), :] = kv_own[half * PIECE:(half + 1) * PIECE, t * E:(t + 1) * E]

    def kv_blk(t, owner):
        return kv_s.at[t, :, pl.ds(pl.multiple_of(owner * PIECE, 32), PIECE), :]

    def kv_send_own(t, g):
        blk = kv_blk(t, me)
        to = dev(2 * g) + 1 - core if g else dev(1)
        return pltpu.make_async_remote_copy(
            src_ref=blk, dst_ref=blk, send_sem=kv_send.at[t], recv_sem=kv_recv.at[t, 1 if g else 0],
            device_id={'cp': to}, device_id_type=pl.DeviceIdType.MESH)

    def kv_sum(t, n):
        blks = kv_s.at[t, :, 0:n * PIECE, :]
        return rcopy(blks, blks, kv_pass.at[t], kv_recv.at[t, 1], 1)

    for t in range(2):
        for g in (1, 2, 3, 0):
            kv_send_own(t, g).start()

    def hand_on(t):
        @pl.when(core == 1)
        def _():
            kv_sum(t, 6).wait_recv()
            for g in (3, 1, 2):
                both = kv_s.at[t, :, pl.ds(pl.multiple_of((dev(2 * g) - core) * PIECE, 64), 2 * PIECE), :]
                rcopy(both, both, kv_pass.at[t], kv_recv.at[t, 1], 1).start()

    def wait_blocks(t):
        @pl.when(core == 0)
        def _():
            kv_sum(t, 6).wait_recv()
        rcopy(kv_blk(t, dev(1)), kv_blk(t, dev(1)), kv_send.at[t], kv_recv.at[t, 0], 1).wait_recv()

    def put_rows(dst, val, h):
        dst[0, h * PIECE:(h + 1) * PIECE, :] = val[0:PIECE]
        dst[1, h * PIECE:(h + 1) * PIECE, :] = val[PIECE:TOK]

    for h0, h1 in GROUPS:
        for c in ld_wq[:2] if h0 == 0 else ld_wq[2:]:
            c.wait()
        ld_wo[0 if h0 == 0 else 1].start()
        val = dot(x_s[...], side_by_side(wq_s, h0, h1, 0, D)).astype(BF16)
        for h in range(h0, h1):
            put_rows(q_s, val[:, (h - h0) * E:(h - h0 + 1) * E], h)
    doc_sum = rcopy(doc_s.at[1:NDEV], doc_s.at[1:NDEV], doc_send, doc_recv, 1)
    doc_sum.wait_recv()
    ld_dy.wait()
    for h0, h1 in GROUPS:
        ld_wo[0 if h0 == 0 else 1].wait()
        val = dot(dy_s[...], wo_s[h0 * E:h1 * E, :], NT).astype(BF16)
        for h in range(h0, h1):
            put_rows(do_s, val[:, (h - h0) * E:(h - h0 + 1) * E], h)
        if h0 == 0:
            my_doc = doc_ref[...].astype(F32)
            eye = (lax.broadcasted_iota(jnp.int32, (TOK, TOK), 0) == lax.broadcasted_iota(jnp.int32, (TOK, TOK), 1))
            doc_col = jnp.sum(jnp.where(eye, jnp.broadcast_to(my_doc, (TOK, TOK)), 0.0), axis=1, keepdims=True)
            less = jnp.zeros((TOK, TOK), F32)
            for d in range(NDEV):
                less = less + jnp.where(doc_s[d].astype(F32) < doc_col, 1.0, 0.0)
            first = jnp.sum(less, axis=1, keepdims=True)
            rowi = lax.broadcasted_iota(jnp.int32, (PIECE, 1), 0)
            pos_lo = (me * PIECE + rowi).astype(F32)
            pos_hi = ((2 * NDEV - 1 - me) * PIECE + rowi).astype(F32)
            lane = lax.broadcasted_iota(jnp.int32, (1, HALF), 1).astype(F32)
            kpos_lo = lane
            kpos_hi = (2 * NDEV - 1) * PIECE + lane - 2 * PIECE * jnp.floor((lane + 0.5) * (1.0 / PIECE))

            def cap_of(kpos, lo, hi):
                return jnp.where((kpos >= lo) & (kpos <= hi), jnp.inf, NEG_BIG)

            cap_s[:, 0:HALF] = cap_of(kpos_lo, first[PIECE:TOK], pos_hi)
            cap_s[:, HALF:2 * HALF] = cap_of(kpos_hi, first[PIECE:TOK], pos_hi)
            cap_s[:, 2 * HALF:3 * HALF] = cap_of(kpos_lo, first[0:PIECE], pos_lo)
            hand_on(0)
        else:
            for piece in range(2):
                qt_s[piece] = q_s[piece].T

    wait_blocks(0)

    k_scale = E ** -0.5
    exp_scale = k_scale * math.log2(math.e)
    def keys(t, a, b):
        return kv_s[t, a // HALF, a % HALF:a % HALF + (b - a), :]

    def over_keys(src, t, base, segs):
        parts = []
        for a, b in ((0, ROWS // 2), (ROWS // 2, ROWS)):
            acc = None
            for c, d in segs:
                val = dot(src[a:b, base + c:base + d], keys(t, c, d))
                acc = val if acc is None else acc + val
            parts.append(acc)
        return jnp.concatenate(parts, axis=0)

    def side(ref, rows, base, segs):
        return jnp.concatenate([ref[rows, base + c:base + d] for c, d in segs], axis=1)

    def softmax(base, segs, h):
        rb = 16 if sum(d - c for c, d in segs) > HALF else 32
        for b in range(PIECE // rb):
            rows = slice(h * PIECE + b * rb, h * PIECE + (b + 1) * rb)
            s = jnp.minimum(side(s_s, rows, base, segs), side(cap_s, slice(b * rb, (b + 1) * rb), base, segs))
            m = jnp.max(s, axis=1, keepdims=True)
            e = jnp.exp2((s - m) * exp_scale)
            l = jnp.sum(e, axis=1, keepdims=True)
            p = (e * (1.0 / l)).astype(BF16)
            at = 0
            for c, d in segs:
                p_s[rows, base + c:base + d] = p[:, at:at + d - c]
                at += d - c

    def d2d(t, half, late):
        q = slice(2 if half and late else 0, 4)
        return rcopy(acc_s.at[t, half, q, 1 - core], rb1.at[t, half, q], d2d_send.at[t, half], d2d_recv.at[t, half], 1)

    def rs(t, half, g):
        return rcopy(comb.at[t, half, g], rb2.at[t, half, g], rs_send.at[1 - t * half], rs_recv.at[t, half], 2 * g)

    def add_peer(t, half, g, late):
        if half and late and g >= 2:
            comb[t, half, g] = jnp.zeros((PIECE, E), F32)
            return
        q = dev(2 * g) // 2
        comb[t, half, g] = acc_s[t, half, q, core] + rb1[t, half, q]

    def rs_sum(t, half, n):
        blks = rb1.at[0, 0, 0:n]
        return rcopy(blks, blks, rs_send.at[1 - t * half], rs_recv.at[t, half], 2)

    def combine_direct(t, half, late):
        d2d(t, half, late).wait_recv()
        for g in (3, 1, 2, 0):
            if not (half and late and g >= 2):
                add_peer(t, half, g, late)
                if g:
                    rs(t, half, g).start()

    first_dev = lax.rem(cy + core, 2) * 4 + lax.rem(cx + 1 - core, 2) * 2 + core
    second_dev = lax.rem(cy + 1 - core, 2) * 4 + lax.rem(cx + core, 2) * 2 + core
    first_g, second_g = 1 + core, 2 - core

    def to_first(t, half, i):
        if i == 0:
            src, dst, sem = comb.at[t, half, 3], relay.at[t, half], relay_recv.at[t]
        else:
            src, dst, sem = comb.at[t, half, first_g], rb2.at[t, half, 1], rs_recv.at[t, half]
        return pltpu.make_async_remote_copy(
            src_ref=src, dst_ref=dst, send_sem=rs_send.at[1], recv_sem=sem,
            device_id={'cp': first_dev}, device_id_type=pl.DeviceIdType.MESH)

    def to_second(t, half):
        return pltpu.make_async_remote_copy(
            src_ref=comb.at[t, half, second_g], dst_ref=rb2.at[t, half, 2], send_sem=rs_send.at[1],
            recv_sem=rs_recv.at[t, half], device_id={'cp': second_dev}, device_id_type=pl.DeviceIdType.MESH)

    def combine_relayed(t, half, late):
        d2d(t, half, late).wait_recv()
        add_peer(t, half, 3, late)
        to_first(t, half, 0).start()
        add_peer(t, half, 1, late)
        add_peer(t, half, 2, late)
        to_first(t, half, 1).start()
        add_peer(t, half, 0, late)

    def pass_on(t, half):
        to_first(t, half, 0).wait_recv()
        comb[t, half, second_g] = comb[t, half, second_g] + relay[t, half]
        to_second(t, half).start()

    QUART = HALF // 2

    def attention(late):
        hi = ((0, HALF), (HALF + QUART, SEQ)) if late else ((0, HALF), (HALF, SEQ))
        lo = ((0, HALF),) if late else ((0, QUART),)
        hi_blocks = [(a, min(a + 512, d)) for c, d in hi for a in range(c, d, 512)]
        lo_blocks = [(a, min(a + 512, d)) for c, d in lo for a in range(c, d, 512)]

        def grad(t, half, lhs_t, src):
            cuts = ((QUART, 512), (512, HALF)) if half and late else ((0, 256), (256, 512), (512, HALF))
            for a, b in cuts:
                c = b if late else min(b, QUART)
                if t == 0:
                    ds_rows(1, 0, ((half * HALF + a, half * HALF + b),))
                    if not half and c > a:
                        ds_rows(0, SEQ, ((a, c),))
                val = dot(lhs_t[1], src[:, half * HALF + a:half * HALF + b])
                if not half and c > a:
                    more = dot(lhs_t[0], src[:, SEQ + a:SEQ + c])
                    val = val + more if c == b else jnp.concatenate([val[:, :c - a] + more, val[:, c - a:]], axis=1)
                val = val.T
                for r in range(a - a % PIECE, b, PIECE):
                    c, d = max(a, r), min(b, r + PIECE)
                    slot = r // PIECE
                    acc_s[t, half, slot // 2, slot % 2, c - r:d - r, :] = val[c - a:d - a]
            d2d(t, half, late).start()

        def s_part(piece, base, a, b, r0=0, r1=ROWS):
            s_s[r0:r1, base + a:base + b] = dot(q_s[piece, r0:r1, :], keys(0, a, b), NT)

        def dp_part(piece, base, a, b):
            dp_s[:, base + a:base + b] = dot(do_s[piece], keys(1, a, b), NT)

        def o_part(piece, base, segs):
            o_bf = over_keys(p_s, 1, base, segs).astype(BF16)
            delta_s[piece] = jnp.sum(do_s[piece].astype(F32) * o_bf.astype(F32), axis=1, keepdims=True)
            for h in range(HEADS):
                o_s[piece * PIECE:(piece + 1) * PIECE, h * E:(h + 1) * E] = o_bf[h * PIECE:(h + 1) * PIECE]

        def ds_rows(piece, base, segs):
            for h in range(HEADS):
                for c in range(PIECE // 32):
                    r0 = h * PIECE + c * 32
                    for a, b in segs:
                        ds_s[r0:r0 + 32, base + a:base + b] = (
                            p_s[r0:r0 + 32, base + a:base + b].astype(F32)
                            * (dp_s[r0:r0 + 32, base + a:base + b] - delta_s[piece, r0:r0 + 32, :])).astype(BF16)

        def dq_part(piece, base, segs):
            dq_bf = (over_keys(ds_s, 0, base, segs) * k_scale).astype(BF16)
            for h in range(HEADS):
                dq_s[piece * PIECE:(piece + 1) * PIECE, h * E:(h + 1) * E] = dq_bf[h * PIECE:(h + 1) * PIECE]

        def softmax_with(base, segs, h0, h1, others):
            for h in range(h0, h1):
                softmax(base, segs, h)
                left = h1 - h
                take = -(-len(others) // left)
                for fn in others[:take]:
                    fn()
                others = others[take:]

        for a, b in hi_blocks:
            s_part(1, 0, a, b, 0, 192)
        for piece in range(2):
            dot_s[piece] = do_s[piece].T
        softmax_with(0, hi, 0, 2, [lambda a=a, b=b: s_part(1, 0, a, b, 192, ROWS) for a, b in hi_blocks])
        hand_on(1)
        softmax_with(0, hi, 2, HEADS, [lambda a=a, b=b: s_part(0, SEQ, a, b) for a, b in lo_blocks])
        grad(1, 1, dot_s, p_s)
        wait_blocks(1)
        softmax_with(SEQ, lo, 0, HEADS, [lambda a=a, b=b: dp_part(1, 0, a, b) for a, b in hi_blocks])
        grad(1, 0, dot_s, p_s)
        combine_direct(1, 1, late)
        o_part(1, 0, hi)
        for a, b in lo_blocks:
            dp_part(0, SEQ, a, b)
        grad(0, 1, qt_s, ds_s)
        combine_relayed(1, 0, late)
        o_part(0, SEQ, lo)
        grad(0, 0, qt_s, ds_s)
        combine_relayed(0, 1, late)
        dq_part(1, 0, hi)
        dq_part(0, SEQ, lo)

    for late in range(2):
        pl.when(cy == late)(lambda late=late: attention(late))

    combine_direct(0, 0, 0)
    NY = 896

    def y_part(a, b):
        y_s[:, a:b] = dot(o_s[...], wo_s[:, a:b]).astype(BF16)

    y_part(0, 1792)
    pass_on(1, 0)
    y_part(1792, D)
    pass_on(0, 1)
    for i in range(D // NY):
        dx_s[:, i * NY:(i + 1) * NY] = dot(dq_s[...], side_by_side(wq_s, 0, HEADS, i * NY, (i + 1) * NY), NT)

    def put_total(t, half, tot):
        if t == 0:
            tot = tot * k_scale
        dkv_s[half * PIECE:(half + 1) * PIECE, t * E:(t + 1) * E] = tot.astype(BF16)

    @pl.when(cy == 0)
    def _():
        rs_sum(1, 1, 1).wait_recv()
        put_total(1, 1, comb[1, 1, 0] + rb2[1, 1, 1])

    @pl.when(cy == 1)
    def _():
        rs_sum(1, 1, 3).wait_recv()
        put_total(1, 1, (comb[1, 1, 0] + rb2[1, 1, 1]) + (rb2[1, 1, 2] + rb2[1, 1, 3]))

    for t, half in UNITS[1:3]:
        rs_sum(t, half, 2).wait_recv()
        put_total(t, half, comb[t, half, 0] + (rb2[t, half, 1] + rb2[t, half, 2]))
    rs_sum(0, 0, 3).wait_recv()
    put_total(0, 0, (comb[0, 0, 0] + rb2[0, 0, 1]) + (rb2[0, 0, 2] + rb2[0, 0, 3]))

    doc_sum.wait_send()
    for t in range(2):
        four = kv_s.at[t, :, 0:4 * PIECE, :]
        rcopy(four, four, kv_send.at[t], kv_recv.at[t, 0], 1).wait_send()

    @pl.when(core == 1)
    def _():
        for t in range(2):
            kv_sum(t, 6).wait_send()

    for t in range(2):
        d2d(t, 0, 0).wait_send()

    @pl.when(cy == 0)
    def _():
        for t in range(2):
            d2d(t, 1, 0).wait_send()
        rs_sum(1, 1, 3).wait_send()

    @pl.when(cy == 1)
    def _():
        for t in range(2):
            d2d(t, 1, 1).wait_send()
        rs_sum(1, 1, 1).wait_send()

    nine = s_s.at[0:9 * PIECE * E // (3 * HALF), :]
    rcopy(nine, nine, rs_send.at[1], rs_recv.at[0, 0], 2).wait_send()


FIN = ((0, 1536), (1536, 2560), (2560, 3584))


def final_kernel(y_s, dx_s, dkv_s, wkv_s, y_hbm, dx_hbm, dxo_s, y_sem, dx_sem):
    y_cp = pltpu.make_async_copy(y_s, y_hbm, y_sem)
    y_cp.start()
    copies = [y_cp]
    for i, (a, b) in enumerate(FIN):
        dxo_s[:, a:b] = (dx_s[:, a:b] + dot(dkv_s[...], side_by_side(wkv_s, 0, 2, a, b), NT)).astype(BF16)
        cp = pltpu.make_async_copy(dxo_s.at[:, a:b], dx_hbm.at[:, a:b], dx_sem.at[i])
        cp.start()
        copies.append(cp)
    for cp in copies:
        cp.wait()


def solution(mesh):
    row_spec = P(('dp', 'cp'))
    full_spec = P()
    hbm_spec = pl.BlockSpec(memory_space=pltpu.HBM)
    vmem_spec = pl.BlockSpec(memory_space=pltpu.VMEM)

    def local_layer(x_in, dy_in, doc_id, w_q, w_k, w_v, w_o):
        V = pltpu.VMEM
        dma = pltpu.SemaphoreType.DMA
        sds = jax.ShapeDtypeStruct
        hbm = lambda a: pltpu.with_memory_space_constraint(a, pltpu.HBM)
        parts = pl.pallas_call(
            main_kernel,
            out_shape=(V((TOK, D), BF16), V((TOK, D), F32), V((TOK, 2 * E), BF16), V((2, D, E), BF16)),
            in_specs=[hbm_spec, hbm_spec, hbm_spec, hbm_spec, hbm_spec, hbm_spec, hbm_spec],
            out_specs=(vmem_spec,) * 4,
            scratch_shapes=[
                V((TOK, D), BF16), V((TOK, D), BF16), V((HEADS, D, E), BF16), V((HE, D), BF16), V((1, TOK), jnp.int32),
                V((2, 2, HALF, E), BF16), V((NDEV, 1, TOK), jnp.int32),
                V((2, ROWS, E), BF16), V((2, ROWS, E), BF16), V((2, E, ROWS), BF16), V((2, E, ROWS), BF16),
                V((PIECE, 3 * HALF), F32),
                V((ROWS, 3 * HALF), F32), V((ROWS, 3 * HALF), BF16), V((ROWS, 3 * HALF), F32),
                V((ROWS, 3 * HALF), BF16),
                V((TOK, HE), BF16), V((TOK, HE), BF16), V((2, ROWS, 1), F32),
                V((2, 2, 4, 2, PIECE, E), F32),
                V((2, 2, 4, PIECE, E), F32), V((2, 2, 4, PIECE, E), F32), V((2, 2, 4, PIECE, E), F32), V((2, 2, PIECE, E), F32),
                dma((len(KPARTS), 3)), dma((3,)), dma((2,)), dma, dma,
                dma, dma, dma((2,)), dma((2, 2)), dma((2,)),
                dma((2, 2)), dma((2, 2)), dma((2,)), dma((2, 2)), dma((2,)),
            ],
            compiler_params=pltpu.CompilerParams(collective_id=0, has_side_effects=True,
                                                 vmem_limit_bytes=50 * 1024 * 1024),
        )(hbm(x_in), hbm(dy_in), hbm(doc_id.reshape(1, TOK)), hbm(jnp.transpose(w_q, (1, 0, 2))), hbm(w_k.reshape(D, E)),
          hbm(w_v.reshape(D, E)), hbm(w_o.reshape(HE, D)))
        return pl.pallas_call(
            final_kernel,
            out_shape=(sds((TOK, D), BF16), sds((TOK, D), BF16)),
            in_specs=[vmem_spec] * 4,
            out_specs=(hbm_spec, hbm_spec),
            scratch_shapes=[V((TOK, D), BF16), dma, dma((len(FIN),))],
            compiler_params=pltpu.CompilerParams(vmem_limit_bytes=12 * 1024 * 1024),
        )(*[pltpu.with_memory_space_constraint(a, pltpu.VMEM) for a in parts])

    return jax.shard_map(local_layer, mesh=mesh,
                         in_specs=(row_spec, row_spec, row_spec, full_spec, full_spec, full_spec, full_spec),
                         out_specs=(row_spec, row_spec), check_vma=False)
```

```python
import math

import jax
import jax.numpy as jnp
from jax import lax
from jax.experimental import pallas as pl
from jax.experimental.pallas import tpu as pltpu
from jax.sharding import PartitionSpec as P

NEG_BIG = -1.0e30
F32 = jnp.float32
BF16 = jnp.bfloat16

NDEV = 8
HEADS = 7
E = 128
PIECE = 96
TOK = 192
D = 3584
HE = HEADS * E
ROWS = HEADS * PIECE
HALF = NDEV * PIECE
SEQ = 2 * HALF
KPARTS = ((0, 2048), (2048, D))

NT = (((1,), (1,)), ((), ()))
NN = (((1,), (0,)), ((), ()))
UNITS = ((1, 1), (1, 0), (0, 1), (0, 0))
GROUPS = ((0, 4), (4, 7))


def dot(a, b, dims=NN):
    return lax.dot_general(a, b, dims, preferred_element_type=F32)


def side_by_side(ref, h0, h1, r0, r1):
    return jnp.concatenate([ref[h, r0:r1, :] for h in range(h0, h1)], axis=1)


def main_kernel(x_hbm, dy_hbm, doc_hbm, wq_hbm, wk_hbm, wv_hbm, wo_hbm,
                y_s, dx_s, dkv_s, wkv_s,
                x_s, dy_s, wq_s, wo_s, doc_ref,
                kv_s, doc_s, q_s, do_s, qt_s, dot_s, cap_s,
                s_s, p_s, dp_s, ds_s, o_s, dq_s, delta_s,
                acc_s, rb1, comb, rb2, relay,
                in_sem, wq_sem, wo_sem, dy_sem, doc_sem,
                doc_send, doc_recv, kv_send, kv_recv, kv_pass,
                d2d_send, d2d_recv, rs_send, rs_recv, relay_recv):
    me = lax.axis_index('cp')
    core = lax.rem(me, 2)
    chip = me // 2
    cx = lax.rem(chip, 2)
    cy = chip // 2

    def dev(r):
        yy = lax.rem(cy + (r // 4), 2)
        xx = lax.rem(cx + ((r // 2) % 2), 2)
        cc = lax.rem(core + (r % 2), 2)
        return yy * 4 + xx * 2 + cc

    def rcopy(src, dst, ssem, rsem, r):
        return pltpu.make_async_remote_copy(src_ref=src, dst_ref=dst, send_sem=ssem, recv_sem=rsem,
                                            device_id={'cp': dev(r)}, device_id_type=pl.DeviceIdType.MESH)

    ld_in = []
    for i, (ka, kb) in enumerate(KPARTS):
        ks = slice(ka, kb)
        ld_in.append([pltpu.make_async_copy(x_hbm.at[:, ks], x_s.at[:, ks], in_sem.at[i, 0]),
                      pltpu.make_async_copy(wk_hbm.at[ks], wkv_s.at[0, ks], in_sem.at[i, 1]),
                      pltpu.make_async_copy(wv_hbm.at[ks], wkv_s.at[1, ks], in_sem.at[i, 2])])
    ld_dy = pltpu.make_async_copy(dy_hbm, dy_s, dy_sem)
    ld_doc = pltpu.make_async_copy(doc_hbm, doc_ref, doc_sem)
    ld_wq = [pltpu.make_async_copy(wq_hbm.at[a:b], wq_s.at[a:b], wq_sem.at[i])
             for i, (a, b) in enumerate(((0, 2), (2, 4), (4, HEADS)))]
    ld_wo = [pltpu.make_async_copy(wo_hbm.at[a * E:b * E], wo_s.at[a * E:b * E], wo_sem.at[i])
             for i, (a, b) in enumerate(GROUPS)]
    for part in ld_in + [[ld_doc], ld_wq[:1]]:
        for c in part:
            c.start()
    LATER = (ld_wq[1:2], ld_wq[2:] + [ld_dy])

    barrier = pltpu.get_barrier_semaphore()
    for r in range(1, NDEV):
        pl.semaphore_signal(barrier, inc=1, device_id={'cp': dev(r)}, device_id_type=pl.DeviceIdType.MESH)

    for i, (ka, kb) in enumerate(KPARTS):
        for c in ld_in[i]:
            c.wait()
        for c in LATER[i]:
            c.start()
        kv_part = jnp.concatenate([dot(x_s[a:a + PIECE, ka:kb], side_by_side(wkv_s, 0, 2, ka, kb))
                                   for a in (0, PIECE)], axis=0)
        if i:
            kv_part = s_s[0:TOK, 0:2 * E] + kv_part
        if i < len(KPARTS) - 1:
            s_s[0:TOK, 0:2 * E] = kv_part
        if i == 0:
            pl.semaphore_wait(barrier, NDEV - 1)
            ld_doc.wait()
            doc_s[me] = doc_ref[...]
            doc_out = {}
            for r in range(1, NDEV):
                doc_out[r] = rcopy(doc_ref, doc_s.at[me], doc_send, doc_recv, r)
                doc_out[r].start()
    kv_own = kv_part.astype(BF16)
    my_off = pl.multiple_of(me * PIECE, 32)
    for t in range(2):
        for half in range(2):
            kv_s[t, half, pl.ds(my_off, PIECE), :] = kv_own[half * PIECE:(half + 1) * PIECE, t * E:(t + 1) * E]

    def kv_blk(t, owner):
        return kv_s.at[t, :, pl.ds(pl.multiple_of(owner * PIECE, 32), PIECE), :]

    def kv_send_own(t, g):
        blk = kv_blk(t, me)
        to = dev(2 * g) + 1 - core if g else dev(1)
        return pltpu.make_async_remote_copy(
            src_ref=blk, dst_ref=blk, send_sem=kv_send.at[t], recv_sem=kv_recv.at[t, 1 if g else 0],
            device_id={'cp': to}, device_id_type=pl.DeviceIdType.MESH)

    def kv_sum(t, n):
        blks = kv_s.at[t, :, 0:n * PIECE, :]
        return rcopy(blks, blks, kv_pass.at[t], kv_recv.at[t, 1], 1)

    for t in range(2):
        for g in (1, 2, 3, 0):
            kv_send_own(t, g).start()

    def hand_on(t):
        @pl.when(core == 1)
        def _():
            kv_sum(t, 6).wait_recv()
            for g in (3, 1, 2):
                both = kv_s.at[t, :, pl.ds(pl.multiple_of((dev(2 * g) - core) * PIECE, 64), 2 * PIECE), :]
                rcopy(both, both, kv_pass.at[t], kv_recv.at[t, 1], 1).start()

    def wait_blocks(t):
        @pl.when(core == 0)
        def _():
            kv_sum(t, 6).wait_recv()
        rcopy(kv_blk(t, dev(1)), kv_blk(t, dev(1)), kv_send.at[t], kv_recv.at[t, 0], 1).wait_recv()

    def put_rows(dst, val, h):
        dst[0, h * PIECE:(h + 1) * PIECE, :] = val[0:PIECE]
        dst[1, h * PIECE:(h + 1) * PIECE, :] = val[PIECE:TOK]

    for h0, h1 in GROUPS:
        for c in ld_wq[:2] if h0 == 0 else ld_wq[2:]:
            c.wait()
        ld_wo[0 if h0 == 0 else 1].start()
        val = dot(x_s[...], side_by_side(wq_s, h0, h1, 0, D)).astype(BF16)
        for h in range(h0, h1):
            put_rows(q_s, val[:, (h - h0) * E:(h - h0 + 1) * E], h)
    doc_sum = rcopy(doc_s.at[1:NDEV], doc_s.at[1:NDEV], doc_send, doc_recv, 1)
    doc_sum.wait_recv()
    ld_dy.wait()
    for h0, h1 in GROUPS:
        ld_wo[0 if h0 == 0 else 1].wait()
        val = dot(dy_s[...], wo_s[h0 * E:h1 * E, :], NT).astype(BF16)
        for h in range(h0, h1):
            put_rows(do_s, val[:, (h - h0) * E:(h - h0 + 1) * E], h)
        if h0 == 0:
            my_doc = doc_ref[...].astype(F32)
            eye = (lax.broadcasted_iota(jnp.int32, (TOK, TOK), 0) == lax.broadcasted_iota(jnp.int32, (TOK, TOK), 1))
            doc_col = jnp.sum(jnp.where(eye, jnp.broadcast_to(my_doc, (TOK, TOK)), 0.0), axis=1, keepdims=True)
            less = jnp.zeros((TOK, TOK), F32)
            for d in range(NDEV):
                less = less + jnp.where(doc_s[d].astype(F32) < doc_col, 1.0, 0.0)
            first = jnp.sum(less, axis=1, keepdims=True)
            rowi = lax.broadcasted_iota(jnp.int32, (PIECE, 1), 0)
            pos_lo = (me * PIECE + rowi).astype(F32)
            pos_hi = ((2 * NDEV - 1 - me) * PIECE + rowi).astype(F32)
            lane = lax.broadcasted_iota(jnp.int32, (1, HALF), 1).astype(F32)
            kpos_lo = lane
            kpos_hi = (2 * NDEV - 1) * PIECE + lane - 2 * PIECE * jnp.floor((lane + 0.5) * (1.0 / PIECE))

            def cap_of(kpos, lo, hi):
                return jnp.where((kpos >= lo) & (kpos <= hi), jnp.inf, NEG_BIG)

            cap_s[:, 0:HALF] = cap_of(kpos_lo, first[PIECE:TOK], pos_hi)
            cap_s[:, HALF:2 * HALF] = cap_of(kpos_hi, first[PIECE:TOK], pos_hi)
            cap_s[:, 2 * HALF:3 * HALF] = cap_of(kpos_lo, first[0:PIECE], pos_lo)
            hand_on(0)
        else:
            for piece in range(2):
                qt_s[piece] = q_s[piece].T

    wait_blocks(0)

    k_scale = E ** -0.5
    exp_scale = k_scale * math.log2(math.e)
    def keys(t, a, b):
        return kv_s[t, a // HALF, a % HALF:a % HALF + (b - a), :]

    def over_keys(src, t, base, segs):
        parts = []
        for a, b in ((0, ROWS // 2), (ROWS // 2, ROWS)):
            acc = None
            for c, d in segs:
                val = dot(src[a:b, base + c:base + d], keys(t, c, d))
                acc = val if acc is None else acc + val
            parts.append(acc)
        return jnp.concatenate(parts, axis=0)

    def side(ref, rows, base, segs):
        return jnp.concatenate([ref[rows, base + c:base + d] for c, d in segs], axis=1)

    def softmax(base, segs, h):
        rb = 16 if sum(d - c for c, d in segs) > HALF else 32
        for b in range(PIECE // rb):
            rows = slice(h * PIECE + b * rb, h * PIECE + (b + 1) * rb)
            s = jnp.minimum(side(s_s, rows, base, segs), side(cap_s, slice(b * rb, (b + 1) * rb), base, segs))
            m = jnp.max(s, axis=1, keepdims=True)
            e = jnp.exp2((s - m) * exp_scale)
            l = jnp.sum(e, axis=1, keepdims=True)
            p = (e * (1.0 / l)).astype(BF16)
            at = 0
            for c, d in segs:
                p_s[rows, base + c:base + d] = p[:, at:at + d - c]
                at += d - c

    def d2d(t, half, late):
        q = slice(2 if half and late else 0, 4)
        return rcopy(acc_s.at[t, half, q, 1 - core], rb1.at[t, half, q], d2d_send.at[t, half], d2d_recv.at[t, half], 1)

    def rs(t, half, g):
        return rcopy(comb.at[t, half, g], rb2.at[t, half, g], rs_send.at[1 - t * half], rs_recv.at[t, half], 2 * g)

    def add_peer(t, half, g, late):
        if half and late and g >= 2:
            comb[t, half, g] = jnp.zeros((PIECE, E), F32)
            return
        q = dev(2 * g) // 2
        comb[t, half, g] = acc_s[t, half, q, core] + rb1[t, half, q]

    def rs_sum(t, half, n):
        blks = rb1.at[0, 0, 0:n]
        return rcopy(blks, blks, rs_send.at[1 - t * half], rs_recv.at[t, half], 2)

    def combine_direct(t, half, late):
        d2d(t, half, late).wait_recv()
        for g in (3, 1, 2, 0):
            if not (half and late and g >= 2):
                add_peer(t, half, g, late)
                if g:
                    rs(t, half, g).start()

    first_dev = lax.rem(cy + core, 2) * 4 + lax.rem(cx + 1 - core, 2) * 2 + core
    second_dev = lax.rem(cy + 1 - core, 2) * 4 + lax.rem(cx + core, 2) * 2 + core
    first_g, second_g = 1 + core, 2 - core

    def to_first(t, half, i):
        if i == 0:
            src, dst, sem = comb.at[t, half, 3], relay.at[t, half], relay_recv.at[t]
        else:
            src, dst, sem = comb.at[t, half, first_g], rb2.at[t, half, 1], rs_recv.at[t, half]
        return pltpu.make_async_remote_copy(
            src_ref=src, dst_ref=dst, send_sem=rs_send.at[1], recv_sem=sem,
            device_id={'cp': first_dev}, device_id_type=pl.DeviceIdType.MESH)

    def to_second(t, half):
        return pltpu.make_async_remote_copy(
            src_ref=comb.at[t, half, second_g], dst_ref=rb2.at[t, half, 2], send_sem=rs_send.at[1],
            recv_sem=rs_recv.at[t, half], device_id={'cp': second_dev}, device_id_type=pl.DeviceIdType.MESH)

    def combine_relayed(t, half, late):
        d2d(t, half, late).wait_recv()
        add_peer(t, half, 3, late)
        to_first(t, half, 0).start()
        add_peer(t, half, 1, late)
        add_peer(t, half, 2, late)
        to_first(t, half, 1).start()
        add_peer(t, half, 0, late)

    def pass_on(t, half):
        to_first(t, half, 0).wait_recv()
        comb[t, half, second_g] = comb[t, half, second_g] + relay[t, half]
        to_second(t, half).start()

    QUART = HALF // 2

    def attention(late):
        hi = ((0, HALF), (HALF + QUART, SEQ)) if late else ((0, HALF), (HALF, SEQ))
        lo = ((0, HALF),) if late else ((0, QUART),)
        hi_blocks = [(a, min(a + 512, d)) for c, d in hi for a in range(c, d, 512)]
        lo_blocks = [(a, min(a + 512, d)) for c, d in lo for a in range(c, d, 512)]

        def grad(t, half, lhs_t, src):
            cuts = ((QUART, 512), (512, HALF)) if half and late else ((0, 256), (256, 512), (512, HALF))
            for a, b in cuts:
                c = b if late else min(b, QUART)
                if t == 0:
                    ds_rows(1, 0, ((half * HALF + a, half * HALF + b),))
                    if not half and c > a:
                        ds_rows(0, SEQ, ((a, c),))
                val = dot(lhs_t[1], src[:, half * HALF + a:half * HALF + b])
                if not half and c > a:
                    more = dot(lhs_t[0], src[:, SEQ + a:SEQ + c])
                    val = val + more if c == b else jnp.concatenate([val[:, :c - a] + more, val[:, c - a:]], axis=1)
                val = val.T
                for r in range(a - a % PIECE, b, PIECE):
                    c, d = max(a, r), min(b, r + PIECE)
                    slot = r // PIECE
                    acc_s[t, half, slot // 2, slot % 2, c - r:d - r, :] = val[c - a:d - a]
            d2d(t, half, late).start()

        def s_part(piece, base, a, b, r0=0, r1=ROWS):
            s_s[r0:r1, base + a:base + b] = dot(q_s[piece, r0:r1, :], keys(0, a, b), NT)

        def dp_part(piece, base, a, b):
            dp_s[:, base + a:base + b] = dot(do_s[piece], keys(1, a, b), NT)

        def o_part(piece, base, segs):
            o_bf = over_keys(p_s, 1, base, segs).astype(BF16)
            delta_s[piece] = jnp.sum(do_s[piece].astype(F32) * o_bf.astype(F32), axis=1, keepdims=True)
            for h in range(HEADS):
                o_s[piece * PIECE:(piece + 1) * PIECE, h * E:(h + 1) * E] = o_bf[h * PIECE:(h + 1) * PIECE]

        def ds_rows(piece, base, segs):
            for h in range(HEADS):
                for c in range(PIECE // 32):
                    r0 = h * PIECE + c * 32
                    for a, b in segs:
                        ds_s[r0:r0 + 32, base + a:base + b] = (
                            p_s[r0:r0 + 32, base + a:base + b].astype(F32)
                            * (dp_s[r0:r0 + 32, base + a:base + b] - delta_s[piece, r0:r0 + 32, :])).astype(BF16)

        def dq_part(piece, base, segs):
            dq_bf = (over_keys(ds_s, 0, base, segs) * k_scale).astype(BF16)
            for h in range(HEADS):
                dq_s[piece * PIECE:(piece + 1) * PIECE, h * E:(h + 1) * E] = dq_bf[h * PIECE:(h + 1) * PIECE]

        def softmax_with(base, segs, h0, h1, others):
            for h in range(h0, h1):
                softmax(base, segs, h)
                left = h1 - h
                take = -(-len(others) // left)
                for fn in others[:take]:
                    fn()
                others = others[take:]

        for a, b in hi_blocks:
            s_part(1, 0, a, b, 0, 192)
        for piece in range(2):
            dot_s[piece] = do_s[piece].T
        softmax_with(0, hi, 0, 2, [lambda a=a, b=b: s_part(1, 0, a, b, 192, ROWS) for a, b in hi_blocks])
        hand_on(1)
        softmax_with(0, hi, 2, HEADS, [lambda a=a, b=b: s_part(0, SEQ, a, b) for a, b in lo_blocks])
        grad(1, 1, dot_s, p_s)
        wait_blocks(1)
        softmax_with(SEQ, lo, 0, HEADS, [lambda a=a, b=b: dp_part(1, 0, a, b) for a, b in hi_blocks])
        grad(1, 0, dot_s, p_s)
        combine_direct(1, 1, late)
        o_part(1, 0, hi)
        for a, b in lo_blocks:
            dp_part(0, SEQ, a, b)
        grad(0, 1, qt_s, ds_s)
        combine_relayed(1, 0, late)
        o_part(0, SEQ, lo)
        grad(0, 0, qt_s, ds_s)
        combine_relayed(0, 1, late)
        dq_part(1, 0, hi)
        dq_part(0, SEQ, lo)

    for late in range(2):
        pl.when(cy == late)(lambda late=late: attention(late))

    combine_direct(0, 0, 0)
    NY = 896

    def y_part(a, b):
        y_s[:, a:b] = dot(o_s[...], wo_s[:, a:b]).astype(BF16)

    y_part(0, 1792)
    pass_on(1, 0)
    y_part(1792, D)
    pass_on(0, 1)
    def put_total(t, half, tot):
        if t == 0:
            tot = tot * k_scale
        dkv_s[half * PIECE:(half + 1) * PIECE, t * E:(t + 1) * E] = tot.astype(BF16)

    @pl.when(cy == 0)
    def _():
        rs_sum(1, 1, 1).wait_recv()
        put_total(1, 1, comb[1, 1, 0] + rb2[1, 1, 1])

    @pl.when(cy == 1)
    def _():
        rs_sum(1, 1, 3).wait_recv()
        put_total(1, 1, (comb[1, 1, 0] + rb2[1, 1, 1]) + (rb2[1, 1, 2] + rb2[1, 1, 3]))

    for i in range(D // NY):
        dx_s[:, i * NY:(i + 1) * NY] = dot(dq_s[...], side_by_side(wq_s, 0, HEADS, i * NY, (i + 1) * NY), NT)

    for t, half in UNITS[1:3]:
        rs_sum(t, half, 2).wait_recv()
        put_total(t, half, comb[t, half, 0] + (rb2[t, half, 1] + rb2[t, half, 2]))
    rs_sum(0, 0, 3).wait_recv()
    put_total(0, 0, (comb[0, 0, 0] + rb2[0, 0, 1]) + (rb2[0, 0, 2] + rb2[0, 0, 3]))

    doc_sum.wait_send()
    for t in range(2):
        four = kv_s.at[t, :, 0:4 * PIECE, :]
        rcopy(four, four, kv_send.at[t], kv_recv.at[t, 0], 1).wait_send()

    @pl.when(core == 1)
    def _():
        for t in range(2):
            kv_sum(t, 6).wait_send()

    for t in range(2):
        d2d(t, 0, 0).wait_send()

    @pl.when(cy == 0)
    def _():
        for t in range(2):
            d2d(t, 1, 0).wait_send()
        rs_sum(1, 1, 3).wait_send()

    @pl.when(cy == 1)
    def _():
        for t in range(2):
            d2d(t, 1, 1).wait_send()
        rs_sum(1, 1, 1).wait_send()

    nine = s_s.at[0:9 * PIECE * E // (3 * HALF), :]
    rcopy(nine, nine, rs_send.at[1], rs_recv.at[0, 0], 2).wait_send()


FIN = ((0, 1536), (1536, 2560), (2560, 3584))


def final_kernel(y_s, dx_s, dkv_s, wkv_s, y_hbm, dx_hbm, dxo_s, y_sem, dx_sem):
    y_cp = pltpu.make_async_copy(y_s, y_hbm, y_sem)
    y_cp.start()
    copies = [y_cp]
    for i, (a, b) in enumerate(FIN):
        dxo_s[:, a:b] = (dx_s[:, a:b] + dot(dkv_s[...], side_by_side(wkv_s, 0, 2, a, b), NT)).astype(BF16)
        cp = pltpu.make_async_copy(dxo_s.at[:, a:b], dx_hbm.at[:, a:b], dx_sem.at[i])
        cp.start()
        copies.append(cp)
    for cp in copies:
        cp.wait()


def solution(mesh):
    row_spec = P(('dp', 'cp'))
    full_spec = P()
    hbm_spec = pl.BlockSpec(memory_space=pltpu.HBM)
    vmem_spec = pl.BlockSpec(memory_space=pltpu.VMEM)

    def local_layer(x_in, dy_in, doc_id, w_q, w_k, w_v, w_o):
        V = pltpu.VMEM
        dma = pltpu.SemaphoreType.DMA
        sds = jax.ShapeDtypeStruct
        hbm = lambda a: pltpu.with_memory_space_constraint(a, pltpu.HBM)
        parts = pl.pallas_call(
            main_kernel,
            out_shape=(V((TOK, D), BF16), V((TOK, D), F32), V((TOK, 2 * E), BF16), V((2, D, E), BF16)),
            in_specs=[hbm_spec, hbm_spec, hbm_spec, hbm_spec, hbm_spec, hbm_spec, hbm_spec],
            out_specs=(vmem_spec,) * 4,
            scratch_shapes=[
                V((TOK, D), BF16), V((TOK, D), BF16), V((HEADS, D, E), BF16), V((HE, D), BF16), V((1, TOK), jnp.int32),
                V((2, 2, HALF, E), BF16), V((NDEV, 1, TOK), jnp.int32),
                V((2, ROWS, E), BF16), V((2, ROWS, E), BF16), V((2, E, ROWS), BF16), V((2, E, ROWS), BF16),
                V((PIECE, 3 * HALF), F32),
                V((ROWS, 3 * HALF), F32), V((ROWS, 3 * HALF), BF16), V((ROWS, 3 * HALF), F32),
                V((ROWS, 3 * HALF), BF16),
                V((TOK, HE), BF16), V((TOK, HE), BF16), V((2, ROWS, 1), F32),
                V((2, 2, 4, 2, PIECE, E), F32),
                V((2, 2, 4, PIECE, E), F32), V((2, 2, 4, PIECE, E), F32), V((2, 2, 4, PIECE, E), F32), V((2, 2, PIECE, E), F32),
                dma((len(KPARTS), 3)), dma((3,)), dma((2,)), dma, dma,
                dma, dma, dma((2,)), dma((2, 2)), dma((2,)),
                dma((2, 2)), dma((2, 2)), dma((2,)), dma((2, 2)), dma((2,)),
            ],
            compiler_params=pltpu.CompilerParams(collective_id=0, has_side_effects=True,
                                                 vmem_limit_bytes=50 * 1024 * 1024),
        )(hbm(x_in), hbm(dy_in), hbm(doc_id.reshape(1, TOK)), hbm(jnp.transpose(w_q, (1, 0, 2))), hbm(w_k.reshape(D, E)),
          hbm(w_v.reshape(D, E)), hbm(w_o.reshape(HE, D)))
        return pl.pallas_call(
            final_kernel,
            out_shape=(sds((TOK, D), BF16), sds((TOK, D), BF16)),
            in_specs=[vmem_spec] * 4,
            out_specs=(hbm_spec, hbm_spec),
            scratch_shapes=[V((TOK, D), BF16), dma, dma((len(FIN),))],
            compiler_params=pltpu.CompilerParams(vmem_limit_bytes=12 * 1024 * 1024),
        )(*[pltpu.with_memory_space_constraint(a, pltpu.VMEM) for a in parts])

    return jax.shard_map(local_layer, mesh=mesh,
                         in_specs=(row_spec, row_spec, row_spec, full_spec, full_spec, full_spec, full_spec),
                         out_specs=(row_spec, row_spec), check_vma=False)
```
